32 devices in a mesh: dp: 1 (over z), sz: 4 (over y), sy: 4 (over x), sx: 2 (over core).
Axes of the slice: x: 4, y: 4, z: 1, core: 2. Of those that a mesh axis runs over, the one named last changes fastest.
The devices are a block of a 4x4x8 slice.
Arguments:
- rhs_grid: float32 [256, 256, 256], P(('dp', 'sx'), 'sy', 'sz')
- u_start: float32 [256, 256, 256], P(('dp', 'sx'), 'sy', 'sz')
Outputs:
- output: float32 [256, 256, 256], P(('dp', 'sx'), 'sy', 'sz')
All inputs are finite; a program needn't handle non-finite values.
Results may differ from the reference program's by a relative error of at most 0.001.
Values sent between devices are 32-bit elements.
A program may use at most 768 MiB of HBM per device.

```python
import math
import jax
import jax.numpy as jnp
from jax import lax

GRID_SIZE = 256
LEVELS = 4
SMOOTH_SWEEPS = 2
COARSE_SWEEPS = 16
BUMPS = 8


def setup_inputs(seed: int = 0, part: int = 0) -> dict:
    key = jax.random.fold_in(jax.random.key(seed), part)
    key_amp, key_pos, key_bump, key_init = jax.random.split(key, 4)
    cells = jnp.arange(GRID_SIZE, dtype=jnp.float32)
    coords = (cells + 1.0) / (GRID_SIZE + 1)
    sine = jnp.sin(math.pi * coords)
    mode_amp = jax.random.uniform(key_amp, (), jnp.float32, 0.5, 1.5)
    smooth = (3.0 * math.pi ** 2) * mode_amp * sine[:, None, None] * sine[None, :, None] * sine[None, None, :]
    centers = jax.random.randint(key_pos, (BUMPS, 3), 1, 8).astype(jnp.float32) * (GRID_SIZE // 8) - 0.5
    width = GRID_SIZE / 32.0
    bump_amp = jax.random.normal(key_bump, (BUMPS,), jnp.float32) * (0.8 * ((GRID_SIZE + 1) / width) ** 2)
    gauss = jnp.exp(-((cells[None, :, None] - centers[:, None, :]) ** 2) / (2.0 * width ** 2))
    bumps = jnp.einsum('bi,bj,bk->ijk', gauss[:, :, 0] * bump_amp[:, None], gauss[:, :, 1], gauss[:, :, 2])
    rhs_grid = smooth + bumps
    u_start = jax.random.normal(key_init, (GRID_SIZE, GRID_SIZE, GRID_SIZE), jnp.float32)
    return {'rhs_grid': rhs_grid, 'u_start': u_start}


def neighbour_sum(field):
    padded = jnp.pad(field, 1)
    return (padded[:-2, 1:-1, 1:-1] + padded[2:, 1:-1, 1:-1]
            + padded[1:-1, :-2, 1:-1] + padded[1:-1, 2:, 1:-1]
            + padded[1:-1, 1:-1, :-2] + padded[1:-1, 1:-1, 2:])


def residual(source, field, stiffness):
    return source - stiffness * (6.0 * field - neighbour_sum(field))


def jacobi_sweep(source, field, stiffness):
    return field + residual(source, field, stiffness) / (9.0 * stiffness)


def restrict_axis(fine, axis):
    half = fine.shape[axis] // 2
    pairs = fine.reshape(fine.shape[:axis] + (half, 2) + fine.shape[axis + 1:])
    even = lax.index_in_dim(pairs, 0, axis + 1, keepdims=False)
    odd = lax.index_in_dim(pairs, 1, axis + 1, keepdims=False)
    lower = jnp.zeros_like(lax.slice_in_dim(odd, 0, 1, axis=axis))
    odd_prev = jnp.concatenate([lower, lax.slice_in_dim(odd, 0, half - 1, axis=axis)], axis=axis)
    return 0.25 * (odd_prev + odd) + 0.5 * even


def prolong_axis(coarse, axis):
    length = coarse.shape[axis]
    upper = jnp.zeros_like(lax.slice_in_dim(coarse, 0, 1, axis=axis))
    shifted = jnp.concatenate([lax.slice_in_dim(coarse, 1, length, axis=axis), upper], axis=axis)
    stacked = jnp.stack([coarse, 0.5 * (coarse + shifted)], axis=axis + 1)
    return stacked.reshape(coarse.shape[:axis] + (2 * length,) + coarse.shape[axis + 1:])


def restrict(fine):
    for axis in range(3):
        fine = restrict_axis(fine, axis)
    return fine


def prolong(coarse):
    for axis in range(3):
        coarse = prolong_axis(coarse, axis)
    return coarse


def vcycle(level, source, field):
    stiffness = ((GRID_SIZE + 1) / 2 ** level) ** 2
    coarsest = level == LEVELS - 1
    sweeps = COARSE_SWEEPS if coarsest else SMOOTH_SWEEPS
    if field is None:
        field = source / (9.0 * stiffness)
        sweeps = sweeps - 1
    for sweep in range(sweeps):
        field = jacobi_sweep(source, field, stiffness)
    if coarsest:
        return field
    correction = vcycle(level + 1, restrict(residual(source, field, stiffness)), None)
    field = field + prolong(correction)
    for sweep in range(SMOOTH_SWEEPS):
        field = jacobi_sweep(source, field, stiffness)
    return field


def reference(rhs_grid, u_start):
    return vcycle(0, rhs_grid, u_start)
```

```python
import functools
import types
import jax
import jax.numpy as jnp
from jax import lax
from jax.experimental import pallas as pl
from jax.experimental.pallas import tpu as pltpu
from jax.sharding import PartitionSpec as P

F32 = jnp.float32
MESH = pl.DeviceIdType.MESH
HX = 8
TOP = 8
COARSE_SWEEPS = 16
CHUNK = 16
OPPOSITE = (1, 0, 3, 2, 7, 6, 5, 4)
STEP_Y = (-1, 1, 0, 0, -1, -1, 1, 1)
STEP_Z = (0, 0, -1, 1, -1, 1, -1, 1)


def make_level(nx, ny, nz, y0, rows, wide):
    lv = types.SimpleNamespace(nx=nx, ny=ny, nz=nz, y0=y0, rows=rows, wide=wide)
    lv.depth = rows + 16
    lv.planes = nx + 2 * HX
    lv.packs = 128 // nz
    lv.groups = nx // 16
    lv.own = pl.ds(y0, ny)
    lv.all = pl.ds(TOP, rows)
    return lv


def lanes_of(shape):
    return lax.broadcasted_iota(jnp.int32, shape, 1)


def rows_of(shape):
    return lax.broadcasted_iota(jnp.int32, shape, 0)


def roll(x, shift, axis=1):
    return pltpu.roll(x, shift, axis)


def signed(lane):
    return jnp.where(lane < 96, lane, lane - 128)


def kernel(cfg, rhs, start, out, *scratch):
    (stage_u, stage_f, u0, v0, f0, a1, b1, p1, a2, b2, p2, e3, pz, pb, s3, p3, slots, message,
     sy0, sz0, sd0, ry0, rz0, rd0, sy1, sz1, sd1, ry1, rz1, rd1, sy2, sz2, sd2, ry2, rz2, rd2,
     load_sem, out_sem, send_sem, recv_sem, xs_sem, xr_sem, gs_sem, gr_sem) = scratch
    l0, l1, l2 = cfg.levels
    n_x, n_y, n_z = cfg.counts
    cx, cy, cz = lax.axis_index('sx'), lax.axis_index('sy'), lax.axis_index('sz')
    total = n_x * n_y * n_z
    rank = (cz * n_y + cy) * n_x + cx
    turn = cy * n_z + cz

    def load(c, which):
        src, dst = ((start, stage_u), (rhs, stage_f))[which]
        return pltpu.make_async_copy(src.at[pl.ds(c * CHUNK, CHUNK)], dst.at[pl.ds(c * CHUNK, CHUNK)], load_sem.at[which, c])

    n_chunks = l0.nx // CHUNK
    for c in range(n_chunks):
        load(c, 0).start()
        load(c, 1).start()

    def peer(p):
        r = lax.rem(rank + p, total)
        return {'sz': r // (n_x * n_y), 'sy': (r // n_x) % n_y, 'sx': r % n_x}

    barrier = pltpu.get_barrier_semaphore()

    @pl.loop(1, total)
    def _(p):
        pl.semaphore_signal(barrier, inc=1, device_id=peer(p), device_id_type=MESH)

    comm = ((l0, (sy0, sz0, sd0), (ry0, rz0, rd0)), (l1, (sy1, sz1, sd1), (ry1, rz1, rd1)), (l2, (sy2, sz2, sd2), (ry2, rz2, rd2)))

    def exists(d):
        ok = None
        for step, at, count in ((STEP_Y[d], cy, n_y), (STEP_Z[d], cz, n_z)):
            if step:
                one = (at > 0) if step < 0 else (at < count - 1)
                ok = one if ok is None else jnp.logical_and(ok, one)
        return ok

    def buffer(bufs, d):
        return bufs[0].at[d] if d < 2 else bufs[1].at[d - 2] if d < 4 else bufs[2].at[d - 4]

    for lv, _, recv in comm:
        for d in range(8):
            @pl.when(jnp.logical_not(exists(d)))
            def _(recv=recv, d=d):
                buf = buffer(recv, d)

                @pl.loop(0, buf.shape[0])
                def _(i):
                    buf[i] = jnp.zeros(buf.shape[1:], F32)

    for lv, arrays in ((l0, (u0, v0)), (l1, (a1, b1)), (l2, (a2, b2))):
        zero = jnp.zeros((8, 128), F32)
        for arr in arrays:
            @pl.loop(0, lv.planes)
            def _(x, arr=arr, lv=lv):
                arr[x, pl.ds(0, 8)] = zero
                arr[x, pl.ds(TOP + lv.rows, 8)] = zero

            @pl.when(cx == 0)
            def _(arr=arr, lv=lv):
                arr[HX - 1, lv.all] = jnp.zeros((lv.rows, 128), F32)

            @pl.when(cx == n_x - 1)
            def _(arr=arr, lv=lv):
                arr[HX + lv.nx, lv.all] = jnp.zeros((lv.rows, 128), F32)

    pl.semaphore_wait(barrier, total - 1)

    def domain(lv):
        shape = (lv.rows, 128)
        y = rows_of(shape) + (TOP - lv.y0) + cy * lv.ny
        k = signed(lanes_of(shape))
        z = k + cz * lv.nz
        ok = (y >= 0) & (y < n_y * lv.ny) & (z >= 0) & (z < n_z * lv.nz) & (k >= -8) & (k < lv.nz + 8)
        return jnp.where(ok, 1.0, 0.0).astype(F32)

    def first_plane(lv, wide):
        return HX - cx * wide

    def start_send(lv_index, d):
        _, send, recv = comm[lv_index]

        @pl.when(exists(d))
        def _():
            halo_copy(lv_index, d).start()

    def halo_copy(lv_index, d):
        _, send, recv = comm[lv_index]
        return pltpu.make_async_remote_copy(
            src_ref=buffer(send, d), dst_ref=buffer(recv, OPPOSITE[d]),
            send_sem=send_sem.at[lv_index, d], recv_sem=recv_sem.at[lv_index, OPPOSITE[d]],
            device_id={'sy': cy + STEP_Y[d], 'sz': cz + STEP_Z[d]}, device_id_type=MESH)

    def arrival(lv_index, d):
        _, send, recv = comm[lv_index]
        return pltpu.make_async_remote_copy(
            src_ref=buffer(send, d), dst_ref=buffer(recv, d),
            send_sem=send_sem.at[lv_index, d], recv_sem=recv_sem.at[lv_index, d],
            device_id={'sy': cy + STEP_Y[d], 'sz': cz + STEP_Z[d]}, device_id_type=MESH)

    def wait_recv(lv_index, d):
        @pl.when(exists(d))
        def _():
            arrival(lv_index, d).wait_recv()

    def wait_send(lv_index, d):
        @pl.when(exists(d))
        def _():
            halo_copy(lv_index, d).wait_send()

    def faces(lv_index, x):
        lv = comm[lv_index][0]
        if lv_index == 0:
            upper = rows_of((8, 128)) >= 4
            lo = jnp.where(upper, f0[HX + x, pl.ds(lv.y0 - 4, 8)], u0[HX + x, pl.ds(lv.y0, 8)])
            hi = jnp.where(upper, f0[HX + x, pl.ds(lv.y0 + lv.ny - 8, 8)], u0[HX + x, pl.ds(lv.y0 + lv.ny - 4, 8)])
            return lo, hi
        phi = (p1, p2)[lv_index - 1]
        return phi[HX + x, pl.ds(lv.y0, 8)], phi[HX + x, pl.ds(lv.y0 + lv.ny - 8, 8)]

    def pack_rows(lv_index):
        lv, send, _ = comm[lv_index]
        per = lv.nx // lv.packs
        lane = lanes_of((8, 128)) // lv.nz

        @pl.loop(0, per)
        def _(j):
            lo, hi = faces(lv_index, j)
            for q in range(1, lv.packs):
                more = faces(lv_index, j + q * per)
                lo = jnp.where(lane == q, roll(more[0], q * lv.nz), lo)
                hi = jnp.where(lane == q, roll(more[1], q * lv.nz), hi)
            send[0][0, j] = lo
            send[0][1, j] = hi

    def pack_corners(lv_index):
        lv, send, _ = comm[lv_index]
        lane = lanes_of((8, 128)) // 8

        @pl.loop(0, lv.groups)
        def _(g):
            def body(i, acc):
                lo, hi = faces(lv_index, g * 16 + i)
                here = lane == i
                up, down = 8 * i, (8 * i + 128 - (lv.nz - 8)) % 128
                return (jnp.where(here, roll(lo, up), acc[0]), jnp.where(here, roll(lo, down), acc[1]),
                        jnp.where(here, roll(hi, up), acc[2]), jnp.where(here, roll(hi, down), acc[3]))
            acc = lax.fori_loop(0, 16, body, (jnp.zeros((8, 128), F32),) * 4)
            for d in range(4):
                send[2][d, g] = acc[d]

    def pack_lanes(lv_index):
        lv, send, _ = comm[lv_index]
        phi = (p1, p2)[lv_index - 1]
        lane = lanes_of((lv.ny, 128)) // 8

        @pl.loop(0, lv.groups)
        def _(g):
            def body(i, acc):
                t = phi[HX + g * 16 + i, lv.own]
                here = lane == i
                return (jnp.where(here, roll(t, 8 * i), acc[0]),
                        jnp.where(here, roll(t, (8 * i + 128 - (lv.nz - 8)) % 128), acc[1]))
            acc = lax.fori_loop(0, 16, body, (jnp.zeros((lv.ny, 128), F32),) * 2)
            send[1][0, g] = acc[0]
            send[1][1, g] = acc[1]

    def unpack_rows(lv_index):
        lv, _, recv = comm[lv_index]
        per = lv.nx // lv.packs
        lane = lanes_of((8, 128))
        below, above = lane >= 120, (lane >= lv.nz) & (lane < lv.nz + 8)
        inside = lane < lv.nz

        @pl.loop(0, per)
        def _(j):
            for side in range(2):
                tile = recv[0][side, j]
                for q in range(lv.packs):
                    x = j + q * per
                    g, i = x // 16, x % 16
                    t = roll(tile, (128 - q * lv.nz) % 128) if q else tile
                    t = jnp.where(inside, t, 0.0)
                    t = jnp.where(below, roll(recv[2][2 * side, g], (120 + 128 - 8 * i) % 128), t)
                    t = jnp.where(above, roll(recv[2][2 * side + 1, g], (lv.nz + 128 - 8 * i) % 128), t)
                    if lv_index == 0:
                        row = lv.y0 + lv.ny if side else lv.y0 - 4
                        u0[HX + x, pl.ds(row, 4)] = t[:4]
                        f0[HX + x, pl.ds(row, 4)] = t[4:]
                    else:
                        row = lv.y0 + lv.ny if side else lv.y0 - 8
                        (p1, p2)[lv_index - 1][HX + x, pl.ds(row, 8)] = t

    def unpack_lanes(lv_index):
        lv, _, recv = comm[lv_index]
        lane = lanes_of((lv.ny, 128))
        if lv_index == 0:
            below, above = lane >= 124, (lane >= lv.nz) & (lane < lv.nz + 4)
            targets = ((u0, 124, lv.nz), (f0, 120, lv.nz - 4))
        else:
            below, above = lane >= 120, (lane >= lv.nz) & (lane < lv.nz + 8)
            targets = (((p1, p2)[lv_index - 1], 120, lv.nz),)

        @pl.loop(0, lv.groups)
        def _(g):
            lo, hi = recv[1][0, g], recv[1][1, g]

            @pl.loop(0, 16)
            def _(i):
                x = HX + g * 16 + i
                for arr, at_lo, at_hi in targets:
                    t = arr[x, lv.own]
                    t = jnp.where(below, roll(lo, (at_lo + 128 - 8 * i) % 128), t)
                    t = jnp.where(above, roll(hi, (at_hi + 128 - 8 * i) % 128), t)
                    arr[x, lv.own] = t

    def partner_copy(k, arr, lv, wide, up):
        src, dst = (HX + lv.nx - wide, HX - wide) if up else (HX, HX + lv.nx)
        return pltpu.make_async_remote_copy(
            src_ref=arr.at[pl.ds(src, wide), lv.all], dst_ref=arr.at[pl.ds(dst, wide), lv.all],
            send_sem=xs_sem.at[k], recv_sem=xr_sem.at[k],
            device_id={'sx': cx + 1 if up else cx - 1}, device_id_type=MESH)

    def partner_arrival(k, arr, lv, wide, up):
        planes = arr.at[pl.ds(HX + lv.nx if up else HX - wide, wide), lv.all]
        return pltpu.make_async_remote_copy(
            src_ref=planes, dst_ref=planes, send_sem=xs_sem.at[k], recv_sem=xr_sem.at[k],
            device_id={'sx': cx + 1 if up else cx - 1}, device_id_type=MESH)

    def partner_exchange(first, arrays, lv, wide):
        for up, here in ((True, cx < n_x - 1), (False, cx > 0)):
            @pl.when(here)
            def _(up=up):
                for k, arr in enumerate(arrays):
                    partner_copy(first + k, arr, lv, wide, up).start()
        for up, here in ((True, cx < n_x - 1), (False, cx > 0)):
            @pl.when(here)
            def _(up=up):
                for k, arr in enumerate(arrays):
                    partner_copy(first + k, arr, lv, wide, up).wait_send()
                    partner_arrival(first + k, arr, lv, wide, up).wait_recv()

    def exchange(lv_index, arrays, first, wide):
        for d in range(4, 8):
            start_send(lv_index, d)
        for d in range(4):
            start_send(lv_index, d)
        for d in range(8):
            wait_recv(lv_index, d)
        unpack_rows(lv_index)
        unpack_lanes(lv_index)
        partner_exchange(first, arrays, comm[lv_index][0], wide)
        for d in range(8):
            wait_send(lv_index, d)

    def neighbours(xm, c, xp, src, x, row, n):
        around = (xm + xp) + (src[x, pl.ds(row - 1, n)] + src[x, pl.ds(row + 1, n)])
        return around + (roll(c, 1) + roll(c, 127))

    def sweep(src, dst, phi, lv, wide, coef):
        begin = first_plane(lv, wide)

        def one(x, xm, c):
            xp = src[x + 1, lv.all]
            t = neighbours(xm, c, xp, src, x, TOP, lv.rows) + 3.0 * c + phi[x, lv.all]
            dst[x, lv.all] = t * coef
            return c, xp

        def body(i, carry):
            x = begin + 2 * i
            return one(x + 1, *one(x, *carry))
        lax.fori_loop(0, (lv.nx + wide) // 2, body, (src[begin - 1, lv.all], src[begin, lv.all]))

    def first_sweep(dst, phi, lv, wide, coef):
        begin = first_plane(lv, wide)

        @pl.loop(0, lv.nx + wide)
        def _(i):
            dst[begin + i, lv.all] = phi[begin + i, lv.all] * coef

    def last_sweep(src, phi, lv):
        shape = (lv.ny, 128)

        def copy_out(c):
            return pltpu.make_async_copy(stage_u.at[pl.ds(c * CHUNK, CHUNK)], out.at[pl.ds(c * CHUNK, CHUNK)], out_sem.at[c])

        def one(x, xm, c):
            xp = src[HX + x + 1, lv.own]
            t = neighbours(xm, c, xp, src, HX + x, lv.y0, lv.ny) + 3.0 * c + phi[HX + x, lv.own]
            stage_u[x] = (t * (1.0 / 9.0))[:, :lv.nz]
            return c, xp

        carry = (src[HX - 1, lv.own], src[HX, lv.own])
        for c in range(n_chunks):
            def body(i, carry, c=c):
                x = c * CHUNK + 2 * i
                return one(x + 1, *one(x, *carry))
            carry = lax.fori_loop(0, CHUNK // 2, body, carry)
            copy_out(c).start()
        for c in range(n_chunks):
            copy_out(c).wait()

    def restrict_planes(src, phi, lv, mask):
        def res(x, xm, c, xp):
            return neighbours(xm, c, xp, src, x, TOP, lv.rows) + phi[x, lv.all] - 6.0 * c

        def plane(x):
            return src[x, lv.all]
        pm2, pm1, pc = plane(HX - 2), plane(HX - 1), plane(HX)
        before = res(HX - 1, pm2, pm1, pc) * jnp.where(cx > 0, 1.0, 0.0).astype(F32)
        before = jnp.where(cx > 0, before, jnp.zeros_like(before))

        def body(i, carry):
            prev, xm, c = carry
            x = HX + 2 * i
            x1, x2 = plane(x + 1), plane(x + 2)
            even = res(x, xm, c, x1)
            odd = res(x + 1, c, x1, x2)
            pb[i, lv.all] = ((prev + odd) + (even + even)) * mask
            return odd, x1, x2
        lax.fori_loop(0, lv.nx // 2, body, (before, pm1, pc))

    def restricted_rows(i, lv):
        half = lv.ny // 2
        return ((pb[i, pl.ds(lv.y0 - 1, half, stride=2)] + pb[i, pl.ds(lv.y0 + 1, half, stride=2)])
                + 2.0 * pb[i, pl.ds(lv.y0, half, stride=2)])

    def restrict_weights(outside):
        fine = signed(rows_of((128, 128)))
        lane = lanes_of((128, 128))
        coarse = lane % 8 if outside is None else lane
        near = fine - 2 * coarse
        w = jnp.where(near == 0, 2.0, jnp.where((near == 1) | (near == -1), 1.0, 0.0)) * (1.0 / 16.0)
        if outside is not None:
            w = jnp.where(lane < outside, w, 0.0)
        return w.astype(F32)

    def dot(x, w):
        return jnp.dot(x, w, precision=lax.Precision.HIGHEST, preferred_element_type=F32)

    def restrict_level(src, phi, lv, mask, coarse_phi, coarse):
        restrict_planes(src, phi, lv, mask)
        w = restrict_weights(coarse.nz)
        step = 8

        @pl.loop(0, coarse.nx // step)
        def _(c):
            q = jnp.concatenate([restricted_rows(c * step + k, lv) for k in range(step)], axis=0)
            got = dot(q, w)
            for k in range(step):
                coarse_phi[HX + c * step + k, coarse.own] = got[k * coarse.ny:(k + 1) * coarse.ny]

    def prolong_level(e, e_hx, e_y0, e_rows, n_coarse, chunk, dst, lv, wide, mask):
        half = wide // 2
        begin = e_hx - cx * half
        near = signed(lanes_of((128, 128))) - 2 * signed(rows_of((128, 128)))
        w = jnp.where(near == 0, 1.0, jnp.where((near == 1) | (near == -1), 0.5, 0.0)).astype(F32)
        count = n_coarse + half + 1

        @pl.loop(0, count // chunk)
        def _(c):
            at = begin + c * chunk
            got = dot(e[pl.ds(at, chunk), pl.ds(8, e_rows)].reshape(chunk * e_rows, 128), w)
            pz[pl.ds(at, chunk), pl.ds(8, e_rows)] = got.reshape(chunk, e_rows, 128)
        row = e_y0 - (lv.y0 - TOP) // 2
        n = lv.rows // 2

        @pl.loop(0, count)
        def _(i):
            x = begin + i
            a = pz[x, pl.ds(row, n)]
            b = pz[x, pl.ds(row + 1, n)]
            pb[i, pl.ds(TOP, n, stride=2)] = a
            pb[i, pl.ds(TOP + 1, n, stride=2)] = 0.5 * (a + b)
        fine = first_plane(lv, wide)

        def body(i, a):
            b = pb[i + 1, lv.all]
            x = fine + 2 * i
            dst[x, lv.all] = (dst[x, lv.all] + a) * mask
            dst[x + 1, lv.all] = (dst[x + 1, lv.all] + 0.5 * (a + b)) * mask
            return b
        lax.fori_loop(0, n_coarse + half, body, pb[0, lv.all])

    lane0 = lanes_of((l0.ny, 128)) // 4
    pad = jnp.zeros((l0.ny, 128 - l0.nz), F32)

    @pl.loop(0, l0.groups)
    def _(g):
        load(g, 0).wait()
        load(g, 1).wait()

        def body(i, acc):
            lo, hi = acc
            x = g * 16 + i
            u = jnp.concatenate([stage_u[x], pad], axis=1)
            f = jnp.concatenate([stage_f[x], pad], axis=1) * cfg.scale
            u0[HX + x, l0.own] = u
            f0[HX + x, l0.own] = f
            at_u, at_f = lane0 == 2 * i, lane0 == 2 * i + 1
            lo = jnp.where(at_u, roll(u, 8 * i), jnp.where(at_f, roll(f, 8 * i + 4), lo))
            hi = jnp.where(at_u, roll(u, (8 * i + 128 - (l0.nz - 4)) % 128),
                           jnp.where(at_f, roll(f, (8 * i + 4 + 128 - (l0.nz - 4)) % 128), hi))
            return lo, hi
        lo, hi = lax.fori_loop(0, 16, body, (jnp.zeros((l0.ny, 128), F32),) * 2)
        sz0[0, g] = lo
        sz0[1, g] = hi
    pack_rows(0)
    pack_corners(0)
    exchange(0, (u0, f0), 0, 4)

    mask0 = domain(l0)
    sweep(u0, v0, f0, l0, 4, mask0 * (1.0 / 9.0))
    sweep(v0, u0, f0, l0, 2, mask0 * (1.0 / 9.0))
    restrict_level(u0, f0, l0, mask0, p1, l1)

    pack_rows(1)
    pack_lanes(1)
    pack_corners(1)
    exchange(1, (p1,), 2, 5)
    mask1 = domain(l1)
    first_sweep(a1, p1, l1, 6, mask1 * (1.0 / 9.0))
    sweep(a1, b1, p1, l1, 4, mask1 * (1.0 / 9.0))
    restrict_level(b1, p1, l1, mask1, p2, l2)

    pack_rows(2)
    pack_lanes(2)
    pack_corners(2)
    exchange(2, (p2,), 3, 6)
    mask2 = domain(l2)
    first_sweep(a2, p2, l2, 8, mask2 * (1.0 / 9.0))
    sweep(a2, b2, p2, l2, 6, mask2 * (1.0 / 9.0))

    restrict_planes(b2, p2, l2, mask2)
    nx3, ny3, nz3 = l2.nx // 2, l2.ny // 2, l2.nz // 2
    q = jnp.concatenate([restricted_rows(k, l2) for k in range(nx3)], axis=0)
    got = dot(q, restrict_weights(None))
    lane = lanes_of((8, 128))
    block = lane // 8
    packed = jnp.zeros((8, 128), F32)
    for k in range(nx3):
        packed = jnp.where(block == k, got[k * ny3:(k + 1) * ny3], packed)
    packed = roll(packed, 8 * turn)
    message[...] = packed
    slot = cx * (n_y * n_z) + turn
    slots[slot] = packed

    def gather_copy(p):
        return pltpu.make_async_remote_copy(
            src_ref=message, dst_ref=slots.at[slot], send_sem=gs_sem.at[p], recv_sem=gr_sem.at[slot],
            device_id=peer(p), device_id_type=MESH)

    @pl.loop(1, total)
    def _(p):
        gather_copy(p).start()

    @pl.loop(1, total)
    def _(p):
        who = peer(p)
        theirs = who['sx'] * (n_y * n_z) + who['sy'] * n_z + who['sz']
        pltpu.make_async_remote_copy(
            src_ref=message, dst_ref=slots.at[theirs], send_sem=gs_sem.at[p], recv_sem=gr_sem.at[theirs],
            device_id=who, device_id_type=MESH).wait_recv()

    span = nz3 * n_z
    turns = n_y * n_z
    whole = n_x * nx3
    for s in range(2):
        @pl.loop(0, 8)
        def _(i, s=s):
            s3[s, i] = jnp.zeros((8, 128), F32)
            s3[s, 8 + whole + i] = jnp.zeros((8, 128), F32)

    live = lane < 8 * turns

    @pl.loop(0, n_x)
    def _(half):
        @pl.loop(0, nx3)
        def _(k):
            which = (block + 128 - k) % 16
            acc = jnp.zeros((8, 128), F32)
            for t in range(turns):
                acc = jnp.where((block + (16 - t)) % 16 == k, slots[half * turns + t], acc)
            acc = jnp.where(live, roll(acc, (128 - 8 * k) % 128), 0.0)
            p3[half * nx3 + k] = acc
            s3[0, 8 + half * nx3 + k] = acc * (1.0 / 9.0)

    sub = rows_of((8, 128))
    z_first, z_last = lane % span == 0, lane % span == span - 1
    top_row, end_row = sub == 0, sub == 7
    y_first, y_last = top_row & (lane < span), end_row & (lane >= span * (n_y - 1))

    def coarse_sweep(k, carry):
        old, new = k % 2, (k + 1) % 2
        xm, c = s3[old, 7], s3[old, 8]
        for x in range(whole):
            xp = s3[old, 9 + x]
            down, up = roll(c, 1, 0), roll(c, 7, 0)
            ym = jnp.where(y_first, 0.0, jnp.where(top_row, roll(down, span % 128), down))
            yp = jnp.where(y_last, 0.0, jnp.where(end_row, roll(up, (128 - span) % 128), up))
            zm = jnp.where(z_first, 0.0, roll(c, 1))
            zp = jnp.where(z_last, 0.0, roll(c, 127))
            t = (xm + xp) + (ym + yp) + (zm + zp) + 3.0 * c + p3[x]
            s3[new, 8 + x] = t * (1.0 / 9.0)
            xm, c = c, xp
        return carry
    lax.fori_loop(0, COARSE_SWEEPS - 1, coarse_sweep, 0)
    last = (COARSE_SWEEPS - 1) % 2

    gz = signed(lane) + cz * nz3
    z_ok = (gz >= 0) & (gz < span) & (signed(lane) >= -8) & (signed(lane) < nz3 + 8)

    @pl.loop(0, nx3 + 8)
    def _(i):
        c = s3[last, cx * nx3 + i + 4]
        for k in range(3):
            t = roll(c, (256 - 8 * turn - (k - 1) * span) % 128)
            ok = z_ok
            if k == 0:
                ok = ok & (cy > 0)
            if k == 2:
                ok = ok & (cy < n_y - 1)
            e3[i, pl.ds(8 + 8 * k, 8)] = jnp.where(ok, t, 0.0)

    prolong_level(e3, 4, 16, 24, nx3, 5, b2, l2, 6, mask2)
    sweep(b2, a2, p2, l2, 4, mask2 * (1.0 / 9.0))
    sweep(a2, b2, p2, l2, 4, mask2 * (1.0 / 9.0))
    prolong_level(b2, HX, l2.y0, l2.rows, l2.nx, 7, b1, l1, 4, mask1)
    sweep(b1, a1, p1, l1, 4, mask1 * (1.0 / 9.0))
    sweep(a1, b1, p1, l1, 2, mask1 * (1.0 / 9.0))
    prolong_level(b1, HX, l1.y0, l1.rows, l1.nx, 6, u0, l0, 2, mask0)
    sweep(u0, v0, f0, l0, 2, mask0 * (1.0 / 9.0))
    last_sweep(v0, f0, l0)

    @pl.loop(1, total)
    def _(p):
        gather_copy(p).wait_send()


def local_cycle(rhs, start, counts, size):
    nx, ny, nz = rhs.shape
    levels = (make_level(nx, ny, nz, 12, ny + 8, 4), make_level(nx // 2, ny // 2, nz // 2, 16, ny // 2 + 16, 5),
              make_level(nx // 4, ny // 4, nz // 4, 16, ny // 4 + 16, 6))
    l0, l1, l2 = levels
    cfg = types.SimpleNamespace(levels=levels, counts=counts, scale=1.0 / (size + 1) ** 2)
    total = counts[0] * counts[1] * counts[2]

    def vmem(*shape):
        return pltpu.VMEM(shape, F32)

    def ext(lv):
        return vmem(lv.planes, lv.depth, 128)

    def messages(lv):
        return [vmem(2, lv.nx // lv.packs, 8, 128), vmem(2, lv.groups, lv.ny, 128), vmem(4, lv.groups, 8, 128)] * 2

    whole = counts[0] * (l2.nx // 2)
    scratch = [vmem(nx, ny, nz), vmem(nx, ny, nz), ext(l0), ext(l0), ext(l0), ext(l1), ext(l1), ext(l1), ext(l2), ext(l2), ext(l2),
               vmem(l2.nx // 2 + 8, 40, 128), vmem(l1.planes, l1.depth, 128), vmem(l1.planes, l0.depth, 128),
               vmem(2, whole + 16, 8, 128), vmem(whole, 8, 128), vmem(total, 8, 128), vmem(8, 128)]
    scratch += messages(l0) + messages(l1) + messages(l2)
    dma = pltpu.SemaphoreType.DMA
    scratch += [dma((2, nx // CHUNK)), dma((nx // CHUNK,)), dma((3, 8)), dma((3, 8)), dma((4,)), dma((4,)), dma((total,)), dma((total,))]
    return pl.pallas_call(
        functools.partial(kernel, cfg),
        out_shape=jax.ShapeDtypeStruct(rhs.shape, F32),
        in_specs=[pl.BlockSpec(memory_space=pl.ANY)] * 2,
        out_specs=pl.BlockSpec(memory_space=pl.ANY),
        scratch_shapes=scratch,
        compiler_params=pltpu.CompilerParams(collective_id=0, has_side_effects=True, vmem_limit_bytes=62 << 20),
    )(rhs, start)


def solution(mesh):
    counts = (mesh.shape['sx'], mesh.shape['sy'], mesh.shape['sz'])
    spec = P(('dp', 'sx'), 'sy', 'sz')

    def run(rhs_grid, u_start):
        size = rhs_grid.shape[0] // mesh.shape['dp']
        cycle = functools.partial(local_cycle, counts=counts, size=size)
        return jax.shard_map(cycle, mesh=mesh, in_specs=(spec, spec), out_specs=spec, check_vma=False)(rhs_grid, u_start)
    return run
```

```python
import functools
import types
import jax
import jax.numpy as jnp
from jax import lax
from jax.experimental import pallas as pl
from jax.experimental.pallas import tpu as pltpu
from jax.sharding import PartitionSpec as P

F32 = jnp.float32
MESH = pl.DeviceIdType.MESH
LANES = 128
TILE = 8
NINTH = 1.0 / 9.0
COARSE_SWEEPS = 16
OPPOSITE = (1, 0, 3, 2, 7, 6, 5, 4)
STEP_Y = (-1, 1, 0, 0, -1, -1, 1, 1)
STEP_Z = (0, 0, -1, 1, -1, 1, -1, 1)
SIDES = range(len(STEP_Y))


def make_level(shape, hx, z0, top, rows, begin, group, count, wide, block):
    ny, nz, nx = shape
    lv = types.SimpleNamespace(ny=ny, nz=nz, nx=nx, hx=hx, z0=z0, top=top, rows=rows, begin=begin, group=group, count=count, wide=wide)
    lv.planes = ny + 2 * hx
    lv.depth = nz + 2 * z0
    lv.parts = max(nx // LANES, 1)
    lv.own = pl.ds(z0, nz)
    lv.all = pl.ds(top, rows)
    lv.blocks = [(top + i, min(block, rows - i)) for i in range(0, rows, block)]
    return lv


def lanes_of(shape):
    return lax.broadcasted_iota(jnp.int32, shape, len(shape) - 1)


def rows_of(shape):
    return lax.broadcasted_iota(jnp.int32, shape, len(shape) - 2)


def roll(x, shift):
    return pltpu.roll(x, shift, 1)


def from_below(x):
    return jnp.where(lanes_of(x.shape) == 0, 0.0, roll(x, 1))


def from_above(x):
    return jnp.where(lanes_of(x.shape) == LANES - 1, 0.0, roll(x, LANES - 1))


def halves(x):
    return x[:, :LANES], x[:, LANES:]


def get(ref, p, rows, lv):
    return [ref[p, h, rows] for h in range(lv.parts)]


def put(ref, p, rows, values):
    for h, value in enumerate(values):
        ref[p, h, rows] = value


def every(f, *lists):
    return [f(*values) for values in zip(*lists)]


def join(*parts):
    return jnp.concatenate(parts, axis=1)


def stack(parts):
    return jnp.concatenate(parts, axis=0)


def back(shift):
    return (4 * LANES - shift) % LANES


def flag(condition):
    return jnp.where(condition, 1, 0)


def dot(x, w):
    return jnp.dot(x, w, precision=lax.Precision.HIGHEST, preferred_element_type=F32)


def kernel(cfg, rhs, start, out, *scratch):
    (u0, v0, f0, a1, b1, g1, a2, b2, g2, e3, pz, pb, stage_u, stage_f, part_u, part_f, s3, g3, slots, message, mask0, mask1, mask2,
     send_z, recv_z, recv_d, recv_yu, recv_yf, wide_in, wide_nat, wide_out,
     load_sem, out_sem, fine_s, fine_r, send_sem, recv_sem, all_s, all_r) = scratch
    l0, l1, l2 = levels = cfg.levels
    masks = (mask0, mask1, mask2)
    n_x, n_y, n_z = cfg.counts
    cx, cy, cz = lax.axis_index('sx'), lax.axis_index('sy'), lax.axis_index('sz')
    total = n_x * n_y * n_z
    rank = (cz * n_y + cy) * n_x + cx
    row_blocks = n_x * n_y
    yb = cy * n_x + cx

    inner = pl.ds(TILE, l0.nz)
    loads = [pltpu.make_async_copy(src, dst.at[:, inner], load_sem.at[k]) for k, (src, dst) in enumerate(((start, stage_u), (rhs, stage_f)))]
    for copy in loads:
        copy.start()

    def peer(p):
        r = lax.rem(rank + p, total)
        return {'sz': r // row_blocks, 'sy': (r // n_x) % n_y, 'sx': r % n_x}

    barrier = pltpu.get_barrier_semaphore()

    @pl.loop(1, total)
    def _(p):
        pl.semaphore_signal(barrier, inc=1, device_id=peer(p), device_id_type=MESH)

    def inside(step, at, count):
        if step == 0:
            return True
        return at > 0 if step < 0 else at < count - 1

    def exists(d):
        return jnp.logical_and(inside(STEP_Y[d], yb, row_blocks), inside(STEP_Z[d], cz, n_z))

    def zero(ref):
        @pl.loop(0, ref.shape[0])
        def _(i):
            ref[i] = jnp.zeros(ref.shape[1:], F32)

    def span(step, first, n, wide, own):
        if step == 0:
            return pl.ds(first, n)
        if step < 0:
            return pl.ds(first if own else first - wide, wide)
        return pl.ds(first + n - wide if own else first + n, wide)

    def region(index, d, own):
        lv, arr = levels[index], (None, g1, g2)[index]
        return arr.at[span(STEP_Y[d], lv.hx, lv.ny, lv.wide, own), 0, span(STEP_Z[d], lv.z0, lv.nz, TILE, own)]

    def halo_copy(index, d, arriving):
        k = index - 1
        at = yb + STEP_Y[d]
        return pltpu.make_async_remote_copy(
            src_ref=region(index, d, not arriving), dst_ref=region(index, d if arriving else OPPOSITE[d], False),
            send_sem=send_sem.at[k, d], recv_sem=recv_sem.at[k, d if arriving else OPPOSITE[d]],
            device_id={'sx': at % n_x, 'sy': at // n_x, 'sz': cz + STEP_Z[d]}, device_id_type=MESH)

    def each(act):
        for d in (4, 5, 6, 7, 2, 3, 0, 1):
            @pl.when(exists(d))
            def _(d=d):
                act(d)

    def exchange(index):
        each(lambda d: halo_copy(index, d, False).start())
        each(lambda d: halo_copy(index, d, True).wait_recv())

    def drain(index):
        each(lambda d: halo_copy(index, d, False).wait_send())

    chip_y = n_x * l0.ny
    reach = l0.ny + l0.wide
    outer = 2 * cx - 1

    def fine_copies():
        got = []

        def add(sends, arrives, src, dst, arrival, k, theirs, **to):
            made = [pltpu.make_async_remote_copy(
                src_ref=a, dst_ref=b, send_sem=fine_s.at[k], recv_sem=fine_r.at[r], device_id=to, device_id_type=MESH)
                for a, b, r in ((src, dst, theirs[0]), (arrival, arrival, theirs[1]))]
            got.append((sends, arrives, *made))
        n = 0
        for z_side, z_step in enumerate((-1, 1)):
            for y_side, y_step in enumerate((-1, 1)):
                edge = pl.ds(0 if y_step < 0 else chip_y - l0.wide, l0.wide)
                to_z = jnp.logical_and(inside(y_step, cy, n_y), inside(z_step, cz, n_z))
                in_z = jnp.logical_and(jnp.logical_and((cy + outer >= 0) & (cy + outer < n_y), inside(z_step, cz, n_z)), True)
                add(to_z, in_z, send_z.at[z_side, edge], recv_d.at[1 - z_side, cx], recv_d.at[z_side, y_side], n,
                    (8 + 2 * (1 - z_side) + cx, 8 + 2 * z_side + y_side), sx=1 - y_side, sy=cy + y_step, sz=cz + z_step)
                n += 1
        for z_side, z_step in enumerate((-1, 1)):
            for core in range(n_x):
                there = inside(z_step, cz, n_z)
                add(there, there, send_z.at[z_side, pl.ds(core * (chip_y - reach), reach)], recv_z.at[1 - z_side, cx],
                    recv_z.at[z_side, core], n, (12 + 2 * (1 - z_side) + cx, 12 + 2 * z_side + core), sx=core, sz=cz + z_step)
                n += 1
        return got

    def row_copies():
        got = []
        here = (cy + outer >= 0) & (cy + outer < n_y)
        for y_side, y_step in enumerate((-1, 1)):
            edge = pl.ds(0 if y_step < 0 else chip_y - l0.wide, l0.wide)
            for k, (stage, buf) in enumerate(((stage_u, recv_yu), (stage_f, recv_yf))):
                made = [pltpu.make_async_remote_copy(
                    src_ref=a, dst_ref=b, send_sem=fine_s.at[8 + 2 * y_side + k], recv_sem=fine_r.at[2 * r + k],
                    device_id={'sx': 1 - y_side, 'sy': cy + y_step}, device_id_type=MESH)
                    for a, b, r in ((stage.at[edge, inner], buf.at[cx], cx), (buf.at[y_side], buf.at[y_side], y_side))]
                got.append((inside(y_step, cy, n_y), here, *made))
        return got

    def partner_copies():
        other = pl.ds((1 - cx) * (chip_y - reach), reach)
        return [pltpu.make_async_remote_copy(
            src_ref=stage.at[other, inner], dst_ref=buf, send_sem=fine_s.at[12 + k], recv_sem=fine_r.at[4 + k],
            device_id={'sx': 1 - cx}, device_id_type=MESH) for k, (stage, buf) in enumerate(((stage_u, part_u), (stage_f, part_f)))]

    def begin(copies):
        for sends, _, copy, _ in copies:
            @pl.when(sends)
            def _(copy=copy):
                copy.start()

    def arrive(copies):
        for _, arrives, _, copy in copies:
            @pl.when(arrives)
            def _(copy=copy):
                copy.wait_recv()

    def finish(copies):
        for sends, _, copy, _ in copies:
            @pl.when(sends)
            def _(copy=copy):
                copy.wait_send()

    @pl.when(jnp.logical_not((cy + outer >= 0) & (cy + outer < n_y)))
    def _():
        for buf in (recv_yu, recv_yf, recv_d):
            for k in range(2):
                zero(buf.at[k])
    for z_side, z_step in enumerate((-1, 1)):
        @pl.when(jnp.logical_not(inside(z_step, cz, n_z)))
        def _(z_side=z_side):
            for core in range(n_x):
                zero(recv_z.at[z_side, core])
            zero(recv_d.at[z_side])
    for index in (1, 2):
        for d in SIDES:
            @pl.when(jnp.logical_not(exists(d)))
            def _(index=index, d=d):
                zero(region(index, d, False))

    for lv, arrays in ((l0, (u0, v0)), (l1, (a1, b1)), (l2, (a2, b2))):
        for arr in arrays:
            for plane, outside in ((lv.hx - 1, yb == 0), (lv.hx + lv.ny, yb == row_blocks - 1)):
                @pl.when(outside)
                def _(arr=arr, lv=lv, plane=plane):
                    put(arr, plane, lv.all, [jnp.zeros((lv.rows, LANES), F32)] * lv.parts)

    for lv, table in zip(levels, masks):
        shape = (lv.rows, LANES)
        z = rows_of(shape) + (lv.top - lv.z0) + cz * lv.nz
        ok = (z >= 0) & (z < n_z * lv.nz) & (lanes_of(shape) < lv.nx)
        table[0] = jnp.zeros(shape, F32)
        table[1] = jnp.where(ok, 1.0, 0.0).astype(F32)
        table[2] = jnp.where(ok, NINTH, 0.0).astype(F32)

    def valid(lv, p):
        y = p + (yb * lv.ny - lv.hx)
        return flag((y >= 0) & (y < row_blocks * lv.ny))

    big = (2 * LANES, 2 * LANES)
    r, c = rows_of(big), lanes_of(big)

    def cell(k):
        return jnp.where(k < LANES, 2 * k, 2 * k - (2 * LANES - 1))

    def mine(k):
        return (k + LANES * cx) % (2 * LANES)
    wide_in[...] = jnp.where(mine(r) == cell(c), 1.0, 0.0).astype(F32)
    wide_nat[...] = jnp.where(r == cell(c), 1.0, 0.0).astype(F32)
    wide_out[...] = jnp.where(cell(r) == mine(c), 1.0, 0.0).astype(F32)
    pl.semaphore_wait(barrier, total - 1)

    def across(c, lv):
        if lv.parts > 1:
            even, odd = c
            return [odd + from_below(odd), even + from_above(even)]
        if lv.nx == LANES:
            return [from_below(c[0]) + from_above(c[0])]
        return [roll(c[0], 1) + roll(c[0], LANES - 1)]

    def neighbours(src, p, xm, c, xp, lv, top, n):
        zm, zp = get(src, p, pl.ds(top - 1, n), lv), get(src, p, pl.ds(top + 1, n), lv)
        return every(lambda a, b, d, e, f: ((a + b) + (d + e)) + f, xm, xp, zm, zp, across(c, lv))

    def table_rows(table, k, lv, top, n):
        return table[k, pl.ds(top - lv.top, n)]

    def sweep(src, dst, rhs_ref, lv, table, scale=None):
        @pl.loop(0, lv.count)
        def _(g):
            base = lv.begin + g * lv.group
            for top, n in lv.blocks:
                rows = pl.ds(top, n)
                xm, c = get(src, base - 1, rows, lv), get(src, base, rows, lv)
                for j in range(lv.group):
                    p = base + j
                    xp = get(src, p + 1, rows, lv)
                    t = every(lambda a, b: a + 3.0 * b, neighbours(src, p, xm, c, xp, lv, top, n), c)
                    if scale is not None:
                        t = [x * scale for x in t]
                    keep = table_rows(table, 2 * valid(lv, p), lv, top, n)
                    put(dst, p, rows, every(lambda a, b: (a + b) * keep, t, get(rhs_ref, p, rows, lv)))
                    xm, c = c, xp

    def first_sweep(dst, rhs_ref, lv, table):
        @pl.loop(0, lv.count)
        def _(g):
            for j in range(lv.group):
                p = lv.begin + g * lv.group + j
                dst[p, 0, lv.all] = rhs_ref[p, 0, lv.all] * table[2 * valid(lv, p)]

    def restrict_planes(src, rhs_ref, lv, table, group):
        def res(p, xm, c, xp, top, n):
            return every(lambda a, b, d: a + b - 6.0 * d, neighbours(src, p, xm, c, xp, lv, top, n), get(rhs_ref, p, pl.ds(top, n), lv), c)

        @pl.loop(0, lv.ny // 2 // group)
        def _(i):
            for top, n in lv.blocks:
                rows = pl.ds(top, n)
                p = lv.hx + 2 * group * i
                xm, c = get(src, p - 1, rows, lv), get(src, p, rows, lv)
                prev = res(p - 1, get(src, p - 2, rows, lv), xm, c, top, n)
                prev = [jnp.where((yb > 0) | (i > 0), x, 0.0) for x in prev]
                keep = table_rows(table, 1, lv, top, n)
                for j in range(group):
                    x1, x2 = get(src, p + 1, rows, lv), get(src, p + 2, rows, lv)
                    even = res(p, xm, c, x1, top, n)
                    odd = res(p + 1, c, x1, x2, top, n)
                    for h in range(lv.parts):
                        pb[h, i * group + j, rows] = ((prev[h] + odd[h]) + (even[h] + even[h])) * keep
                    prev, xm, c, p = odd, x1, x2, p + 2

    def restricted_rows(i, lv, h=0):
        half = lv.nz // 2
        return ((pb[h, i, pl.ds(lv.z0 - 1, half, stride=2)] + pb[h, i, pl.ds(lv.z0 + 1, half, stride=2)])
                + 2.0 * pb[h, i, pl.ds(lv.z0, half, stride=2)])

    def weights(near, one, other):
        return jnp.where(near == 0, one, jnp.where((near == 1) | (near == -1), other, 0.0)).astype(F32)

    square = (LANES, LANES)
    eighth = 1.0 / (TILE * TILE)

    def restrict_level(src, rhs_ref, lv, table, coarse_rhs, coarse, group, step):
        restrict_planes(src, rhs_ref, lv, table, group)
        lane = lanes_of(square)
        w = jnp.where(lane < coarse.nx, weights(rows_of(square) - 2 * lane, 2.0 * eighth, eighth), 0.0)

        @pl.loop(0, coarse.ny // step)
        def _(i):
            got = [restricted_rows(i * step + j, lv) for j in range(step)]
            if lv.parts > 1:
                odds = [restricted_rows(i * step + j, lv, 1) for j in range(step)]
                got = [((odd + from_below(odd)) + 2.0 * even) * eighth for even, odd in zip(got, odds)]
            else:
                got = dot(stack(got), w)
                got = [got[j * coarse.nz:(j + 1) * coarse.nz] for j in range(step)]
            for j in range(step):
                coarse_rhs[coarse.hx + i * step + j, 0, coarse.own] = got[j]

    def prolong_planes(e, first, e_z0, e_top, e_rows, e_nx, chunk, n_chunks, lv):
        lane, below = lanes_of(square), rows_of(square)
        w = jnp.where(below < e_nx, weights(lane - 2 * below, 4.0, 2.0), 0.0)
        row = e_z0 - e_top - (lv.z0 - lv.top) // 2
        n = lv.rows // 2

        @pl.loop(0, n_chunks)
        def _(i):
            planes = pl.ds(first + i * chunk, chunk)
            got = e[planes, 0, pl.ds(e_top, e_rows)]
            if lv.parts == 1:
                got = dot(got.reshape(chunk * e_rows, LANES), w).reshape(chunk, e_rows, LANES)
            else:
                got = got * 4.0
            pz[pl.ds(i * chunk, chunk), pl.ds(0, e_rows)] = got

        @pl.loop(0, n_chunks)
        def _(i):
            for j in range(chunk):
                a = pz[i * chunk + j, pl.ds(row, n)]
                b = pz[i * chunk + j, pl.ds(row + 1, n)]
                pb[0, i * chunk + j, pl.ds(lv.top, n, stride=2)] = a
                pb[0, i * chunk + j, pl.ds(lv.top + 1, n, stride=2)] = 0.5 * (a + b)

    def correct(dst, lv, table, pairs):
        def load(at, rows):
            a = pb[0, at, rows]
            return [a, 0.5 * (a + from_above(a))] if lv.parts > 1 else [a]

        @pl.loop(0, lv.group * lv.count // (2 * pairs))
        def _(i):
            for top, n in lv.blocks:
                rows = pl.ds(top, n)
                a = load(i * pairs, rows)
                for j in range(pairs):
                    b = load(i * pairs + j + 1, rows)
                    p = lv.begin + 2 * (pairs * i + j)
                    between = every(lambda x, y: 0.5 * (x + y), a, b)
                    for q, add in ((p, a), (p + 1, between)):
                        keep = table_rows(table, valid(lv, q), lv, top, n)
                        put(dst, q, rows, every(lambda x, y: (x + y) * keep, get(dst, q, rows, lv), add))
                    a = b

    partner, row_halo, halo = partner_copies(), row_copies(), fine_copies()
    for copy in loads:
        copy.wait()
    begin(row_halo)
    for copy in partner:
        copy.start()
    half = TILE // 2
    upper = rows_of((TILE, LANES)) >= half

    @pl.loop(0, chip_y // TILE)
    def _(i):
        for j in range(TILE):
            y = i * TILE + j
            for side, row in enumerate((TILE, TILE + l0.nz - half)):
                send_z[side, y] = jnp.where(upper, stage_f[y, pl.ds(row - half, TILE)], stage_u[y, pl.ds(row, TILE)])
    begin(halo)

    step = 2
    for copy in partner:
        copy.wait_recv()
    for stage, buf, dst in ((stage_u, part_u, u0), (stage_f, part_f, f0)):
        @pl.loop(0, reach // step)
        def _(i, stage=stage, buf=buf, dst=dst):
            planes = pl.ds(cx * (chip_y - reach) + i * step, step)
            mine_, theirs = stage[planes, inner], buf[pl.ds(i * step, step)]
            got = dot(join(mine_.reshape(step * l0.nz, LANES), theirs.reshape(step * l0.nz, LANES)), wide_in[...])
            put(dst, pl.ds(l0.hx - cx * l0.wide + i * step, step), l0.own, [x.reshape(step, l0.nz, LANES) for x in halves(got)])
    arrive(row_halo)
    arrive(halo)
    finish(row_halo)
    finish(halo)
    for copy in partner:
        copy.wait_send()
    outer_plane = l0.hx - l0.wide + cx * reach

    def together(buf, at, n):
        return join(buf[0, at].reshape(n, LANES), buf[1, at].reshape(n, LANES))
    for buf, dst in ((recv_yu, u0), (recv_yf, f0)):
        @pl.loop(0, l0.wide // step)
        def _(i, buf=buf, dst=dst):
            got = dot(together(buf, pl.ds(i * step, step), step * l0.nz), wide_nat[...])
            put(dst, pl.ds(outer_plane + i * step, step), l0.own, [x.reshape(step, l0.nz, LANES) for x in halves(got)])

    def put_rows(p, side, tile):
        row = l0.z0 + l0.nz if side else l0.z0 - half
        for h, part in enumerate(halves(tile)):
            pltpu.store(u0.at[p, h, pl.ds(row, TILE)], part, mask=jnp.logical_not(upper))
            pltpu.store(f0.at[p, h, pl.ds(row - half, TILE)], part, mask=upper)
    some = reach // 3
    for side in range(2):
        @pl.loop(0, reach // some)
        def _(i, side=side):
            got = dot(together(recv_z.at[side], pl.ds(i * some, some), some * TILE), wide_nat[...])
            for j in range(some):
                put_rows(l0.hx - cx * l0.wide + i * some + j, side, got[j * TILE:(j + 1) * TILE])
        got = dot(together(recv_d.at[side], pl.ds(0, l0.wide), l0.wide * TILE), wide_nat[...])
        for j in range(l0.wide):
            put_rows(outer_plane + j, side, got[j * TILE:(j + 1) * TILE])
    sweep(u0, v0, f0, l0, mask0, cfg.stiffness)
    sweep(v0, u0, f0, l0, mask0)
    restrict_level(u0, f0, l0, mask0, g1, l1, 4, 4)

    exchange(1)
    first_sweep(a1, g1, l1, mask1)
    sweep(a1, b1, g1, l1, mask1)
    restrict_level(b1, g1, l1, mask1, g2, l2, 8, 8)
    exchange(2)
    first_sweep(a2, g2, l2, mask2)
    sweep(a2, b2, g2, l2, mask2)

    restrict_planes(b2, g2, l2, mask2, 4)
    ny3, nz3, width = l2.ny // 2, l2.nz // 2, l2.nx // 2
    near = rows_of(square) - 2 * (lanes_of(square) % width)
    got = dot(stack([restricted_rows(j, l2) for j in range(ny3)]), weights(near, 2.0 * eighth, eighth))
    tile = (TILE, LANES)
    lane = lanes_of(tile)
    block = lane // width
    blocks = LANES // width
    packed = got[:nz3]
    for j in range(1, ny3):
        packed = jnp.where(block == j, got[j * nz3:(j + 1) * nz3], packed)
    packed = roll(packed, width * cz)
    message[...] = packed
    slot = yb * n_z + cz
    slots[slot] = packed

    def gather_copy(p, at):
        return pltpu.make_async_remote_copy(
            src_ref=message, dst_ref=slots.at[at], send_sem=all_s.at[p], recv_sem=all_r.at[at], device_id=peer(p), device_id_type=MESH)

    @pl.loop(1, total)
    def _(p):
        gather_copy(p, slot).start()

    @pl.loop(1, total)
    def _(p):
        who = peer(p)
        gather_copy(p, (who['sy'] * n_x + who['sx']) * n_z + who['sz']).wait_recv()

    data = pl.ds(TILE, TILE)
    whole = row_blocks * ny3
    for s in range(2):
        @pl.loop(0, TILE)
        def _(i, s=s):
            for at in (i, TILE + whole + i):
                s3[s, at, data] = jnp.zeros(tile, F32)
    live = lane < width * n_z

    @pl.loop(0, row_blocks)
    def _(part):
        for j in range(ny3):
            acc = jnp.zeros(tile, F32)
            for t in range(n_z):
                acc = jnp.where((block + 2 * blocks - t - j) % blocks == 0, slots[part * n_z + t], acc)
            acc = jnp.where(live, roll(acc, back(width * j)), 0.0)
            g3[part * ny3 + j] = acc
            s3[0, TILE + part * ny3 + j, data] = acc * NINTH

    row = rows_of(tile)
    x_first, x_last = lane % width == 0, lane % width == width - 1
    top, bottom = row == 0, row == TILE - 1
    z_first, z_last = lane < width, lane >= width * (n_z - 1)

    def coarse_sweep(k, carry):
        old, new = k % 2, (k + 1) % 2
        xm, c = s3[old, TILE - 1, data], s3[old, TILE, data]
        for y in range(whole):
            at = TILE + y
            xp = s3[old, at + 1, data]
            above = jnp.where(z_first, 0.0, roll(s3[old, at, pl.ds(2 * TILE - 1, TILE)], width % LANES))
            below = jnp.where(z_last, 0.0, roll(s3[old, at, pl.ds(1, TILE)], back(width)))
            zm = jnp.where(top, above, s3[old, at, pl.ds(TILE - 1, TILE)])
            zp = jnp.where(bottom, below, s3[old, at, pl.ds(TILE + 1, TILE)])
            left = jnp.where(x_first, 0.0, roll(c, 1))
            right = jnp.where(x_last, 0.0, roll(c, LANES - 1))
            t = (xm + xp) + (zm + zp) + (left + right) + 3.0 * c + g3[y]
            s3[new, at, data] = t * NINTH
            xm, c = c, xp
        return carry
    lax.fori_loop(0, COARSE_SWEEPS - 1, coarse_sweep, 0)

    first = (l2.begin - l2.hx) // 2
    for i in range(e3.shape[0]):
        c = s3[(COARSE_SWEEPS - 1) % 2, yb * ny3 + (TILE + i + first), data]
        for k in range(3):
            ok = (lane < width) & (cz + k > 0) & (cz + k < n_z + 1)
            e3[i, 0, pl.ds(TILE * k, TILE)] = jnp.where(ok, roll(c, back((cz + k) * width + LANES - width)), 0.0)

    prolong_planes(e3, 0, TILE, 0, 3 * TILE, width, 6, 2, l2)
    correct(b2, l2, mask2, 5)
    sweep(b2, a2, g2, l2, mask2)
    sweep(a2, b2, g2, l2, mask2)
    prolong_planes(b2, l2.hx + (l1.begin - l1.hx) // 2, l2.z0, l2.top, l2.rows, l2.nx, 8, 2, l1)
    correct(b1, l1, mask1, 7)
    sweep(b1, a1, g1, l1, mask1)
    sweep(a1, b1, g1, l1, mask1)
    prolong_planes(b1, l1.hx + (l0.begin - l0.hx) // 2, l1.z0, l1.top, l1.rows, l1.nx, 8, 3, l0)
    correct(u0, l0, mask0, 4)
    sweep(u0, v0, f0, l0, mask0)

    def results(i):
        here, there = pl.ds(i * step, step), pl.ds(cx * l0.ny + i * step, step)
        return (pltpu.make_async_copy(stage_u.at[here, inner], out.at[there], out_sem.at[0, i]),
                pltpu.make_async_remote_copy(
                    src_ref=stage_f.at[here, inner], dst_ref=out.at[there], send_sem=out_sem.at[1, i], recv_sem=out_sem.at[2, i],
                    device_id={'sx': 1 - cx}, device_id_type=MESH))

    @pl.loop(0, l0.ny // step)
    def _(i):
        got = []
        for j in range(step):
            p = l0.hx + i * step + j
            c = get(v0, p, l0.own, l0)
            around = neighbours(v0, p, get(v0, p - 1, l0.own, l0), c, get(v0, p + 1, l0.own, l0), l0, l0.z0, l0.nz)
            got.append(join(*every(lambda x, y, g: x + 3.0 * y + g, around, c, get(f0, p, l0.own, l0))))
        mine_, theirs = halves(dot(stack(got) * (NINTH / cfg.stiffness), wide_out[...]))
        here = pl.ds(i * step, step)
        stage_u[here, inner] = mine_.reshape(step, l0.nz, LANES)
        stage_f[here, inner] = theirs.reshape(step, l0.nz, LANES)
        for copy in results(i):
            copy.start()

    @pl.loop(0, l0.ny // step)
    def _(i):
        local, remote = results(i)
        local.wait()
        remote.wait()
    drain(1)
    drain(2)

    @pl.loop(1, total)
    def _(p):
        gather_copy(p, slot).wait_send()


def local_cycle(rhs, start, counts, size):
    rhs, start = (jnp.transpose(x, (1, 2, 0)) for x in (rhs, start))
    n_x, n_y, n_z = counts
    chip_y, nz, nx = rhs.shape
    shapes = [(chip_y // n_x >> k, nz >> k, nx * n_x >> k) for k in range(3)]
    l0 = make_level(shapes[0], 6, 8, 4, nz + 8, 2, 8, (shapes[0][0] + 8) // 8, 4, 24)
    l1 = make_level(shapes[1], 8, 16, 8, shapes[1][1] + 16, 2, 14, (shapes[1][0] + 12) // 14, 5, 24)
    l2 = make_level(shapes[2], 8, 16, 8, shapes[2][1] + 16, 2, 10, (shapes[2][0] + 12) // 10, 6, 32)
    cfg = types.SimpleNamespace(levels=(l0, l1, l2), counts=counts, stiffness=float((size + 1) ** 2))
    total = n_x * n_y * n_z

    def vmem(*shape):
        return pltpu.VMEM(shape, F32)

    scratch = [vmem(lv.planes, lv.parts, lv.depth, LANES) for lv in (l0, l1, l2) for _ in range(3)]
    whole = n_x * n_y * (l2.ny // 2)
    reach = l0.ny + l0.wide
    scratch += [vmem(12, 1, 3 * TILE, LANES), vmem(l1.ny + 8, l1.rows, LANES), vmem(2, l1.ny + 8, l0.depth, LANES)]
    scratch += [vmem(chip_y, l0.depth, LANES)] * 2 + [vmem(reach, nz, LANES)] * 2
    scratch += [vmem(2, whole + 2 * TILE, 3 * TILE, LANES), vmem(whole, TILE, LANES), vmem(total, TILE, LANES), vmem(TILE, LANES)]
    scratch += [vmem(3, lv.rows, LANES) for lv in (l0, l1, l2)]
    scratch += [vmem(2, chip_y, TILE, LANES), vmem(2, n_x, reach, TILE, LANES), vmem(2, 2, l0.wide, TILE, LANES)]
    scratch += [vmem(2, l0.wide, nz, LANES)] * 2 + [vmem(2 * LANES, 2 * LANES)] * 3
    sems = [(2,), (3, l0.ny // 2), (16,), (16,), (2, len(SIDES)), (2, len(SIDES)), (total,), (total,)]
    scratch += [pltpu.SemaphoreType.DMA(shape) for shape in sems]
    got = pl.pallas_call(
        functools.partial(kernel, cfg),
        out_shape=jax.ShapeDtypeStruct(rhs.shape, F32),
        in_specs=[pl.BlockSpec(memory_space=pl.ANY)] * 2,
        out_specs=pl.BlockSpec(memory_space=pl.ANY),
        scratch_shapes=scratch,
        compiler_params=pltpu.CompilerParams(collective_id=0, has_side_effects=True, vmem_limit_bytes=60 * 2 ** 20),
    )(rhs, start)
    return jnp.transpose(got, (2, 0, 1))


def solution(mesh):
    counts = (mesh.shape['sx'], mesh.shape['sy'], mesh.shape['sz'])
    spec = P(('dp', 'sx'), 'sy', 'sz')

    def run(rhs_grid, u_start):
        size = rhs_grid.shape[0] // mesh.shape['dp']
        cycle = functools.partial(local_cycle, counts=counts, size=size)
        return jax.shard_map(cycle, mesh=mesh, in_specs=(spec, spec), out_specs=spec, check_vma=False)(rhs_grid, u_start)
    return run
```

```python
import functools
import types
import jax
import jax.numpy as jnp
from jax import lax
from jax.experimental import pallas as pl
from jax.experimental.pallas import tpu as pltpu
from jax.sharding import PartitionSpec as P

F32 = jnp.float32
MESH = pl.DeviceIdType.MESH
LANES = 128
TILE = 8
NINTH = 1.0 / 9.0
COARSE_SWEEPS = 16
OPPOSITE = (1, 0, 3, 2, 7, 6, 5, 4)
STEP_Y = (-1, 1, 0, 0, -1, -1, 1, 1)
STEP_Z = (0, 0, -1, 1, -1, 1, -1, 1)
SIDES = range(len(STEP_Y))


def make_level(shape, hx, z0, top, rows, begin, group, count, wide, block):
    ny, nz, nx = shape
    lv = types.SimpleNamespace(ny=ny, nz=nz, nx=nx, hx=hx, z0=z0, top=top, rows=rows, begin=begin, group=group, count=count, wide=wide)
    lv.planes = ny + 2 * hx
    lv.depth = nz + 2 * z0
    lv.parts = max(nx // LANES, 1)
    lv.own = pl.ds(z0, nz)
    lv.all = pl.ds(top, rows)
    lv.blocks = [(top + i, min(block, rows - i)) for i in range(0, rows, block)]
    return lv


def lanes_of(shape):
    return lax.broadcasted_iota(jnp.int32, shape, len(shape) - 1)


def rows_of(shape):
    return lax.broadcasted_iota(jnp.int32, shape, len(shape) - 2)


def roll(x, shift):
    return pltpu.roll(x, shift, 1)


def from_below(x):
    return jnp.where(lanes_of(x.shape) == 0, 0.0, roll(x, 1))


def from_above(x):
    return jnp.where(lanes_of(x.shape) == LANES - 1, 0.0, roll(x, LANES - 1))


def halves(x):
    return x[:, :LANES], x[:, LANES:]


def get(ref, p, rows, lv):
    return [ref[p, h, rows] for h in range(lv.parts)]


def put(ref, p, rows, values):
    for h, value in enumerate(values):
        ref[p, h, rows] = value


def every(f, *lists):
    return [f(*values) for values in zip(*lists)]


def join(*parts):
    return jnp.concatenate(parts, axis=1)


def stack(parts):
    return jnp.concatenate(parts, axis=0)


def back(shift):
    return (4 * LANES - shift) % LANES


def flag(condition):
    return jnp.where(condition, 1, 0)


def pick(x, index):
    return jnp.take_along_axis(x, index, axis=1, mode='promise_in_bounds')


def dot(x, w):
    return jnp.dot(x, w, precision=lax.Precision.HIGHEST, preferred_element_type=F32)


def kernel(cfg, rhs, start, out, *scratch):
    (u0, v0, f0, a1, b1, g1, a2, b2, g2, e3, pz, pb, stage_u, stage_f, part_u, part_f, s3, g3, slots, message, mask0, mask1, mask2,
     send_z, recv_z, recv_d, recv_yu, recv_yf,
     load_sem, out_sem, fine_s, fine_r, send_sem, recv_sem, all_s, all_r) = scratch
    l0, l1, l2 = levels = cfg.levels
    masks = (mask0, mask1, mask2)
    n_x, n_y, n_z = cfg.counts
    cx, cy, cz = lax.axis_index('sx'), lax.axis_index('sy'), lax.axis_index('sz')
    total = n_x * n_y * n_z
    row_blocks = n_x * n_y
    yb = cy * n_x + cx

    inner = pl.ds(TILE, l0.nz)
    loads = [pltpu.make_async_copy(src, dst.at[:, inner], load_sem.at[k]) for k, (src, dst) in enumerate(((start, stage_u), (rhs, stage_f)))]
    for copy in loads:
        copy.start()

    offsets = [(dz, dy, dx) for dz in range(n_z) for dy in range(n_y) for dx in range(n_x)][1:]

    def peer(offset):
        return {name: lax.rem(at + d, n) for name, at, n, d in zip(('sz', 'sy', 'sx'), (cz, cy, cx), (n_z, n_y, n_x), offset)}

    barrier = pltpu.get_barrier_semaphore()
    for offset in offsets:
        pl.semaphore_signal(barrier, inc=1, device_id=peer(offset), device_id_type=MESH)

    def inside(step, at, count):
        if step == 0:
            return True
        return at > 0 if step < 0 else at < count - 1

    def exists(d):
        return jnp.logical_and(inside(STEP_Y[d], yb, row_blocks), inside(STEP_Z[d], cz, n_z))

    def zero(ref):
        @pl.loop(0, ref.shape[0])
        def _(i):
            ref[i] = jnp.zeros(ref.shape[1:], F32)

    def span(step, first, n, wide, own):
        if step == 0:
            return pl.ds(first, n)
        if step < 0:
            return pl.ds(first if own else first - wide, wide)
        return pl.ds(first + n - wide if own else first + n, wide)

    def region(index, d, own):
        lv, arr = levels[index], (None, g1, g2)[index]
        return arr.at[span(STEP_Y[d], lv.hx, lv.ny, lv.wide, own), 0, span(STEP_Z[d], lv.z0, lv.nz, TILE, own)]

    def halo_copy(index, d, arriving):
        k = index - 1
        at = yb + STEP_Y[d]
        return pltpu.make_async_remote_copy(
            src_ref=region(index, d, not arriving), dst_ref=region(index, d if arriving else OPPOSITE[d], False),
            send_sem=send_sem.at[k, d], recv_sem=recv_sem.at[k, d if arriving else OPPOSITE[d]],
            device_id={'sx': at % n_x, 'sy': at // n_x, 'sz': cz + STEP_Z[d]}, device_id_type=MESH)

    def each(act):
        for d in (4, 5, 6, 7, 2, 3, 0, 1):
            @pl.when(exists(d))
            def _(d=d):
                act(d)

    def exchange(index):
        each(lambda d: halo_copy(index, d, False).start())
        each(lambda d: halo_copy(index, d, True).wait_recv())

    def drain(index):
        each(lambda d: halo_copy(index, d, False).wait_send())

    chip_y = n_x * l0.ny
    reach = l0.ny + l0.wide
    outer = 2 * cx - 1

    def fine_copies():
        got = []

        def add(sends, arrives, src, dst, arrival, k, theirs, **to):
            made = [pltpu.make_async_remote_copy(
                src_ref=a, dst_ref=b, send_sem=fine_s.at[k], recv_sem=fine_r.at[r], device_id=to, device_id_type=MESH)
                for a, b, r in ((src, dst, theirs[0]), (arrival, arrival, theirs[1]))]
            got.append((sends, arrives, *made))
        n = 0
        for z_side, z_step in enumerate((-1, 1)):
            for y_side, y_step in enumerate((-1, 1)):
                edge = pl.ds(0 if y_step < 0 else chip_y - l0.wide, l0.wide)
                to_z = jnp.logical_and(inside(y_step, cy, n_y), inside(z_step, cz, n_z))
                in_z = jnp.logical_and(jnp.logical_and((cy + outer >= 0) & (cy + outer < n_y), inside(z_step, cz, n_z)), True)
                add(to_z, in_z, send_z.at[z_side, edge], recv_d.at[1 - z_side, cx], recv_d.at[z_side, y_side], n,
                    (8 + 2 * (1 - z_side) + cx, 8 + 2 * z_side + y_side), sx=1 - y_side, sy=cy + y_step, sz=cz + z_step)
                n += 1
        for z_side, z_step in enumerate((-1, 1)):
            for core in range(n_x):
                there = inside(z_step, cz, n_z)
                add(there, there, send_z.at[z_side, pl.ds(core * (chip_y - reach), reach)], recv_z.at[1 - z_side, cx],
                    recv_z.at[z_side, core], n, (12 + 2 * (1 - z_side) + cx, 12 + 2 * z_side + core), sx=core, sz=cz + z_step)
                n += 1
        return got

    def row_copies():
        got = []
        here = (cy + outer >= 0) & (cy + outer < n_y)
        for y_side, y_step in enumerate((-1, 1)):
            edge = pl.ds(0 if y_step < 0 else chip_y - l0.wide, l0.wide)
            for k, (stage, buf) in enumerate(((stage_u, recv_yu), (stage_f, recv_yf))):
                made = [pltpu.make_async_remote_copy(
                    src_ref=a, dst_ref=b, send_sem=fine_s.at[8 + 2 * y_side + k], recv_sem=fine_r.at[2 * r + k],
                    device_id={'sx': 1 - y_side, 'sy': cy + y_step}, device_id_type=MESH)
                    for a, b, r in ((stage.at[edge, inner], buf.at[cx], cx), (buf.at[y_side], buf.at[y_side], y_side))]
                got.append((inside(y_step, cy, n_y), here, *made))
        return got

    def partner_copies():
        other = pl.ds((1 - cx) * (chip_y - reach), reach)
        return [pltpu.make_async_remote_copy(
            src_ref=stage.at[other, inner], dst_ref=buf, send_sem=fine_s.at[12 + k], recv_sem=fine_r.at[4 + k],
            device_id={'sx': 1 - cx}, device_id_type=MESH) for k, (stage, buf) in enumerate(((stage_u, part_u), (stage_f, part_f)))]

    def begin(copies):
        for sends, _, copy, _ in copies:
            @pl.when(sends)
            def _(copy=copy):
                copy.start()

    def arrive(copies):
        for _, arrives, _, copy in copies:
            @pl.when(arrives)
            def _(copy=copy):
                copy.wait_recv()

    def finish(copies):
        for sends, _, copy, _ in copies:
            @pl.when(sends)
            def _(copy=copy):
                copy.wait_send()

    @pl.when(jnp.logical_not((cy + outer >= 0) & (cy + outer < n_y)))
    def _():
        for buf in (recv_yu, recv_yf, recv_d):
            for k in range(2):
                zero(buf.at[k])
    for z_side, z_step in enumerate((-1, 1)):
        @pl.when(jnp.logical_not(inside(z_step, cz, n_z)))
        def _(z_side=z_side):
            for core in range(n_x):
                zero(recv_z.at[z_side, core])
            zero(recv_d.at[z_side])
    for index in (1, 2):
        for d in SIDES:
            @pl.when(jnp.logical_not(exists(d)))
            def _(index=index, d=d):
                zero(region(index, d, False))

    for lv, arrays in ((l0, (u0, v0)), (l1, (a1, b1)), (l2, (a2, b2))):
        for arr in arrays:
            for plane, outside in ((lv.hx - 1, yb == 0), (lv.hx + lv.ny, yb == row_blocks - 1)):
                @pl.when(outside)
                def _(arr=arr, lv=lv, plane=plane):
                    put(arr, plane, lv.all, [jnp.zeros((lv.rows, LANES), F32)] * lv.parts)

    for lv, table in zip(levels, masks):
        shape = (lv.rows, LANES)
        z = rows_of(shape) + (lv.top - lv.z0) + cz * lv.nz
        ok = (z >= 0) & (z < n_z * lv.nz) & (lanes_of(shape) < lv.nx)
        table[0] = jnp.zeros(shape, F32)
        table[1] = jnp.where(ok, 1.0, 0.0).astype(F32)
        table[2] = jnp.where(ok, NINTH, 0.0).astype(F32)

    def valid(lv, p):
        y = p + (yb * lv.ny - lv.hx)
        return flag((y >= 0) & (y < row_blocks * lv.ny))

    middle = LANES // 2

    def lower(shape, core):
        return lanes_of(shape) // middle == core

    def split_x(first, second, core):
        lane = lanes_of(first.shape)
        pair = 2 * (lane % middle)
        first, second = pick(first, pair + (lane // middle + core) % 2), pick(second, pair + (lane // middle + 1 - core) % 2)
        here = lower(first.shape, core)
        return [jnp.where(here, first, second), roll(jnp.where(here, second, first), middle)]

    def merge_x(even, odd, core):
        lane = lanes_of(even.shape)
        odd = roll(odd, middle)
        here = lower(even.shape, core)
        spot = lane // 2 + middle * ((lane + core) % 2)
        return pick(jnp.where(here, even, odd), spot), pick(jnp.where(here, odd, even), (spot + middle) % LANES)
    pl.semaphore_wait(barrier, total - 1)

    def across(c, lv):
        if lv.parts > 1:
            even, odd = c
            return [odd + from_below(odd), even + from_above(even)]
        if lv.nx == LANES:
            return [from_below(c[0]) + from_above(c[0])]
        return [roll(c[0], 1) + roll(c[0], LANES - 1)]

    def neighbours(src, p, xm, c, xp, lv, top, n):
        zm, zp = get(src, p, pl.ds(top - 1, n), lv), get(src, p, pl.ds(top + 1, n), lv)
        return every(lambda a, b, d, e, f: ((a + b) + (d + e)) + f, xm, xp, zm, zp, across(c, lv))

    def table_rows(table, k, lv, top, n):
        return table[k, pl.ds(top - lv.top, n)]

    def sweep(src, dst, rhs_ref, lv, table, scale=None):
        @pl.loop(0, lv.count)
        def _(g):
            base = lv.begin + g * lv.group
            for top, n in lv.blocks:
                rows = pl.ds(top, n)
                xm, c = get(src, base - 1, rows, lv), get(src, base, rows, lv)
                for j in range(lv.group):
                    p = base + j
                    xp = get(src, p + 1, rows, lv)
                    t = every(lambda a, b: a + 3.0 * b, neighbours(src, p, xm, c, xp, lv, top, n), c)
                    if scale is not None:
                        t = [x * scale for x in t]
                    keep = table_rows(table, 2 * valid(lv, p), lv, top, n)
                    put(dst, p, rows, every(lambda a, b: (a + b) * keep, t, get(rhs_ref, p, rows, lv)))
                    xm, c = c, xp

    def first_sweep(dst, rhs_ref, lv, table):
        @pl.loop(0, lv.count)
        def _(g):
            for j in range(lv.group):
                p = lv.begin + g * lv.group + j
                dst[p, 0, lv.all] = rhs_ref[p, 0, lv.all] * table[2 * valid(lv, p)]

    def restrict_planes(src, rhs_ref, lv, table, group):
        def res(p, xm, c, xp, top, n):
            return every(lambda a, b, d: a + b - 6.0 * d, neighbours(src, p, xm, c, xp, lv, top, n), get(rhs_ref, p, pl.ds(top, n), lv), c)

        @pl.loop(0, lv.ny // 2 // group)
        def _(i):
            for top, n in lv.blocks:
                rows = pl.ds(top, n)
                p = lv.hx + 2 * group * i
                xm, c = get(src, p - 1, rows, lv), get(src, p, rows, lv)
                prev = res(p - 1, get(src, p - 2, rows, lv), xm, c, top, n)
                prev = [jnp.where((yb > 0) | (i > 0), x, 0.0) for x in prev]
                keep = table_rows(table, 1, lv, top, n)
                for j in range(group):
                    x1, x2 = get(src, p + 1, rows, lv), get(src, p + 2, rows, lv)
                    even = res(p, xm, c, x1, top, n)
                    odd = res(p + 1, c, x1, x2, top, n)
                    for h in range(lv.parts):
                        pb[h, i * group + j, rows] = ((prev[h] + odd[h]) + (even[h] + even[h])) * keep
                    prev, xm, c, p = odd, x1, x2, p + 2

    def restricted_rows(i, lv, h=0):
        half = lv.nz // 2
        return ((pb[h, i, pl.ds(lv.z0 - 1, half, stride=2)] + pb[h, i, pl.ds(lv.z0 + 1, half, stride=2)])
                + 2.0 * pb[h, i, pl.ds(lv.z0, half, stride=2)])

    def weights(near, one, other):
        return jnp.where(near == 0, one, jnp.where((near == 1) | (near == -1), other, 0.0)).astype(F32)

    square = (LANES, LANES)
    eighth = 1.0 / (TILE * TILE)

    def restrict_level(src, rhs_ref, lv, table, coarse_rhs, coarse, group, step):
        restrict_planes(src, rhs_ref, lv, table, group)
        lane = lanes_of(square)
        w = jnp.where(lane < coarse.nx, weights(rows_of(square) - 2 * lane, 2.0 * eighth, eighth), 0.0)

        @pl.loop(0, coarse.ny // step)
        def _(i):
            got = [restricted_rows(i * step + j, lv) for j in range(step)]
            if lv.parts > 1:
                odds = [restricted_rows(i * step + j, lv, 1) for j in range(step)]
                got = [((odd + from_below(odd)) + 2.0 * even) * eighth for even, odd in zip(got, odds)]
            else:
                got = dot(stack(got), w)
                got = [got[j * coarse.nz:(j + 1) * coarse.nz] for j in range(step)]
            for j in range(step):
                coarse_rhs[coarse.hx + i * step + j, 0, coarse.own] = got[j]

    def prolong_planes(e, first, e_z0, e_top, e_rows, e_nx, chunk, n_chunks, lv):
        lane, below = lanes_of(square), rows_of(square)
        w = jnp.where(below < e_nx, weights(lane - 2 * below, 4.0, 2.0), 0.0)
        row = e_z0 - e_top - (lv.z0 - lv.top) // 2
        n = lv.rows // 2

        @pl.loop(0, n_chunks)
        def _(i):
            planes = pl.ds(first + i * chunk, chunk)
            got = e[planes, 0, pl.ds(e_top, e_rows)]
            if lv.parts == 1:
                got = dot(got.reshape(chunk * e_rows, LANES), w).reshape(chunk, e_rows, LANES)
            else:
                got = got * 4.0
            pz[pl.ds(i * chunk, chunk), pl.ds(0, e_rows)] = got

        @pl.loop(0, n_chunks)
        def _(i):
            for j in range(chunk):
                a = pz[i * chunk + j, pl.ds(row, n)]
                b = pz[i * chunk + j, pl.ds(row + 1, n)]
                pb[0, i * chunk + j, pl.ds(lv.top, n, stride=2)] = a
                pb[0, i * chunk + j, pl.ds(lv.top + 1, n, stride=2)] = 0.5 * (a + b)

    def correct(dst, lv, table, pairs):
        def load(at, rows):
            a = pb[0, at, rows]
            return [a, 0.5 * (a + from_above(a))] if lv.parts > 1 else [a]

        @pl.loop(0, lv.group * lv.count // (2 * pairs))
        def _(i):
            for top, n in lv.blocks:
                rows = pl.ds(top, n)
                a = load(i * pairs, rows)
                for j in range(pairs):
                    b = load(i * pairs + j + 1, rows)
                    p = lv.begin + 2 * (pairs * i + j)
                    between = every(lambda x, y: 0.5 * (x + y), a, b)
                    for q, add in ((p, a), (p + 1, between)):
                        keep = table_rows(table, valid(lv, q), lv, top, n)
                        put(dst, q, rows, every(lambda x, y: (x + y) * keep, get(dst, q, rows, lv), add))
                    a = b

    partner, row_halo, halo = partner_copies(), row_copies(), fine_copies()
    for copy in loads:
        copy.wait()
    begin(row_halo)
    for copy in partner:
        copy.start()
    half = TILE // 2
    upper = rows_of((TILE, LANES)) >= half

    @pl.loop(0, chip_y // TILE)
    def _(i):
        for j in range(TILE):
            y = i * TILE + j
            for side, row in enumerate((TILE, TILE + l0.nz - half)):
                send_z[side, y] = jnp.where(upper, stage_f[y, pl.ds(row - half, TILE)], stage_u[y, pl.ds(row, TILE)])
    begin(halo)

    step = 4
    for copy in partner:
        copy.wait_recv()
    for stage, buf, dst in ((stage_u, part_u, u0), (stage_f, part_f, f0)):
        @pl.loop(0, reach // step)
        def _(i, stage=stage, buf=buf, dst=dst):
            for j in range(step):
                k = i * step + j
                put(dst, l0.hx - cx * l0.wide + k, l0.own, split_x(stage[cx * (chip_y - reach) + k, inner], buf[k], cx))
    arrive(row_halo)
    arrive(halo)
    finish(row_halo)
    finish(halo)
    for copy in partner:
        copy.wait_send()
    outer_plane = l0.hx - l0.wide + cx * reach

    for buf, dst in ((recv_yu, u0), (recv_yf, f0)):
        @pl.loop(0, l0.wide // 2)
        def _(i, buf=buf, dst=dst):
            for j in range(2):
                put(dst, outer_plane + 2 * i + j, l0.own, split_x(buf[0, 2 * i + j], buf[1, 2 * i + j], 0))

    def put_rows(p, side, buf, k):
        row = l0.z0 + l0.nz if side else l0.z0 - half
        for h, part in enumerate(split_x(buf[0, k], buf[1, k], 0)):
            pltpu.store(u0.at[p, h, pl.ds(row, TILE)], part, mask=jnp.logical_not(upper))
            pltpu.store(f0.at[p, h, pl.ds(row - half, TILE)], part, mask=upper)
    some = reach // 3

    @pl.loop(0, reach // some)
    def _(i):
        for j in range(some):
            for side in range(2):
                put_rows(l0.hx - cx * l0.wide + i * some + j, side, recv_z.at[side], i * some + j)
    for side in range(2):
        for j in range(l0.wide):
            put_rows(outer_plane + j, side, recv_d.at[side], j)
    sweep(u0, v0, f0, l0, mask0, cfg.stiffness)
    sweep(v0, u0, f0, l0, mask0)
    restrict_level(u0, f0, l0, mask0, g1, l1, 4, 4)

    exchange(1)
    first_sweep(a1, g1, l1, mask1)
    sweep(a1, b1, g1, l1, mask1)
    restrict_level(b1, g1, l1, mask1, g2, l2, 8, 8)
    exchange(2)
    first_sweep(a2, g2, l2, mask2)
    sweep(a2, b2, g2, l2, mask2)

    restrict_planes(b2, g2, l2, mask2, 4)
    ny3, nz3, width = l2.ny // 2, l2.nz // 2, l2.nx // 2
    near = rows_of(square) - 2 * (lanes_of(square) % width)
    got = dot(stack([restricted_rows(j, l2) for j in range(ny3)]), weights(near, 2.0 * eighth, eighth))
    tile = (TILE, LANES)
    lane = lanes_of(tile)
    block = lane // width
    blocks = LANES // width
    packed = got[:nz3]
    for j in range(1, ny3):
        packed = jnp.where(block == j, got[j * nz3:(j + 1) * nz3], packed)
    packed = roll(packed, width * cz)
    message[...] = packed
    slot = yb * n_z + cz
    slots[slot] = packed

    def gather_copy(k, at):
        return pltpu.make_async_remote_copy(
            src_ref=message, dst_ref=slots.at[at], send_sem=all_s.at[k], recv_sem=all_r.at[at], device_id=peer(offsets[k]), device_id_type=MESH)

    for k in range(total - 1):
        gather_copy(k, slot).start()
    for k, offset in enumerate(offsets):
        who = peer(offset)
        gather_copy(k, (who['sy'] * n_x + who['sx']) * n_z + who['sz']).wait_recv()

    data = pl.ds(TILE, TILE)
    whole = row_blocks * ny3
    for s in range(2):
        @pl.loop(0, TILE)
        def _(i, s=s):
            for at in (i, TILE + whole + i):
                s3[s, at, data] = jnp.zeros(tile, F32)
    live = lane < width * n_z

    @pl.loop(0, row_blocks)
    def _(part):
        for j in range(ny3):
            acc = jnp.zeros(tile, F32)
            for t in range(n_z):
                acc = jnp.where((block + 2 * blocks - t - j) % blocks == 0, slots[part * n_z + t], acc)
            acc = jnp.where(live, roll(acc, back(width * j)), 0.0)
            g3[part * ny3 + j] = acc
            s3[0, TILE + part * ny3 + j, data] = acc * NINTH

    row = rows_of(tile)
    x_first, x_last = lane % width == 0, lane % width == width - 1
    top, bottom = row == 0, row == TILE - 1
    z_first, z_last = lane < width, lane >= width * (n_z - 1)

    def coarse_sweep(k, carry):
        old, new = k % 2, (k + 1) % 2
        xm, c = s3[old, TILE - 1, data], s3[old, TILE, data]
        for y in range(whole):
            at = TILE + y
            xp = s3[old, at + 1, data]
            above = jnp.where(z_first, 0.0, roll(s3[old, at, pl.ds(2 * TILE - 1, TILE)], width % LANES))
            below = jnp.where(z_last, 0.0, roll(s3[old, at, pl.ds(1, TILE)], back(width)))
            zm = jnp.where(top, above, s3[old, at, pl.ds(TILE - 1, TILE)])
            zp = jnp.where(bottom, below, s3[old, at, pl.ds(TILE + 1, TILE)])
            left = jnp.where(x_first, 0.0, roll(c, 1))
            right = jnp.where(x_last, 0.0, roll(c, LANES - 1))
            t = (xm + xp) + (zm + zp) + (left + right) + 3.0 * c + g3[y]
            s3[new, at, data] = t * NINTH
            xm, c = c, xp
        return carry
    lax.fori_loop(0, COARSE_SWEEPS - 1, coarse_sweep, 0)

    first = (l2.begin - l2.hx) // 2
    for i in range(e3.shape[0]):
        c = s3[(COARSE_SWEEPS - 1) % 2, yb * ny3 + (TILE + i + first), data]
        for k in range(3):
            ok = (lane < width) & (cz + k > 0) & (cz + k < n_z + 1)
            e3[i, 0, pl.ds(TILE * k, TILE)] = jnp.where(ok, roll(c, back((cz + k) * width + LANES - width)), 0.0)

    prolong_planes(e3, 0, TILE, 0, 3 * TILE, width, 6, 2, l2)
    correct(b2, l2, mask2, 5)
    sweep(b2, a2, g2, l2, mask2)
    sweep(a2, b2, g2, l2, mask2)
    prolong_planes(b2, l2.hx + (l1.begin - l1.hx) // 2, l2.z0, l2.top, l2.rows, l2.nx, 8, 2, l1)
    correct(b1, l1, mask1, 7)
    sweep(b1, a1, g1, l1, mask1)
    sweep(a1, b1, g1, l1, mask1)
    prolong_planes(b1, l1.hx + (l0.begin - l0.hx) // 2, l1.z0, l1.top, l1.rows, l1.nx, 8, 3, l0)
    correct(u0, l0, mask0, 4)
    sweep(u0, v0, f0, l0, mask0)

    def results(i):
        here, there = pl.ds(i * step, step), pl.ds(cx * l0.ny + i * step, step)
        return (pltpu.make_async_copy(stage_u.at[here, inner], out.at[there], out_sem.at[0, i]),
                pltpu.make_async_remote_copy(
                    src_ref=stage_f.at[here, inner], dst_ref=out.at[there], send_sem=out_sem.at[1, i], recv_sem=out_sem.at[2, i],
                    device_id={'sx': 1 - cx}, device_id_type=MESH))

    @pl.loop(0, l0.ny // step)
    def _(i):
        for j in range(step):
            k = i * step + j
            p = l0.hx + k
            c = get(v0, p, l0.own, l0)
            around = neighbours(v0, p, get(v0, p - 1, l0.own, l0), c, get(v0, p + 1, l0.own, l0), l0, l0.z0, l0.nz)
            got = every(lambda x, y, g: (x + 3.0 * y + g) * (NINTH / cfg.stiffness), around, c, get(f0, p, l0.own, l0))
            stage_u[k, inner], stage_f[k, inner] = merge_x(*got, cx)
        for copy in results(i):
            copy.start()

    @pl.loop(0, l0.ny // step)
    def _(i):
        local, remote = results(i)
        local.wait()
        remote.wait()
    drain(1)
    drain(2)

    for k in range(total - 1):
        gather_copy(k, slot).wait_send()


def local_cycle(rhs, start, counts, size):
    rhs, start = (jnp.transpose(x, (1, 2, 0)) for x in (rhs, start))
    n_x, n_y, n_z = counts
    chip_y, nz, nx = rhs.shape
    shapes = [(chip_y // n_x >> k, nz >> k, nx * n_x >> k) for k in range(3)]
    l0 = make_level(shapes[0], 6, 8, 4, nz + 8, 2, 8, (shapes[0][0] + 8) // 8, 4, 24)
    l1 = make_level(shapes[1], 8, 16, 8, shapes[1][1] + 16, 2, 14, (shapes[1][0] + 12) // 14, 5, 24)
    l2 = make_level(shapes[2], 8, 16, 8, shapes[2][1] + 16, 2, 10, (shapes[2][0] + 12) // 10, 6, 32)
    cfg = types.SimpleNamespace(levels=(l0, l1, l2), counts=counts, stiffness=float((size + 1) ** 2))
    total = n_x * n_y * n_z

    def vmem(*shape):
        return pltpu.VMEM(shape, F32)

    scratch = [vmem(lv.planes, lv.parts, lv.depth, LANES) for lv in (l0, l1, l2) for _ in range(3)]
    whole = n_x * n_y * (l2.ny // 2)
    reach = l0.ny + l0.wide
    scratch += [vmem(12, 1, 3 * TILE, LANES), vmem(l1.ny + 8, l1.rows, LANES), vmem(2, l1.ny + 8, l0.depth, LANES)]
    scratch += [vmem(chip_y, l0.depth, LANES)] * 2 + [vmem(reach, nz, LANES)] * 2
    scratch += [vmem(2, whole + 2 * TILE, 3 * TILE, LANES), vmem(whole, TILE, LANES), vmem(total, TILE, LANES), vmem(TILE, LANES)]
    scratch += [vmem(3, lv.rows, LANES) for lv in (l0, l1, l2)]
    scratch += [vmem(2, chip_y, TILE, LANES), vmem(2, n_x, reach, TILE, LANES), vmem(2, 2, l0.wide, TILE, LANES)]
    scratch += [vmem(2, l0.wide, nz, LANES)] * 2
    sems = [(2,), (3, l0.ny // 4), (16,), (16,), (2, len(SIDES)), (2, len(SIDES)), (total,), (total,)]
    scratch += [pltpu.SemaphoreType.DMA(shape) for shape in sems]
    got = pl.pallas_call(
        functools.partial(kernel, cfg),
        out_shape=jax.ShapeDtypeStruct(rhs.shape, F32),
        in_specs=[pl.BlockSpec(memory_space=pl.ANY)] * 2,
        out_specs=pl.BlockSpec(memory_space=pl.ANY),
        scratch_shapes=scratch,
        compiler_params=pltpu.CompilerParams(collective_id=0, has_side_effects=True, vmem_limit_bytes=60 * 2 ** 20),
    )(rhs, start)
    return jnp.transpose(got, (2, 0, 1))


def solution(mesh):
    counts = (mesh.shape['sx'], mesh.shape['sy'], mesh.shape['sz'])
    spec = P(('dp', 'sx'), 'sy', 'sz')

    def run(rhs_grid, u_start):
        size = rhs_grid.shape[0] // mesh.shape['dp']
        cycle = functools.partial(local_cycle, counts=counts, size=size)
        return jax.shard_map(cycle, mesh=mesh, in_specs=(spec, spec), out_specs=spec, check_vma=False)(rhs_grid, u_start)
    return run
```

```python
import functools
import types
import jax
import jax.numpy as jnp
from jax import lax
from jax.experimental import pallas as pl
from jax.experimental.pallas import tpu as pltpu
from jax.sharding import PartitionSpec as P

F32 = jnp.float32
MESH = pl.DeviceIdType.MESH
LANES = 128
TILE = 8
NINTH = 1.0 / 9.0
COARSE_SWEEPS = 16
OPPOSITE = (1, 0, 3, 2, 7, 6, 5, 4)
STEP_Y = (-1, 1, 0, 0, -1, -1, 1, 1)
STEP_Z = (0, 0, -1, 1, -1, 1, -1, 1)
SIDES = range(len(STEP_Y))


def make_level(shape, hx, z0, top, rows, begin, group, count, wide, block):
    ny, nz, nx = shape
    lv = types.SimpleNamespace(ny=ny, nz=nz, nx=nx, hx=hx, z0=z0, top=top, rows=rows, begin=begin, group=group, count=count, wide=wide)
    lv.planes = ny + 2 * hx
    lv.depth = nz + 2 * z0
    lv.parts = max(nx // LANES, 1)
    lv.own = pl.ds(z0, nz)
    lv.all = pl.ds(top, rows)
    lv.blocks = [(top + i, min(block, rows - i)) for i in range(0, rows, block)]
    return lv


def lanes_of(shape):
    return lax.broadcasted_iota(jnp.int32, shape, len(shape) - 1)


def rows_of(shape):
    return lax.broadcasted_iota(jnp.int32, shape, len(shape) - 2)


def roll(x, shift):
    return pltpu.roll(x, shift, 1)


def from_below(x):
    return jnp.where(lanes_of(x.shape) == 0, 0.0, roll(x, 1))


def from_above(x):
    return jnp.where(lanes_of(x.shape) == LANES - 1, 0.0, roll(x, LANES - 1))


def halves(x):
    return x[:, :LANES], x[:, LANES:]


def get(ref, p, rows, lv):
    return [ref[p, h, rows] for h in range(lv.parts)]


def put(ref, p, rows, values):
    for h, value in enumerate(values):
        ref[p, h, rows] = value


def every(f, *lists):
    return [f(*values) for values in zip(*lists)]


def join(*parts):
    return jnp.concatenate(parts, axis=1)


def stack(parts):
    return jnp.concatenate(parts, axis=0)


def back(shift):
    return (4 * LANES - shift) % LANES


def flag(condition):
    return jnp.where(condition, 1, 0)


def pick(x, index):
    return jnp.take_along_axis(x, index, axis=1, mode='promise_in_bounds')


def dot(x, w):
    return jnp.dot(x, w, precision=lax.Precision.HIGHEST, preferred_element_type=F32)


def kernel(cfg, rhs, start, out, *scratch):
    (u0, v0, f0, a1, b1, g1, a2, b2, g2, e3, pz, pb, stage_u, stage_f, part_u, part_f, s3, g3, slots, message, mask0, mask1, mask2,
     send_z, recv_z, recv_d, recv_yu, recv_yf,
     load_sem, out_sem, fine_s, fine_r, send_sem, recv_sem, all_s, all_r, ready) = scratch
    l0, l1, l2 = levels = cfg.levels
    masks = (mask0, mask1, mask2)
    n_x, n_y, n_z = cfg.counts
    cx, cy, cz = lax.axis_index('sx'), lax.axis_index('sy'), lax.axis_index('sz')
    total = n_x * n_y * n_z
    row_blocks = n_x * n_y
    yb = cy * n_x + cx

    inner = pl.ds(TILE, l0.nz)
    loads = [pltpu.make_async_copy(src, dst.at[:, inner], load_sem.at[k]) for k, (src, dst) in enumerate(((start, stage_u), (rhs, stage_f)))]
    for copy in loads:
        copy.start()

    offsets = [(dz, dy, dx) for dz in range(n_z) for dy in range(n_y) for dx in range(n_x)][1:]
    offsets.sort(key=lambda o: -2 * (min(o[0], n_z - o[0]) + min(o[1], n_y - o[1])) - o[2])

    def peer(offset):
        return {name: lax.rem(at + d, n) for name, at, n, d in zip(('sz', 'sy', 'sx'), (cz, cy, cx), (n_z, n_y, n_x), offset)}

    def inside(step, at, count):
        if step == 0:
            return True
        return at > 0 if step < 0 else at < count - 1

    around_me = [o for o in offsets if o[0] in (0, 1, n_z - 1) and o[1] in (0, 1, n_y - 1)]
    barrier = pltpu.get_barrier_semaphore()
    for offset in around_me:
        pl.semaphore_signal(barrier, inc=1, device_id=peer(offset), device_id_type=MESH)
    outer = 2 * cx - 1
    has_outer = (cy + outer >= 0) & (cy + outer < n_y)

    def exists(d):
        return jnp.logical_and(inside(STEP_Y[d], yb, row_blocks), inside(STEP_Z[d], cz, n_z))

    def zero(ref):
        @pl.loop(0, ref.shape[0])
        def _(i):
            ref[i] = jnp.zeros(ref.shape[1:], F32)

    def span(step, first, n, wide, own):
        if step == 0:
            return pl.ds(first, n)
        if step < 0:
            return pl.ds(first if own else first - wide, wide)
        return pl.ds(first + n - wide if own else first + n, wide)

    def region(index, d, own):
        lv, arr = levels[index], (None, g1, g2)[index]
        return arr.at[span(STEP_Y[d], lv.hx, lv.ny, lv.wide, own), 0, span(STEP_Z[d], lv.z0, lv.nz, TILE, own)]

    def halo_copy(index, d, arriving):
        k = index - 1
        at = yb + STEP_Y[d]
        return pltpu.make_async_remote_copy(
            src_ref=region(index, d, not arriving), dst_ref=region(index, d if arriving else OPPOSITE[d], False),
            send_sem=send_sem.at[k, d], recv_sem=recv_sem.at[k, d if arriving else OPPOSITE[d]],
            device_id={'sx': at % n_x, 'sy': at // n_x, 'sz': cz + STEP_Z[d]}, device_id_type=MESH)

    def each(act):
        for d in (4, 5, 6, 7, 2, 3, 0, 1):
            @pl.when(exists(d))
            def _(d=d):
                act(d)

    def exchange(index):
        each(lambda d: halo_copy(index, d, False).start())
        each(lambda d: halo_copy(index, d, True).wait_recv())

    def drain(index):
        each(lambda d: halo_copy(index, d, False).wait_send())

    chip_y = n_x * l0.ny
    reach = l0.ny + l0.wide

    def fine_copies():
        got = []

        def add(sends, arrives, src, dst, arrival, k, theirs, **to):
            made = [pltpu.make_async_remote_copy(
                src_ref=a, dst_ref=b, send_sem=fine_s.at[k], recv_sem=fine_r.at[r], device_id=to, device_id_type=MESH)
                for a, b, r in ((src, dst, theirs[0]), (arrival, arrival, theirs[1]))]
            got.append((sends, arrives, *made))
        n = 0
        for z_side, z_step in enumerate((-1, 1)):
            for y_side, y_step in enumerate((-1, 1)):
                edge = pl.ds(0 if y_step < 0 else chip_y - l0.wide, l0.wide)
                to_z = jnp.logical_and(inside(y_step, cy, n_y), inside(z_step, cz, n_z))
                in_z = jnp.logical_and(has_outer, inside(z_step, cz, n_z))
                add(to_z, in_z, send_z.at[z_side, edge], recv_d.at[1 - z_side, cx], recv_d.at[z_side, y_side], n,
                    (8 + 2 * (1 - z_side) + cx, 8 + 2 * z_side + y_side), sx=1 - y_side, sy=cy + y_step, sz=cz + z_step)
                n += 1
        for z_side, z_step in enumerate((-1, 1)):
            for core in range(n_x):
                there = inside(z_step, cz, n_z)
                add(there, there, send_z.at[z_side, pl.ds(core * (chip_y - reach), reach)], recv_z.at[1 - z_side, cx],
                    recv_z.at[z_side, core], n, (12 + 2 * (1 - z_side) + cx, 12 + 2 * z_side + core), sx=core, sz=cz + z_step)
                n += 1
        return got

    def row_copies():
        got = []
        for y_side, y_step in enumerate((-1, 1)):
            edge = pl.ds(0 if y_step < 0 else chip_y - l0.wide, l0.wide)
            for k, (stage, buf) in enumerate(((stage_u, recv_yu), (stage_f, recv_yf))):
                made = [pltpu.make_async_remote_copy(
                    src_ref=a, dst_ref=b, send_sem=fine_s.at[8 + 2 * y_side + k], recv_sem=fine_r.at[2 * r + k],
                    device_id={'sx': 1 - y_side, 'sy': cy + y_step}, device_id_type=MESH)
                    for a, b, r in ((stage.at[edge, inner], buf.at[cx], cx), (buf.at[y_side], buf.at[y_side], y_side))]
                got.append((inside(y_step, cy, n_y), has_outer, *made))
        return got

    def partner_copies():
        other = pl.ds((1 - cx) * (chip_y - reach), reach)
        return [pltpu.make_async_remote_copy(
            src_ref=stage.at[other, inner], dst_ref=buf, send_sem=fine_s.at[12 + k], recv_sem=fine_r.at[4 + k],
            device_id={'sx': 1 - cx}, device_id_type=MESH) for k, (stage, buf) in enumerate(((stage_u, part_u), (stage_f, part_f)))]

    def begin(copies):
        for sends, _, copy, _ in copies:
            @pl.when(sends)
            def _(copy=copy):
                copy.start()

    def arrive(copies):
        for _, arrives, _, copy in copies:
            @pl.when(arrives)
            def _(copy=copy):
                copy.wait_recv()

    def finish(copies):
        for sends, _, copy, _ in copies:
            @pl.when(sends)
            def _(copy=copy):
                copy.wait_send()

    @pl.when(jnp.logical_not(has_outer))
    def _():
        for buf in (recv_yu, recv_yf, recv_d):
            for k in range(2):
                zero(buf.at[k])
    for z_side, z_step in enumerate((-1, 1)):
        @pl.when(jnp.logical_not(inside(z_step, cz, n_z)))
        def _(z_side=z_side):
            for core in range(n_x):
                zero(recv_z.at[z_side, core])
            zero(recv_d.at[z_side])
    for index in (1, 2):
        for d in SIDES:
            @pl.when(jnp.logical_not(exists(d)))
            def _(index=index, d=d):
                zero(region(index, d, False))

    for lv, arrays in ((l0, (u0, v0)), (l1, (a1, b1)), (l2, (a2, b2))):
        for arr in arrays:
            for plane, outside in ((lv.hx - 1, yb == 0), (lv.hx + lv.ny, yb == row_blocks - 1)):
                @pl.when(outside)
                def _(arr=arr, lv=lv, plane=plane):
                    put(arr, plane, lv.all, [jnp.zeros((lv.rows, LANES), F32)] * lv.parts)

    for lv, table in zip(levels, masks):
        shape = (lv.rows, LANES)
        z = rows_of(shape) + (lv.top - lv.z0) + cz * lv.nz
        ok = (z >= 0) & (z < n_z * lv.nz) & (lanes_of(shape) < lv.nx)
        table[0] = jnp.zeros(shape, F32)
        table[1] = jnp.where(ok, 1.0, 0.0).astype(F32)
        table[2] = jnp.where(ok, NINTH, 0.0).astype(F32)

    def valid(lv, p):
        y = p + (yb * lv.ny - lv.hx)
        return flag((y >= 0) & (y < row_blocks * lv.ny))

    middle = LANES // 2

    def lower(shape, core):
        return lanes_of(shape) // middle == core

    def split_x(first, second, core):
        lane = lanes_of(first.shape)
        pair = 2 * (lane % middle)
        first, second = pick(first, pair + (lane // middle + core) % 2), pick(second, pair + (lane // middle + 1 - core) % 2)
        here = lower(first.shape, core)
        return [jnp.where(here, first, second), roll(jnp.where(here, second, first), middle)]

    def merge_x(even, odd, core):
        lane = lanes_of(even.shape)
        odd = roll(odd, middle)
        here = lower(even.shape, core)
        spot = lane // 2 + middle * ((lane + core) % 2)
        return pick(jnp.where(here, even, odd), spot), pick(jnp.where(here, odd, even), (spot + middle) % LANES)
    pl.semaphore_wait(barrier, len(around_me))

    def across(c, lv):
        if lv.parts > 1:
            even, odd = c
            return [odd + from_below(odd), even + from_above(even)]
        if lv.nx == LANES:
            return [from_below(c[0]) + from_above(c[0])]
        return [roll(c[0], 1) + roll(c[0], LANES - 1)]

    def neighbours(src, p, xm, c, xp, lv, top, n):
        zm, zp = get(src, p, pl.ds(top - 1, n), lv), get(src, p, pl.ds(top + 1, n), lv)
        return every(lambda a, b, d, e, f: ((a + b) + (d + e)) + f, xm, xp, zm, zp, across(c, lv))

    def table_rows(table, k, lv, top, n):
        return table[k, pl.ds(top - lv.top, n)]

    def sweep(src, dst, rhs_ref, lv, table, scale=None):
        @pl.loop(0, lv.count)
        def _(g):
            base = lv.begin + g * lv.group
            for top, n in lv.blocks:
                rows = pl.ds(top, n)
                xm, c = get(src, base - 1, rows, lv), get(src, base, rows, lv)
                for j in range(lv.group):
                    p = base + j
                    xp = get(src, p + 1, rows, lv)
                    t = every(lambda a, b: a + 3.0 * b, neighbours(src, p, xm, c, xp, lv, top, n), c)
                    if scale is not None:
                        t = [x * scale for x in t]
                    keep = table_rows(table, 2 * valid(lv, p), lv, top, n)
                    put(dst, p, rows, every(lambda a, b: (a + b) * keep, t, get(rhs_ref, p, rows, lv)))
                    xm, c = c, xp

    def first_sweep(dst, rhs_ref, lv, table):
        @pl.loop(0, lv.count)
        def _(g):
            for j in range(lv.group):
                p = lv.begin + g * lv.group + j
                dst[p, 0, lv.all] = rhs_ref[p, 0, lv.all] * table[2 * valid(lv, p)]

    def restrict_planes(src, rhs_ref, lv, table, group):
        def res(p, xm, c, xp, top, n):
            return every(lambda a, b, d: a + b - 6.0 * d, neighbours(src, p, xm, c, xp, lv, top, n), get(rhs_ref, p, pl.ds(top, n), lv), c)

        @pl.loop(0, lv.ny // 2 // group)
        def _(i):
            for top, n in lv.blocks:
                rows = pl.ds(top, n)
                p = lv.hx + 2 * group * i
                xm, c = get(src, p - 1, rows, lv), get(src, p, rows, lv)
                prev = res(p - 1, get(src, p - 2, rows, lv), xm, c, top, n)
                prev = [jnp.where((yb > 0) | (i > 0), x, 0.0) for x in prev]
                keep = table_rows(table, 1, lv, top, n)
                for j in range(group):
                    x1, x2 = get(src, p + 1, rows, lv), get(src, p + 2, rows, lv)
                    even = res(p, xm, c, x1, top, n)
                    odd = res(p + 1, c, x1, x2, top, n)
                    for h in range(lv.parts):
                        pb[h, i * group + j, rows] = ((prev[h] + odd[h]) + (even[h] + even[h])) * keep
                    prev, xm, c, p = odd, x1, x2, p + 2

    def restricted_rows(i, lv, h=0):
        half = lv.nz // 2
        return ((pb[h, i, pl.ds(lv.z0 - 1, half, stride=2)] + pb[h, i, pl.ds(lv.z0 + 1, half, stride=2)])
                + 2.0 * pb[h, i, pl.ds(lv.z0, half, stride=2)])

    def weights(near, one, other):
        return jnp.where(near == 0, one, jnp.where((near == 1) | (near == -1), other, 0.0)).astype(F32)

    square = (LANES, LANES)
    eighth = 1.0 / (TILE * TILE)

    def restrict_level(src, rhs_ref, lv, table, coarse_rhs, coarse, group, step):
        restrict_planes(src, rhs_ref, lv, table, group)
        lane = lanes_of(square)
        w = jnp.where(lane < coarse.nx, weights(rows_of(square) - 2 * lane, 2.0 * eighth, eighth), 0.0)

        @pl.loop(0, coarse.ny // step)
        def _(i):
            got = [restricted_rows(i * step + j, lv) for j in range(step)]
            if lv.parts > 1:
                odds = [restricted_rows(i * step + j, lv, 1) for j in range(step)]
                got = [((odd + from_below(odd)) + 2.0 * even) * eighth for even, odd in zip(got, odds)]
            else:
                got = dot(stack(got), w)
                got = [got[j * coarse.nz:(j + 1) * coarse.nz] for j in range(step)]
            for j in range(step):
                coarse_rhs[coarse.hx + i * step + j, 0, coarse.own] = got[j]

    def prolong_planes(e, first, e_z0, e_top, e_rows, e_nx, chunk, n_chunks, lv):
        lane, below = lanes_of(square), rows_of(square)
        w = jnp.where(below < e_nx, weights(lane - 2 * below, 4.0, 2.0), 0.0)
        row = e_z0 - e_top - (lv.z0 - lv.top) // 2
        n = lv.rows // 2

        @pl.loop(0, n_chunks)
        def _(i):
            planes = pl.ds(first + i * chunk, chunk)
            got = e[planes, 0, pl.ds(e_top, e_rows)]
            if lv.parts == 1:
                got = dot(got.reshape(chunk * e_rows, LANES), w).reshape(chunk, e_rows, LANES)
            else:
                got = got * 4.0
            pz[pl.ds(i * chunk, chunk), pl.ds(0, e_rows)] = got

        @pl.loop(0, n_chunks)
        def _(i):
            for j in range(chunk):
                a = pz[i * chunk + j, pl.ds(row, n)]
                b = pz[i * chunk + j, pl.ds(row + 1, n)]
                pb[0, i * chunk + j, pl.ds(lv.top, n, stride=2)] = a
                pb[0, i * chunk + j, pl.ds(lv.top + 1, n, stride=2)] = 0.5 * (a + b)

    def correct(dst, lv, table, pairs):
        def load(at, rows):
            a = pb[0, at, rows]
            return [a, 0.5 * (a + from_above(a))] if lv.parts > 1 else [a]

        @pl.loop(0, lv.group * lv.count // (2 * pairs))
        def _(i):
            for top, n in lv.blocks:
                rows = pl.ds(top, n)
                a = load(i * pairs, rows)
                for j in range(pairs):
                    b = load(i * pairs + j + 1, rows)
                    p = lv.begin + 2 * (pairs * i + j)
                    between = every(lambda x, y: 0.5 * (x + y), a, b)
                    for q, add in ((p, a), (p + 1, between)):
                        keep = table_rows(table, valid(lv, q), lv, top, n)
                        put(dst, q, rows, every(lambda x, y: (x + y) * keep, get(dst, q, rows, lv), add))
                    a = b

    partner, row_halo, halo = partner_copies(), row_copies(), fine_copies()
    for copy in loads:
        copy.wait()
    begin(row_halo)
    for copy in partner:
        copy.start()
    half = TILE // 2
    upper = rows_of((TILE, LANES)) >= half

    @pl.loop(0, chip_y // TILE)
    def _(i):
        for j in range(TILE):
            y = i * TILE + j
            for side, row in enumerate((TILE, TILE + l0.nz - half)):
                send_z[side, y] = jnp.where(upper, stage_f[y, pl.ds(row - half, TILE)], stage_u[y, pl.ds(row, TILE)])
    begin(halo)
    for offset in around_me:
        pl.semaphore_signal(ready, inc=1, device_id=peer(offset), device_id_type=MESH)

    step = 4
    some = reach // 3
    for copy in partner:
        copy.wait_recv()
    for stage, buf, dst in ((stage_u, part_u, u0), (stage_f, part_f, f0)):
        @pl.loop(0, reach // step)
        def _(i, stage=stage, buf=buf, dst=dst):
            for j in range(step):
                k = i * step + j
                put(dst, l0.hx - cx * l0.wide + k, l0.own, split_x(stage[cx * (chip_y - reach) + k, inner], buf[k], cx))
    arrive(row_halo)
    outer_plane = l0.hx - l0.wide + cx * reach

    for buf, dst in ((recv_yu, u0), (recv_yf, f0)):
        for j in range(l0.wide):
            put(dst, outer_plane + j, l0.own, split_x(buf[0, j], buf[1, j], 0))
    arrive(halo)
    finish(row_halo)
    finish(halo)
    for copy in partner:
        copy.wait_send()

    def put_rows(p, side, buf, k):
        row = l0.z0 + l0.nz if side else l0.z0 - half
        for h, part in enumerate(split_x(buf[0, k], buf[1, k], 0)):
            pltpu.store(u0.at[p, h, pl.ds(row, TILE)], part, mask=jnp.logical_not(upper))
            pltpu.store(f0.at[p, h, pl.ds(row - half, TILE)], part, mask=upper)

    @pl.loop(0, reach // some)
    def _(i):
        for j in range(some):
            for side in range(2):
                put_rows(l0.hx - cx * l0.wide + i * some + j, side, recv_z.at[side], i * some + j)
    for side in range(2):
        for j in range(l0.wide):
            put_rows(outer_plane + j, side, recv_d.at[side], j)
    sweep(u0, v0, f0, l0, mask0, cfg.stiffness)
    sweep(v0, u0, f0, l0, mask0)
    restrict_level(u0, f0, l0, mask0, g1, l1, 4, 4)

    exchange(1)
    first_sweep(a1, g1, l1, mask1)
    sweep(a1, b1, g1, l1, mask1)
    restrict_level(b1, g1, l1, mask1, g2, l2, 8, 8)
    exchange(2)
    first_sweep(a2, g2, l2, mask2)
    sweep(a2, b2, g2, l2, mask2)

    restrict_planes(b2, g2, l2, mask2, 4)
    ny3, nz3, width = l2.ny // 2, l2.nz // 2, l2.nx // 2
    near = rows_of(square) - 2 * (lanes_of(square) % width)
    got = dot(stack([restricted_rows(j, l2) for j in range(ny3)]), weights(near, 2.0 * eighth, eighth))
    tile = (TILE, LANES)
    lane = lanes_of(tile)
    block = lane // width
    blocks = LANES // width
    packed = got[:nz3]
    for j in range(1, ny3):
        packed = jnp.where(block == j, got[j * nz3:(j + 1) * nz3], packed)
    packed = roll(packed, width * cy)
    message[...] = packed
    slot = yb * n_z + cz
    slots[slot] = packed

    def gather_copy(k, at):
        return pltpu.make_async_remote_copy(
            src_ref=message, dst_ref=slots.at[at], send_sem=all_s.at[k], recv_sem=all_r.at[at], device_id=peer(offsets[k]), device_id_type=MESH)

    pl.semaphore_wait(ready, len(around_me))
    for k in range(total - 1):
        gather_copy(k, slot).start()
    for k, offset in enumerate(offsets):
        who = peer(offset)
        gather_copy(k, (who['sy'] * n_x + who['sx']) * n_z + who['sz']).wait_recv()

    tall = nz3 * n_z
    data = pl.ds(TILE, tall)
    for which in range(2):
        for y in range(TILE):
            for at in (0, TILE + tall):
                s3[which, y, pl.ds(at, TILE)] = jnp.zeros(tile, F32)
    live = lane < width * n_y

    @pl.loop(0, n_x)
    def _(core):
        for j in range(ny3):
            for z in range(n_z):
                acc = jnp.zeros(tile, F32)
                for t in range(n_y):
                    acc = jnp.where((block + 2 * blocks - t - j) % blocks == 0, slots[(t * n_x + core) * n_z + z], acc)
                acc = jnp.where(live, roll(acc, back(width * j)), 0.0)
                rows = pl.ds(TILE + nz3 * z, nz3)
                g3[core * ny3 + j, rows] = acc
                s3[0, core * ny3 + j, rows] = acc * NINTH

    long = (tall, LANES)
    along = lanes_of(long)
    x_first, x_last = along % width == 0, along % width == width - 1
    y_first, y_last = along < width, along >= width * (n_y - 1)

    def coarse_sweep(k, carry):
        old, new = k % 2, (k + 1) % 2
        lowest, highest = s3[old, 0, data], s3[old, TILE - 1, data]
        c = lowest
        ym = jnp.where(y_first, 0.0, roll(highest, width % LANES))
        beyond = jnp.where(y_last, 0.0, roll(lowest, back(width)))
        for y in range(TILE):
            yp = s3[old, y + 1, data] if y < TILE - 1 else beyond
            around = (ym + yp) + (s3[old, y, pl.ds(TILE - 1, tall)] + s3[old, y, pl.ds(TILE + 1, tall)])
            left = jnp.where(x_first, 0.0, roll(c, 1))
            right = jnp.where(x_last, 0.0, roll(c, LANES - 1))
            s3[new, y, data] = (around + (left + right) + 3.0 * c + g3[y, data]) * NINTH
            ym, c = c, yp
        return carry
    lax.fori_loop(0, COARSE_SWEEPS - 1, coarse_sweep, 0)

    first = (l2.begin - l2.hx) // 2
    for i in range(e3.shape[0]):
        y = yb * ny3 + (i + first)
        c = s3[(COARSE_SWEEPS - 1) % 2, (y + TILE) % TILE, pl.ds(pl.multiple_of(cz * nz3, TILE), 3 * TILE)]
        ok = (lanes_of(c.shape) < width) & (y >= 0) & (y < row_blocks * ny3)
        e3[i, 0] = jnp.where(ok, roll(c, back((y + TILE) // TILE * width + LANES - width)), 0.0)

    prolong_planes(e3, 0, TILE, 0, 3 * TILE, width, 6, 2, l2)
    correct(b2, l2, mask2, 5)
    sweep(b2, a2, g2, l2, mask2)
    sweep(a2, b2, g2, l2, mask2)
    prolong_planes(b2, l2.hx + (l1.begin - l1.hx) // 2, l2.z0, l2.top, l2.rows, l2.nx, 8, 2, l1)
    correct(b1, l1, mask1, 7)
    sweep(b1, a1, g1, l1, mask1)
    sweep(a1, b1, g1, l1, mask1)
    prolong_planes(b1, l1.hx + (l0.begin - l0.hx) // 2, l1.z0, l1.top, l1.rows, l1.nx, 8, 3, l0)
    correct(u0, l0, mask0, 4)
    sweep(u0, v0, f0, l0, mask0)

    def results(i):
        here, there = pl.ds(i * step, step), pl.ds(cx * l0.ny + i * step, step)
        return pltpu.make_async_remote_copy(
            src_ref=stage_f.at[here, inner], dst_ref=out.at[there], send_sem=out_sem.at[0, i], recv_sem=out_sem.at[1, i],
            device_id={'sx': 1 - cx}, device_id_type=MESH)

    @pl.loop(0, l0.ny // step)
    def _(i):
        for j in range(step):
            k = i * step + j
            p = l0.hx + k
            c = get(v0, p, l0.own, l0)
            around = neighbours(v0, p, get(v0, p - 1, l0.own, l0), c, get(v0, p + 1, l0.own, l0), l0, l0.z0, l0.nz)
            got = every(lambda x, y, g: (x + 3.0 * y + g) * (NINTH / cfg.stiffness), around, c, get(f0, p, l0.own, l0))
            out[cx * l0.ny + k], stage_f[k, inner] = merge_x(*got, cx)
        results(i).start()

    @pl.loop(0, l0.ny // step)
    def _(i):
        results(i).wait()
    drain(1)
    drain(2)

    for k in range(total - 1):
        gather_copy(k, slot).wait_send()


def write_out(held, out, sem):
    pltpu.make_async_copy(held, out, sem).start()
    pltpu.make_async_copy(held, out, sem).wait()


def local_cycle(rhs, start, counts, size):
    rhs, start = (jnp.transpose(x, (1, 2, 0)) for x in (rhs, start))
    n_x, n_y, n_z = counts
    chip_y, nz, nx = rhs.shape
    shapes = [(chip_y // n_x >> k, nz >> k, nx * n_x >> k) for k in range(3)]
    l0 = make_level(shapes[0], 6, 8, 4, nz + 8, 2, 8, (shapes[0][0] + 8) // 8, 4, 24)
    l1 = make_level(shapes[1], 8, 16, 8, shapes[1][1] + 16, 2, 14, (shapes[1][0] + 12) // 14, 5, 24)
    l2 = make_level(shapes[2], 8, 16, 8, shapes[2][1] + 16, 2, 10, (shapes[2][0] + 12) // 10, 6, 32)
    cfg = types.SimpleNamespace(levels=(l0, l1, l2), counts=counts, stiffness=float((size + 1) ** 2))
    total = n_x * n_y * n_z

    def vmem(*shape):
        return pltpu.VMEM(shape, F32)

    scratch = [vmem(lv.planes, lv.parts, lv.depth, LANES) for lv in (l0, l1, l2) for _ in range(3)]
    reach = l0.ny + l0.wide
    scratch += [vmem(12, 1, 3 * TILE, LANES), vmem(l1.ny + 8, l1.rows, LANES), vmem(2, l1.ny + 8, l0.depth, LANES)]
    scratch += [vmem(chip_y, l0.depth, LANES)] * 2 + [vmem(reach, nz, LANES)] * 2
    scratch += [vmem(2, TILE, l2.nz // 2 * n_z + 2 * TILE, LANES), vmem(TILE, l2.nz // 2 * n_z + 2 * TILE, LANES), vmem(total, TILE, LANES), vmem(TILE, LANES)]
    scratch += [vmem(3, lv.rows, LANES) for lv in (l0, l1, l2)]
    scratch += [vmem(2, chip_y, TILE, LANES), vmem(2, n_x, reach, TILE, LANES), vmem(2, 2, l0.wide, TILE, LANES)]
    scratch += [vmem(2, l0.wide, nz, LANES)] * 2
    sems = [(2,), (2, l0.ny // 4), (16,), (16,), (2, len(SIDES)), (2, len(SIDES)), (total,), (total,)]
    scratch += [pltpu.SemaphoreType.DMA(shape) for shape in sems] + [pltpu.SemaphoreType.REGULAR]
    got = pl.pallas_call(
        functools.partial(kernel, cfg),
        out_shape=pltpu.VMEM(rhs.shape, F32),
        in_specs=[pl.BlockSpec(memory_space=pl.ANY)] * 2,
        out_specs=pl.BlockSpec(memory_space=pltpu.VMEM),
        scratch_shapes=scratch,
        compiler_params=pltpu.CompilerParams(collective_id=0, has_side_effects=True, vmem_limit_bytes=60 * 2 ** 20),
    )(rhs, start)
    got = pl.pallas_call(
        write_out,
        out_shape=jax.ShapeDtypeStruct(rhs.shape, F32),
        in_specs=[pl.BlockSpec(memory_space=pltpu.VMEM)],
        out_specs=pl.BlockSpec(memory_space=pl.ANY),
        scratch_shapes=[pltpu.SemaphoreType.DMA],
    )(pltpu.with_memory_space_constraint(got, pltpu.VMEM))
    return jnp.transpose(got, (2, 0, 1))


def solution(mesh):
    counts = (mesh.shape['sx'], mesh.shape['sy'], mesh.shape['sz'])
    spec = P(('dp', 'sx'), 'sy', 'sz')

    def run(rhs_grid, u_start):
        size = rhs_grid.shape[0] // mesh.shape['dp']
        cycle = functools.partial(local_cycle, counts=counts, size=size)
        return jax.shard_map(cycle, mesh=mesh, in_specs=(spec, spec), out_specs=spec, check_vma=False)(rhs_grid, u_start)
    return run
```

```python
import functools
import types
import jax
import jax.numpy as jnp
from jax import lax
from jax.experimental import pallas as pl
from jax.experimental.pallas import tpu as pltpu
from jax.sharding import PartitionSpec as P

F32 = jnp.float32
MESH = pl.DeviceIdType.MESH
LANES = 128
TILE = 8
NINTH = 1.0 / 9.0
COARSE_SWEEPS = 16
OPPOSITE = (1, 0, 3, 2, 7, 6, 5, 4)
STEP_Y = (-1, 1, 0, 0, -1, -1, 1, 1)
STEP_Z = (0, 0, -1, 1, -1, 1, -1, 1)
SIDES = range(len(STEP_Y))


def make_level(shape, hx, z0, top, rows, begin, group, count, wide, block):
    ny, nz, nx = shape
    lv = types.SimpleNamespace(ny=ny, nz=nz, nx=nx, hx=hx, z0=z0, top=top, rows=rows, begin=begin, group=group, count=count, wide=wide)
    lv.planes = ny + 2 * hx
    lv.depth = nz + 2 * z0
    lv.parts = max(nx // LANES, 1)
    lv.own = pl.ds(z0, nz)
    lv.all = pl.ds(top, rows)
    lv.blocks = [(top + i, min(block, rows - i)) for i in range(0, rows, block)]
    return lv


def lanes_of(shape):
    return lax.broadcasted_iota(jnp.int32, shape, len(shape) - 1)


def rows_of(shape):
    return lax.broadcasted_iota(jnp.int32, shape, len(shape) - 2)


def roll(x, shift):
    return pltpu.roll(x, shift, 1)


def from_below(x):
    return jnp.where(lanes_of(x.shape) == 0, 0.0, roll(x, 1))


def from_above(x):
    return jnp.where(lanes_of(x.shape) == LANES - 1, 0.0, roll(x, LANES - 1))


def halves(x):
    return x[:, :LANES], x[:, LANES:]


def get(ref, p, rows, lv):
    return [ref[p, h, rows] for h in range(lv.parts)]


def put(ref, p, rows, values):
    for h, value in enumerate(values):
        ref[p, h, rows] = value


def every(f, *lists):
    return [f(*values) for values in zip(*lists)]


def join(*parts):
    return jnp.concatenate(parts, axis=1)


def stack(parts):
    return jnp.concatenate(parts, axis=0)


def back(shift):
    return (4 * LANES - shift) % LANES


def flag(condition):
    return jnp.where(condition, 1, 0)


def pick(x, index):
    return jnp.take_along_axis(x, index, axis=1, mode='promise_in_bounds')


def dot(x, w):
    return jnp.dot(x, w, precision=lax.Precision.HIGHEST, preferred_element_type=F32)


def kernel(cfg, rhs, start, out, *scratch):
    (u0, v0, f0, a1, b1, g1, a2, b2, g2, e3, pz, pb, stage_u, stage_f, part_u, part_f, s3, g3, slots, message, mask0, mask1, mask2,
     send_z, recv_z, recv_d, recv_yu, recv_yf,
     load_sem, out_sem, fine_s, fine_r, send_sem, recv_sem, all_s, all_r, ready) = scratch
    l0, l1, l2 = levels = cfg.levels
    masks = (mask0, mask1, mask2)
    n_x, n_y, n_z = cfg.counts
    cx, cy, cz = lax.axis_index('sx'), lax.axis_index('sy'), lax.axis_index('sz')
    total = n_x * n_y * n_z
    row_blocks = n_x * n_y
    yb = cy * n_x + cx

    inner = pl.ds(TILE, l0.nz)
    chip_y = n_x * l0.ny

    def load(planes, rows):
        shifted = pl.ds(rows.start + TILE, rows.size)
        k = len(loads)
        loads.append(pltpu.make_async_copy(start.at[planes, rows], stage_u.at[planes, shifted], load_sem.at[k]))
        loads.append(pltpu.make_async_copy(rhs.at[planes, rows], stage_f.at[planes, shifted], load_sem.at[k + 1]))
    loads = []
    between = pl.ds(TILE, l0.nz - 2 * TILE)
    for row in (0, l0.nz - TILE):
        load(pl.ds(0, chip_y), pl.ds(row, TILE))
    for plane in (0, chip_y - l0.wide):
        load(pl.ds(plane, l0.wide), between)
    load(pl.ds(l0.wide, chip_y - 2 * l0.wide), between)
    for copy in loads:
        copy.start()

    offsets = [(dz, dy, dx) for dz in range(n_z) for dy in range(n_y) for dx in range(n_x)][1:]
    offsets.sort(key=lambda o: -2 * (min(o[0], n_z - o[0]) + min(o[1], n_y - o[1])) - o[2])

    def peer(offset):
        return {name: lax.rem(at + d, n) for name, at, n, d in zip(('sz', 'sy', 'sx'), (cz, cy, cx), (n_z, n_y, n_x), offset)}

    def inside(step, at, count):
        if step == 0:
            return True
        return at > 0 if step < 0 else at < count - 1

    around_me = [o for o in offsets if o[0] in (0, 1, n_z - 1) and o[1] in (0, 1, n_y - 1)]
    barrier = pltpu.get_barrier_semaphore()
    for offset in around_me:
        pl.semaphore_signal(barrier, inc=1, device_id=peer(offset), device_id_type=MESH)
    outer = 2 * cx - 1
    has_outer = (cy + outer >= 0) & (cy + outer < n_y)

    def exists(d):
        return jnp.logical_and(inside(STEP_Y[d], yb, row_blocks), inside(STEP_Z[d], cz, n_z))

    def zero(ref):
        @pl.loop(0, ref.shape[0])
        def _(i):
            ref[i] = jnp.zeros(ref.shape[1:], F32)

    def span(step, first, n, wide, own):
        if step == 0:
            return pl.ds(first, n)
        if step < 0:
            return pl.ds(first if own else first - wide, wide)
        return pl.ds(first + n - wide if own else first + n, wide)

    def region(index, d, own):
        lv, arr = levels[index], (None, g1, g2)[index]
        return arr.at[span(STEP_Y[d], lv.hx, lv.ny, lv.wide, own), 0, span(STEP_Z[d], lv.z0, lv.nz, TILE, own)]

    def halo_copy(index, d, arriving):
        k = index - 1
        at = yb + STEP_Y[d]
        return pltpu.make_async_remote_copy(
            src_ref=region(index, d, not arriving), dst_ref=region(index, d if arriving else OPPOSITE[d], False),
            send_sem=send_sem.at[k, d], recv_sem=recv_sem.at[k, d if arriving else OPPOSITE[d]],
            device_id={'sx': at % n_x, 'sy': at // n_x, 'sz': cz + STEP_Z[d]}, device_id_type=MESH)

    def each(act):
        for d in (4, 5, 6, 7, 2, 3, 0, 1):
            @pl.when(exists(d))
            def _(d=d):
                act(d)

    def exchange(index):
        each(lambda d: halo_copy(index, d, False).start())
        each(lambda d: halo_copy(index, d, True).wait_recv())

    def drain(index):
        each(lambda d: halo_copy(index, d, False).wait_send())

    reach = l0.ny + l0.wide

    def fine_copies():
        got = []

        def add(sends, arrives, src, dst, arrival, k, theirs, **to):
            made = [pltpu.make_async_remote_copy(
                src_ref=a, dst_ref=b, send_sem=fine_s.at[k], recv_sem=fine_r.at[r], device_id=to, device_id_type=MESH)
                for a, b, r in ((src, dst, theirs[0]), (arrival, arrival, theirs[1]))]
            got.append((sends, arrives, *made))
        n = 0
        for z_side, z_step in enumerate((-1, 1)):
            for y_side, y_step in enumerate((-1, 1)):
                edge = pl.ds(0 if y_step < 0 else chip_y - l0.wide, l0.wide)
                to_z = jnp.logical_and(inside(y_step, cy, n_y), inside(z_step, cz, n_z))
                in_z = jnp.logical_and(has_outer, inside(z_step, cz, n_z))
                add(to_z, in_z, send_z.at[z_side, edge], recv_d.at[1 - z_side, cx], recv_d.at[z_side, y_side], n,
                    (8 + 2 * (1 - z_side) + cx, 8 + 2 * z_side + y_side), sx=1 - y_side, sy=cy + y_step, sz=cz + z_step)
                n += 1
        for z_side, z_step in enumerate((-1, 1)):
            for core in range(n_x):
                there = inside(z_step, cz, n_z)
                add(there, there, send_z.at[z_side, pl.ds(core * (chip_y - reach), reach)], recv_z.at[1 - z_side, cx],
                    recv_z.at[z_side, core], n, (12 + 2 * (1 - z_side) + cx, 12 + 2 * z_side + core), sx=core, sz=cz + z_step)
                n += 1
        return got

    def row_copies():
        got = []
        for y_side, y_step in enumerate((-1, 1)):
            edge = pl.ds(0 if y_step < 0 else chip_y - l0.wide, l0.wide)
            for k, (stage, buf) in enumerate(((stage_u, recv_yu), (stage_f, recv_yf))):
                made = [pltpu.make_async_remote_copy(
                    src_ref=a, dst_ref=b, send_sem=fine_s.at[8 + 2 * y_side + k], recv_sem=fine_r.at[2 * r + k],
                    device_id={'sx': 1 - y_side, 'sy': cy + y_step}, device_id_type=MESH)
                    for a, b, r in ((stage.at[edge, inner], buf.at[cx], cx), (buf.at[y_side], buf.at[y_side], y_side))]
                got.append((inside(y_step, cy, n_y), has_outer, *made))
        return got

    def partner_copies():
        other = pl.ds((1 - cx) * (chip_y - reach), reach)
        return [pltpu.make_async_remote_copy(
            src_ref=stage.at[other, inner], dst_ref=buf, send_sem=fine_s.at[12 + k], recv_sem=fine_r.at[4 + k],
            device_id={'sx': 1 - cx}, device_id_type=MESH) for k, (stage, buf) in enumerate(((stage_u, part_u), (stage_f, part_f)))]

    def begin(copies):
        for sends, _, copy, _ in copies:
            @pl.when(sends)
            def _(copy=copy):
                copy.start()

    def arrive(copies):
        for _, arrives, _, copy in copies:
            @pl.when(arrives)
            def _(copy=copy):
                copy.wait_recv()

    def finish(copies):
        for sends, _, copy, _ in copies:
            @pl.when(sends)
            def _(copy=copy):
                copy.wait_send()

    @pl.when(jnp.logical_not(has_outer))
    def _():
        for buf in (recv_yu, recv_yf, recv_d):
            for k in range(2):
                zero(buf.at[k])
    for z_side, z_step in enumerate((-1, 1)):
        @pl.when(jnp.logical_not(inside(z_step, cz, n_z)))
        def _(z_side=z_side):
            for core in range(n_x):
                zero(recv_z.at[z_side, core])
            zero(recv_d.at[z_side])
    for index in (1, 2):
        for d in SIDES:
            @pl.when(jnp.logical_not(exists(d)))
            def _(index=index, d=d):
                zero(region(index, d, False))

    for lv, arrays in ((l0, (u0, v0)), (l1, (a1, b1)), (l2, (a2, b2))):
        for arr in arrays:
            for plane, outside in ((lv.hx - 1, yb == 0), (lv.hx + lv.ny, yb == row_blocks - 1)):
                @pl.when(outside)
                def _(arr=arr, lv=lv, plane=plane):
                    put(arr, plane, lv.all, [jnp.zeros((lv.rows, LANES), F32)] * lv.parts)

    for lv, table in zip(levels, masks):
        shape = (lv.rows, LANES)
        z = rows_of(shape) + (lv.top - lv.z0) + cz * lv.nz
        ok = (z >= 0) & (z < n_z * lv.nz) & (lanes_of(shape) < lv.nx)
        table[0] = jnp.zeros(shape, F32)
        table[1] = jnp.where(ok, 1.0, 0.0).astype(F32)
        table[2] = jnp.where(ok, NINTH, 0.0).astype(F32)

    def valid(lv, p):
        y = p + (yb * lv.ny - lv.hx)
        return flag((y >= 0) & (y < row_blocks * lv.ny))

    middle = LANES // 2

    def lower(shape, core):
        return lanes_of(shape) // middle == core

    def split_x(first, second, core):
        lane = lanes_of(first.shape)
        pair = 2 * (lane % middle)
        first, second = pick(first, pair + (lane // middle + core) % 2), pick(second, pair + (lane // middle + 1 - core) % 2)
        here = lower(first.shape, core)
        return [jnp.where(here, first, second), roll(jnp.where(here, second, first), middle)]

    def merge_x(even, odd, core):
        lane = lanes_of(even.shape)
        odd = roll(odd, middle)
        here = lower(even.shape, core)
        spot = lane // 2 + middle * ((lane + core) % 2)
        return pick(jnp.where(here, even, odd), spot), pick(jnp.where(here, odd, even), (spot + middle) % LANES)
    pl.semaphore_wait(barrier, len(around_me))

    def across(c, lv):
        if lv.parts > 1:
            even, odd = c
            return [odd + from_below(odd), even + from_above(even)]
        if lv.nx == LANES:
            return [from_below(c[0]) + from_above(c[0])]
        return [roll(c[0], 1) + roll(c[0], LANES - 1)]

    def neighbours(src, p, xm, c, xp, lv, top, n):
        zm, zp = get(src, p, pl.ds(top - 1, n), lv), get(src, p, pl.ds(top + 1, n), lv)
        return every(lambda a, b, d, e, f: ((a + b) + (d + e)) + f, xm, xp, zm, zp, across(c, lv))

    def table_rows(table, k, lv, top, n):
        return table[k, pl.ds(top - lv.top, n)]

    def sweep(src, dst, rhs_ref, lv, table, scale=None):
        @pl.loop(0, lv.count)
        def _(g):
            base = lv.begin + g * lv.group
            for top, n in lv.blocks:
                rows = pl.ds(top, n)
                xm, c = get(src, base - 1, rows, lv), get(src, base, rows, lv)
                for j in range(lv.group):
                    p = base + j
                    xp = get(src, p + 1, rows, lv)
                    t = every(lambda a, b: a + 3.0 * b, neighbours(src, p, xm, c, xp, lv, top, n), c)
                    if scale is not None:
                        t = [x * scale for x in t]
                    keep = table_rows(table, 2 * valid(lv, p), lv, top, n)
                    put(dst, p, rows, every(lambda a, b: (a + b) * keep, t, get(rhs_ref, p, rows, lv)))
                    xm, c = c, xp

    def first_sweep(dst, rhs_ref, lv, table):
        @pl.loop(0, lv.count)
        def _(g):
            for j in range(lv.group):
                p = lv.begin + g * lv.group + j
                dst[p, 0, lv.all] = rhs_ref[p, 0, lv.all] * table[2 * valid(lv, p)]

    def restrict_planes(src, rhs_ref, lv, table, group):
        def res(p, xm, c, xp, top, n):
            return every(lambda a, b, d: a + b - 6.0 * d, neighbours(src, p, xm, c, xp, lv, top, n), get(rhs_ref, p, pl.ds(top, n), lv), c)

        @pl.loop(0, lv.ny // 2 // group)
        def _(i):
            for top, n in lv.blocks:
                rows = pl.ds(top, n)
                p = lv.hx + 2 * group * i
                xm, c = get(src, p - 1, rows, lv), get(src, p, rows, lv)
                prev = res(p - 1, get(src, p - 2, rows, lv), xm, c, top, n)
                prev = [jnp.where((yb > 0) | (i > 0), x, 0.0) for x in prev]
                keep = table_rows(table, 1, lv, top, n)
                for j in range(group):
                    x1, x2 = get(src, p + 1, rows, lv), get(src, p + 2, rows, lv)
                    even = res(p, xm, c, x1, top, n)
                    odd = res(p + 1, c, x1, x2, top, n)
                    for h in range(lv.parts):
                        pb[h, i * group + j, rows] = ((prev[h] + odd[h]) + (even[h] + even[h])) * keep
                    prev, xm, c, p = odd, x1, x2, p + 2

    def restricted_rows(i, lv, h=0):
        half = lv.nz // 2
        return ((pb[h, i, pl.ds(lv.z0 - 1, half, stride=2)] + pb[h, i, pl.ds(lv.z0 + 1, half, stride=2)])
                + 2.0 * pb[h, i, pl.ds(lv.z0, half, stride=2)])

    def weights(near, one, other):
        return jnp.where(near == 0, one, jnp.where((near == 1) | (near == -1), other, 0.0)).astype(F32)

    square = (LANES, LANES)
    eighth = 1.0 / (TILE * TILE)

    def restrict_level(src, rhs_ref, lv, table, coarse_rhs, coarse, group, step):
        restrict_planes(src, rhs_ref, lv, table, group)
        lane = lanes_of(square)
        w = jnp.where(lane < coarse.nx, weights(rows_of(square) - 2 * lane, 2.0 * eighth, eighth), 0.0)

        @pl.loop(0, coarse.ny // step)
        def _(i):
            got = [restricted_rows(i * step + j, lv) for j in range(step)]
            if lv.parts > 1:
                odds = [restricted_rows(i * step + j, lv, 1) for j in range(step)]
                got = [((odd + from_below(odd)) + 2.0 * even) * eighth for even, odd in zip(got, odds)]
            else:
                got = dot(stack(got), w)
                got = [got[j * coarse.nz:(j + 1) * coarse.nz] for j in range(step)]
            for j in range(step):
                coarse_rhs[coarse.hx + i * step + j, 0, coarse.own] = got[j]

    def prolong_planes(e, first, e_z0, e_top, e_rows, e_nx, chunk, n_chunks, lv):
        lane, below = lanes_of(square), rows_of(square)
        w = jnp.where(below < e_nx, weights(lane - 2 * below, 4.0, 2.0), 0.0)
        row = e_z0 - e_top - (lv.z0 - lv.top) // 2
        n = lv.rows // 2

        @pl.loop(0, n_chunks)
        def _(i):
            planes = pl.ds(first + i * chunk, chunk)
            got = e[planes, 0, pl.ds(e_top, e_rows)]
            if lv.parts == 1:
                got = dot(got.reshape(chunk * e_rows, LANES), w).reshape(chunk, e_rows, LANES)
            else:
                got = got * 4.0
            pz[pl.ds(i * chunk, chunk), pl.ds(0, e_rows)] = got

        @pl.loop(0, n_chunks)
        def _(i):
            for j in range(chunk):
                a = pz[i * chunk + j, pl.ds(row, n)]
                b = pz[i * chunk + j, pl.ds(row + 1, n)]
                pb[0, i * chunk + j, pl.ds(lv.top, n, stride=2)] = a
                pb[0, i * chunk + j, pl.ds(lv.top + 1, n, stride=2)] = 0.5 * (a + b)

    def correct(dst, lv, table, pairs):
        def load(at, rows):
            a = pb[0, at, rows]
            return [a, 0.5 * (a + from_above(a))] if lv.parts > 1 else [a]

        @pl.loop(0, lv.group * lv.count // (2 * pairs))
        def _(i):
            for top, n in lv.blocks:
                rows = pl.ds(top, n)
                a = load(i * pairs, rows)
                for j in range(pairs):
                    b = load(i * pairs + j + 1, rows)
                    p = lv.begin + 2 * (pairs * i + j)
                    between = every(lambda x, y: 0.5 * (x + y), a, b)
                    for q, add in ((p, a), (p + 1, between)):
                        keep = table_rows(table, valid(lv, q), lv, top, n)
                        put(dst, q, rows, every(lambda x, y: (x + y) * keep, get(dst, q, rows, lv), add))
                    a = b

    partner, row_halo, halo = partner_copies(), row_copies(), fine_copies()
    for copy in loads[:4]:
        copy.wait()
    half = TILE // 2
    upper = rows_of((TILE, LANES)) >= half

    @pl.loop(0, chip_y // TILE)
    def _(i):
        for j in range(TILE):
            y = i * TILE + j
            for side, row in enumerate((TILE, TILE + l0.nz - half)):
                send_z[side, y] = jnp.where(upper, stage_f[y, pl.ds(row - half, TILE)], stage_u[y, pl.ds(row, TILE)])
    begin(halo)
    for copy in loads[4:8]:
        copy.wait()
    begin(row_halo)
    for copy in loads[8:]:
        copy.wait()
    for copy in partner:
        copy.start()
    for offset in around_me:
        pl.semaphore_signal(ready, inc=1, device_id=peer(offset), device_id_type=MESH)

    step = 4
    some = reach // 3
    for copy in partner:
        copy.wait_recv()
    for stage, buf, dst in ((stage_u, part_u, u0), (stage_f, part_f, f0)):
        @pl.loop(0, reach // step)
        def _(i, stage=stage, buf=buf, dst=dst):
            for j in range(step):
                k = i * step + j
                put(dst, l0.hx - cx * l0.wide + k, l0.own, split_x(stage[cx * (chip_y - reach) + k, inner], buf[k], cx))
    arrive(row_halo)
    outer_plane = l0.hx - l0.wide + cx * reach

    for buf, dst in ((recv_yu, u0), (recv_yf, f0)):
        for j in range(l0.wide):
            put(dst, outer_plane + j, l0.own, split_x(buf[0, j], buf[1, j], 0))
    arrive(halo)
    finish(row_halo)
    finish(halo)
    for copy in partner:
        copy.wait_send()

    def put_rows(p, side, buf, k):
        row = l0.z0 + l0.nz if side else l0.z0 - half
        for h, part in enumerate(split_x(buf[0, k], buf[1, k], 0)):
            pltpu.store(u0.at[p, h, pl.ds(row, TILE)], part, mask=jnp.logical_not(upper))
            pltpu.store(f0.at[p, h, pl.ds(row - half, TILE)], part, mask=upper)

    @pl.loop(0, reach // some)
    def _(i):
        for j in range(some):
            for side in range(2):
                put_rows(l0.hx - cx * l0.wide + i * some + j, side, recv_z.at[side], i * some + j)
    for side in range(2):
        for j in range(l0.wide):
            put_rows(outer_plane + j, side, recv_d.at[side], j)
    sweep(u0, v0, f0, l0, mask0, cfg.stiffness)
    sweep(v0, u0, f0, l0, mask0)
    restrict_level(u0, f0, l0, mask0, g1, l1, 4, 4)

    exchange(1)
    first_sweep(a1, g1, l1, mask1)
    sweep(a1, b1, g1, l1, mask1)
    restrict_level(b1, g1, l1, mask1, g2, l2, 8, 8)
    exchange(2)
    first_sweep(a2, g2, l2, mask2)
    sweep(a2, b2, g2, l2, mask2)

    restrict_planes(b2, g2, l2, mask2, 4)
    ny3, nz3, width = l2.ny // 2, l2.nz // 2, l2.nx // 2
    near = rows_of(square) - 2 * (lanes_of(square) % width)
    got = dot(stack([restricted_rows(j, l2) for j in range(ny3)]), weights(near, 2.0 * eighth, eighth))
    tile = (TILE, LANES)
    lane = lanes_of(tile)
    block = lane // width
    blocks = LANES // width
    packed = got[:nz3]
    for j in range(1, ny3):
        packed = jnp.where(block == j, got[j * nz3:(j + 1) * nz3], packed)
    packed = roll(packed, width * cy)
    message[...] = packed
    slot = yb * n_z + cz
    slots[slot] = packed

    def gather_copy(k, at):
        return pltpu.make_async_remote_copy(
            src_ref=message, dst_ref=slots.at[at], send_sem=all_s.at[k], recv_sem=all_r.at[at], device_id=peer(offsets[k]), device_id_type=MESH)

    pl.semaphore_wait(ready, len(around_me))
    for k in range(total - 1):
        gather_copy(k, slot).start()
    for k, offset in enumerate(offsets):
        who = peer(offset)
        gather_copy(k, (who['sy'] * n_x + who['sx']) * n_z + who['sz']).wait_recv()

    tall = nz3 * n_z
    data = pl.ds(TILE, tall)
    for which in range(2):
        for y in range(TILE):
            for at in (0, TILE + tall):
                s3[which, y, pl.ds(at, TILE)] = jnp.zeros(tile, F32)
    live = lane < width * n_y

    @pl.loop(0, n_x)
    def _(core):
        for j in range(ny3):
            for z in range(n_z):
                acc = jnp.zeros(tile, F32)
                for t in range(n_y):
                    acc = jnp.where((block + 2 * blocks - t - j) % blocks == 0, slots[(t * n_x + core) * n_z + z], acc)
                acc = jnp.where(live, roll(acc, back(width * j)), 0.0)
                rows = pl.ds(TILE + nz3 * z, nz3)
                g3[core * ny3 + j, rows] = acc
                s3[0, core * ny3 + j, rows] = acc * NINTH

    long = (tall, LANES)
    along = lanes_of(long)
    x_first, x_last = along % width == 0, along % width == width - 1
    y_first, y_last = along < width, along >= width * (n_y - 1)

    def coarse_sweep(k, carry):
        old, new = k % 2, (k + 1) % 2
        lowest, highest = s3[old, 0, data], s3[old, TILE - 1, data]
        c = lowest
        ym = jnp.where(y_first, 0.0, roll(highest, width % LANES))
        beyond = jnp.where(y_last, 0.0, roll(lowest, back(width)))
        for y in range(TILE):
            yp = s3[old, y + 1, data] if y < TILE - 1 else beyond
            around = (ym + yp) + (s3[old, y, pl.ds(TILE - 1, tall)] + s3[old, y, pl.ds(TILE + 1, tall)])
            left = jnp.where(x_first, 0.0, roll(c, 1))
            right = jnp.where(x_last, 0.0, roll(c, LANES - 1))
            s3[new, y, data] = (around + (left + right) + 3.0 * c + g3[y, data]) * NINTH
            ym, c = c, yp
        return carry
    lax.fori_loop(0, COARSE_SWEEPS - 1, coarse_sweep, 0)

    first = (l2.begin - l2.hx) // 2
    for i in range(e3.shape[0]):
        y = yb * ny3 + (i + first)
        c = s3[(COARSE_SWEEPS - 1) % 2, (y + TILE) % TILE, pl.ds(pl.multiple_of(cz * nz3, TILE), 3 * TILE)]
        ok = (lanes_of(c.shape) < width) & (y >= 0) & (y < row_blocks * ny3)
        e3[i, 0] = jnp.where(ok, roll(c, back((y + TILE) // TILE * width + LANES - width)), 0.0)

    prolong_planes(e3, 0, TILE, 0, 3 * TILE, width, 6, 2, l2)
    correct(b2, l2, mask2, 5)
    sweep(b2, a2, g2, l2, mask2)
    sweep(a2, b2, g2, l2, mask2)
    prolong_planes(b2, l2.hx + (l1.begin - l1.hx) // 2, l2.z0, l2.top, l2.rows, l2.nx, 8, 2, l1)
    correct(b1, l1, mask1, 7)
    sweep(b1, a1, g1, l1, mask1)
    sweep(a1, b1, g1, l1, mask1)
    prolong_planes(b1, l1.hx + (l0.begin - l0.hx) // 2, l1.z0, l1.top, l1.rows, l1.nx, 8, 3, l0)
    correct(u0, l0, mask0, 4)
    sweep(u0, v0, f0, l0, mask0)

    def results(i):
        here, there = pl.ds(i * step, step), pl.ds(cx * l0.ny + i * step, step)
        return pltpu.make_async_remote_copy(
            src_ref=stage_f.at[here, inner], dst_ref=out.at[there], send_sem=out_sem.at[0, i], recv_sem=out_sem.at[1, i],
            device_id={'sx': 1 - cx}, device_id_type=MESH)

    def merge_group(i):
        for j in range(step):
            k = i * step + j
            out[cx * l0.ny + k], stage_f[k, inner] = merge_x(*get(u0, l0.hx + k, l0.own, l0), cx)

    @pl.loop(0, l0.ny // step)
    def _(i):
        before = (i + l0.ny // step - 1) % (l0.ny // step)
        merge_group(before)
        for j in range(step):
            p = l0.hx + i * step + j
            c = get(v0, p, l0.own, l0)
            around = neighbours(v0, p, get(v0, p - 1, l0.own, l0), c, get(v0, p + 1, l0.own, l0), l0, l0.z0, l0.nz)
            put(u0, p, l0.own, every(lambda x, y, g: (x + 3.0 * y + g) * (NINTH / cfg.stiffness), around, c, get(f0, p, l0.own, l0)))

        @pl.when(i > 0)
        def _():
            results(before).start()
    merge_group(l0.ny // step - 1)
    results(l0.ny // step - 1).start()

    @pl.loop(0, l0.ny // step)
    def _(i):
        results(i).wait()
    drain(1)
    drain(2)

    for k in range(total - 1):
        gather_copy(k, slot).wait_send()


def write_out(held, out, sem):
    pltpu.make_async_copy(held, out, sem).start()
    pltpu.make_async_copy(held, out, sem).wait()


def local_cycle(rhs, start, counts, size):
    rhs, start = (jnp.transpose(x, (1, 2, 0)) for x in (rhs, start))
    n_x, n_y, n_z = counts
    chip_y, nz, nx = rhs.shape
    shapes = [(chip_y // n_x >> k, nz >> k, nx * n_x >> k) for k in range(3)]
    l0 = make_level(shapes[0], 6, 8, 4, nz + 8, 2, 8, (shapes[0][0] + 8) // 8, 4, 24)
    l1 = make_level(shapes[1], 8, 16, 8, shapes[1][1] + 16, 2, 14, (shapes[1][0] + 12) // 14, 5, 24)
    l2 = make_level(shapes[2], 8, 16, 8, shapes[2][1] + 16, 2, 10, (shapes[2][0] + 12) // 10, 6, 32)
    cfg = types.SimpleNamespace(levels=(l0, l1, l2), counts=counts, stiffness=float((size + 1) ** 2))
    total = n_x * n_y * n_z

    def vmem(*shape):
        return pltpu.VMEM(shape, F32)

    scratch = [vmem(lv.planes, lv.parts, lv.depth, LANES) for lv in (l0, l1, l2) for _ in range(3)]
    reach = l0.ny + l0.wide
    scratch += [vmem(12, 1, 3 * TILE, LANES), vmem(l1.ny + 8, l1.rows, LANES), vmem(2, l1.ny + 8, l0.depth, LANES)]
    scratch += [vmem(chip_y, l0.depth, LANES)] * 2 + [vmem(reach, nz, LANES)] * 2
    scratch += [vmem(2, TILE, l2.nz // 2 * n_z + 2 * TILE, LANES), vmem(TILE, l2.nz // 2 * n_z + 2 * TILE, LANES), vmem(total, TILE, LANES), vmem(TILE, LANES)]
    scratch += [vmem(3, lv.rows, LANES) for lv in (l0, l1, l2)]
    scratch += [vmem(2, chip_y, TILE, LANES), vmem(2, n_x, reach, TILE, LANES), vmem(2, 2, l0.wide, TILE, LANES)]
    scratch += [vmem(2, l0.wide, nz, LANES)] * 2
    sems = [(10,), (2, l0.ny // 4), (16,), (16,), (2, len(SIDES)), (2, len(SIDES)), (total,), (total,)]
    scratch += [pltpu.SemaphoreType.DMA(shape) for shape in sems] + [pltpu.SemaphoreType.REGULAR]
    got = pl.pallas_call(
        functools.partial(kernel, cfg),
        out_shape=pltpu.VMEM(rhs.shape, F32),
        in_specs=[pl.BlockSpec(memory_space=pl.ANY)] * 2,
        out_specs=pl.BlockSpec(memory_space=pltpu.VMEM),
        scratch_shapes=scratch,
        compiler_params=pltpu.CompilerParams(collective_id=0, has_side_effects=True, vmem_limit_bytes=60 * 2 ** 20),
    )(rhs, start)
    got = pl.pallas_call(
        write_out,
        out_shape=jax.ShapeDtypeStruct(rhs.shape, F32),
        in_specs=[pl.BlockSpec(memory_space=pltpu.VMEM)],
        out_specs=pl.BlockSpec(memory_space=pl.ANY),
        scratch_shapes=[pltpu.SemaphoreType.DMA],
    )(pltpu.with_memory_space_constraint(got, pltpu.VMEM))
    return jnp.transpose(got, (2, 0, 1))


def solution(mesh):
    counts = (mesh.shape['sx'], mesh.shape['sy'], mesh.shape['sz'])
    spec = P(('dp', 'sx'), 'sy', 'sz')

    def run(rhs_grid, u_start):
        size = rhs_grid.shape[0] // mesh.shape['dp']
        cycle = functools.partial(local_cycle, counts=counts, size=size)
        return jax.shard_map(cycle, mesh=mesh, in_specs=(spec, spec), out_specs=spec, check_vma=False)(rhs_grid, u_start)
    return run
```

```python
import functools
import types
import jax
import jax.numpy as jnp
from jax import lax
from jax.experimental import pallas as pl
from jax.experimental.pallas import tpu as pltpu
from jax.sharding import PartitionSpec as P

F32 = jnp.float32
MESH = pl.DeviceIdType.MESH
LANES = 128
TILE = 8
NINTH = 1.0 / 9.0
COARSE_SWEEPS = 16
PARTS = 3
OPPOSITE = (1, 0, 3, 2, 7, 6, 5, 4)
STEP_Y = (-1, 1, 0, 0, -1, -1, 1, 1)
STEP_Z = (0, 0, -1, 1, -1, 1, -1, 1)
SIDES = range(len(STEP_Y))


def make_level(shape, hx, z0, top, rows, begin, group, count, wide, block):
    ny, nz, nx = shape
    lv = types.SimpleNamespace(ny=ny, nz=nz, nx=nx, hx=hx, z0=z0, top=top, rows=rows, begin=begin, group=group, count=count, wide=wide)
    lv.planes = ny + 2 * hx
    lv.depth = nz + 2 * z0
    lv.parts = max(nx // LANES, 1)
    lv.own = pl.ds(z0, nz)
    lv.all = pl.ds(top, rows)
    lv.blocks = [(top + i, min(block, rows - i)) for i in range(0, rows, block)]
    return lv


def lanes_of(shape):
    return lax.broadcasted_iota(jnp.int32, shape, len(shape) - 1)


def rows_of(shape):
    return lax.broadcasted_iota(jnp.int32, shape, len(shape) - 2)


def roll(x, shift):
    return pltpu.roll(x, shift, 1)


def from_below(x):
    return jnp.where(lanes_of(x.shape) == 0, 0.0, roll(x, 1))


def from_above(x):
    return jnp.where(lanes_of(x.shape) == LANES - 1, 0.0, roll(x, LANES - 1))


def halves(x):
    return x[:, :LANES], x[:, LANES:]


def get(ref, p, rows, lv):
    return [ref[p, h, rows] for h in range(lv.parts)]


def put(ref, p, rows, values):
    for h, value in enumerate(values):
        ref[p, h, rows] = value


def every(f, *lists):
    return [f(*values) for values in zip(*lists)]


def join(*parts):
    return jnp.concatenate(parts, axis=1)


def stack(parts):
    return jnp.concatenate(parts, axis=0)


def back(shift):
    return (4 * LANES - shift) % LANES


def flag(condition):
    return jnp.where(condition, 1, 0)


def pick(x, index):
    return jnp.take_along_axis(x, index, axis=1, mode='promise_in_bounds')


def dot(x, w):
    return jnp.dot(x, w, precision=lax.Precision.HIGHEST, preferred_element_type=F32)


def kernel(cfg, rhs, start, out, *scratch):
    (u0, v0, f0, a1, b1, g1, a2, b2, g2, e3, pz, pb, stage_u, stage_f, part_u, part_f, s3, g3, slots, message, mask0, mask1, mask2,
     send_z, recv_z, recv_d, recv_yu, recv_yf,
     load_sem, out_sem, fine_s, fine_r, send_sem, recv_sem, all_s, all_r, part_s, part_r, ready) = scratch
    l0, l1, l2 = levels = cfg.levels
    masks = (mask0, mask1, mask2)
    n_x, n_y, n_z = cfg.counts
    cx, cy, cz = lax.axis_index('sx'), lax.axis_index('sy'), lax.axis_index('sz')
    total = n_x * n_y * n_z
    row_blocks = n_x * n_y
    yb = cy * n_x + cx

    inner = pl.ds(TILE, l0.nz)
    chip_y = n_x * l0.ny

    def load(planes, rows):
        shifted = pl.ds(rows.start + TILE, rows.size)
        k = len(loads)
        loads.append(pltpu.make_async_copy(start.at[planes, rows], stage_u.at[planes, shifted], load_sem.at[k]))
        loads.append(pltpu.make_async_copy(rhs.at[planes, rows], stage_f.at[planes, shifted], load_sem.at[k + 1]))
    loads = []
    between = pl.ds(TILE, l0.nz - 2 * TILE)
    for row in (0, l0.nz - TILE):
        load(pl.ds(0, chip_y), pl.ds(row, TILE))
    for plane in (0, chip_y - l0.wide):
        load(pl.ds(plane, l0.wide), between)
    load(pl.ds(l0.wide, chip_y - 2 * l0.wide), between)
    for copy in loads:
        copy.start()

    offsets = [(dz, dy, dx) for dz in range(n_z) for dy in range(n_y) for dx in range(n_x)][1:]
    offsets.sort(key=lambda o: -2 * (min(o[0], n_z - o[0]) + min(o[1], n_y - o[1])) - o[2])

    def peer(offset):
        return {name: lax.rem(at + d, n) for name, at, n, d in zip(('sz', 'sy', 'sx'), (cz, cy, cx), (n_z, n_y, n_x), offset)}

    def inside(step, at, count):
        if step == 0:
            return True
        return at > 0 if step < 0 else at < count - 1

    around_me = [o for o in offsets if o[0] in (0, 1, n_z - 1) and o[1] in (0, 1, n_y - 1)]
    barrier = pltpu.get_barrier_semaphore()
    for offset in around_me:
        pl.semaphore_signal(barrier, inc=1, device_id=peer(offset), device_id_type=MESH)
    outer = 2 * cx - 1
    has_outer = (cy + outer >= 0) & (cy + outer < n_y)

    def exists(d):
        return jnp.logical_and(inside(STEP_Y[d], yb, row_blocks), inside(STEP_Z[d], cz, n_z))

    def zero(ref):
        @pl.loop(0, ref.shape[0])
        def _(i):
            ref[i] = jnp.zeros(ref.shape[1:], F32)

    def span(step, first, n, wide, own):
        if step == 0:
            return pl.ds(first, n)
        if step < 0:
            return pl.ds(first if own else first - wide, wide)
        return pl.ds(first + n - wide if own else first + n, wide)

    def region(index, d, own):
        lv, arr = levels[index], (None, g1, g2)[index]
        return arr.at[span(STEP_Y[d], lv.hx, lv.ny, lv.wide, own), 0, span(STEP_Z[d], lv.z0, lv.nz, TILE, own)]

    def halo_copy(index, d, arriving):
        k = index - 1
        at = yb + STEP_Y[d]
        return pltpu.make_async_remote_copy(
            src_ref=region(index, d, not arriving), dst_ref=region(index, d if arriving else OPPOSITE[d], False),
            send_sem=send_sem.at[k, d], recv_sem=recv_sem.at[k, d if arriving else OPPOSITE[d]],
            device_id={'sx': at % n_x, 'sy': at // n_x, 'sz': cz + STEP_Z[d]}, device_id_type=MESH)

    def each(act):
        for d in (4, 5, 6, 7, 2, 3, 0, 1):
            @pl.when(exists(d))
            def _(d=d):
                act(d)

    def exchange(index):
        each(lambda d: halo_copy(index, d, False).start())
        each(lambda d: halo_copy(index, d, True).wait_recv())

    def drain(index):
        each(lambda d: halo_copy(index, d, False).wait_send())

    reach = l0.ny + l0.wide

    def fine_copies():
        got = []

        def add(sends, arrives, src, dst, arrival, k, theirs, **to):
            made = [pltpu.make_async_remote_copy(
                src_ref=a, dst_ref=b, send_sem=fine_s.at[k], recv_sem=fine_r.at[r], device_id=to, device_id_type=MESH)
                for a, b, r in ((src, dst, theirs[0]), (arrival, arrival, theirs[1]))]
            got.append((sends, arrives, *made))
        n = 0
        for z_side, z_step in enumerate((-1, 1)):
            for y_side, y_step in enumerate((-1, 1)):
                edge = pl.ds(0 if y_step < 0 else chip_y - l0.wide, l0.wide)
                to_z = jnp.logical_and(inside(y_step, cy, n_y), inside(z_step, cz, n_z))
                in_z = jnp.logical_and(has_outer, inside(z_step, cz, n_z))
                add(to_z, in_z, send_z.at[z_side, edge], recv_d.at[1 - z_side, cx], recv_d.at[z_side, y_side], n,
                    (8 + 2 * (1 - z_side) + cx, 8 + 2 * z_side + y_side), sx=1 - y_side, sy=cy + y_step, sz=cz + z_step)
                n += 1
        for z_side, z_step in enumerate((-1, 1)):
            for core in range(n_x):
                there = inside(z_step, cz, n_z)
                add(there, there, send_z.at[z_side, pl.ds(core * (chip_y - reach), reach)], recv_z.at[1 - z_side, cx],
                    recv_z.at[z_side, core], n, (12 + 2 * (1 - z_side) + cx, 12 + 2 * z_side + core), sx=core, sz=cz + z_step)
                n += 1
        return got

    def row_copies():
        got = []
        for y_side, y_step in enumerate((-1, 1)):
            edge = pl.ds(0 if y_step < 0 else chip_y - l0.wide, l0.wide)
            for k, (stage, buf) in enumerate(((stage_u, recv_yu), (stage_f, recv_yf))):
                made = [pltpu.make_async_remote_copy(
                    src_ref=a, dst_ref=b, send_sem=fine_s.at[8 + 2 * y_side + k], recv_sem=fine_r.at[2 * r + k],
                    device_id={'sx': 1 - y_side, 'sy': cy + y_step}, device_id_type=MESH)
                    for a, b, r in ((stage.at[edge, inner], buf.at[cx], cx), (buf.at[y_side], buf.at[y_side], y_side))]
                got.append((inside(y_step, cy, n_y), has_outer, *made))
        return got

    chunk = reach // PARTS

    def partner_copies(part):
        other = pl.ds((1 - cx) * (chip_y - reach) + part * chunk, chunk)
        return [pltpu.make_async_remote_copy(
            src_ref=stage.at[other, inner], dst_ref=buf.at[pl.ds(part * chunk, chunk)], send_sem=part_s.at[part, k],
            recv_sem=part_r.at[part, k], device_id={'sx': 1 - cx}, device_id_type=MESH)
            for k, (stage, buf) in enumerate(((stage_u, part_u), (stage_f, part_f)))]

    def begin(copies):
        for sends, _, copy, _ in copies:
            @pl.when(sends)
            def _(copy=copy):
                copy.start()

    def arrive(copies):
        for _, arrives, _, copy in copies:
            @pl.when(arrives)
            def _(copy=copy):
                copy.wait_recv()

    def finish(copies):
        for sends, _, copy, _ in copies:
            @pl.when(sends)
            def _(copy=copy):
                copy.wait_send()

    @pl.when(jnp.logical_not(has_outer))
    def _():
        for buf in (recv_yu, recv_yf, recv_d):
            for k in range(2):
                zero(buf.at[k])
    for z_side, z_step in enumerate((-1, 1)):
        @pl.when(jnp.logical_not(inside(z_step, cz, n_z)))
        def _(z_side=z_side):
            for core in range(n_x):
                zero(recv_z.at[z_side, core])
            zero(recv_d.at[z_side])
    for index in (1, 2):
        for d in SIDES:
            @pl.when(jnp.logical_not(exists(d)))
            def _(index=index, d=d):
                zero(region(index, d, False))

    for lv, arrays in ((l0, (u0, v0)), (l1, (a1, b1)), (l2, (a2, b2))):
        for arr in arrays:
            for plane, outside in ((lv.hx - 1, yb == 0), (lv.hx + lv.ny, yb == row_blocks - 1)):
                @pl.when(outside)
                def _(arr=arr, lv=lv, plane=plane):
                    put(arr, plane, lv.all, [jnp.zeros((lv.rows, LANES), F32)] * lv.parts)

    for lv, table in zip(levels, masks):
        shape = (lv.rows, LANES)
        z = rows_of(shape) + (lv.top - lv.z0) + cz * lv.nz
        ok = (z >= 0) & (z < n_z * lv.nz) & (lanes_of(shape) < lv.nx)
        table[0] = jnp.zeros(shape, F32)
        table[1] = jnp.where(ok, 1.0, 0.0).astype(F32)
        table[2] = jnp.where(ok, NINTH, 0.0).astype(F32)

    def valid(lv, p):
        y = p + (yb * lv.ny - lv.hx)
        return flag((y >= 0) & (y < row_blocks * lv.ny))

    middle = LANES // 2

    def lower(shape, core):
        return lanes_of(shape) // middle == core

    def split_x(first, second, core):
        lane = lanes_of(first.shape)
        pair = 2 * (lane % middle)
        first, second = pick(first, pair + (lane // middle + core) % 2), pick(second, pair + (lane // middle + 1 - core) % 2)
        here = lower(first.shape, core)
        return [jnp.where(here, first, second), roll(jnp.where(here, second, first), middle)]

    def merge_x(even, odd, core):
        lane = lanes_of(even.shape)
        odd = roll(odd, middle)
        here = lower(even.shape, core)
        spot = lane // 2 + middle * ((lane + core) % 2)
        return pick(jnp.where(here, even, odd), spot), pick(jnp.where(here, odd, even), (spot + middle) % LANES)
    pl.semaphore_wait(barrier, len(around_me))

    def across(c, lv):
        if lv.parts > 1:
            even, odd = c
            return [odd + from_below(odd), even + from_above(even)]
        if lv.nx == LANES:
            return [from_below(c[0]) + from_above(c[0])]
        return [roll(c[0], 1) + roll(c[0], LANES - 1)]

    def neighbours(src, p, xm, c, xp, lv, top, n):
        zm, zp = get(src, p, pl.ds(top - 1, n), lv), get(src, p, pl.ds(top + 1, n), lv)
        return every(lambda a, b, d, e, f: ((a + b) + (d + e)) + f, xm, xp, zm, zp, across(c, lv))

    def table_rows(table, k, lv, top, n):
        return table[k, pl.ds(top - lv.top, n)]

    def sweep(src, dst, rhs_ref, lv, table, scale=None):
        @pl.loop(0, lv.count)
        def _(g):
            base = lv.begin + g * lv.group
            for top, n in lv.blocks:
                rows = pl.ds(top, n)
                xm, c = get(src, base - 1, rows, lv), get(src, base, rows, lv)
                for j in range(lv.group):
                    p = base + j
                    xp = get(src, p + 1, rows, lv)
                    t = every(lambda a, b: a + 3.0 * b, neighbours(src, p, xm, c, xp, lv, top, n), c)
                    if scale is not None:
                        t = [x * scale for x in t]
                    keep = table_rows(table, 2 * valid(lv, p), lv, top, n)
                    put(dst, p, rows, every(lambda a, b: (a + b) * keep, t, get(rhs_ref, p, rows, lv)))
                    xm, c = c, xp

    def first_sweep(dst, rhs_ref, lv, table):
        @pl.loop(0, lv.count)
        def _(g):
            for j in range(lv.group):
                p = lv.begin + g * lv.group + j
                dst[p, 0, lv.all] = rhs_ref[p, 0, lv.all] * table[2 * valid(lv, p)]

    def restrict_planes(src, rhs_ref, lv, table, group):
        def res(p, xm, c, xp, top, n):
            return every(lambda a, b, d: a + b - 6.0 * d, neighbours(src, p, xm, c, xp, lv, top, n), get(rhs_ref, p, pl.ds(top, n), lv), c)

        @pl.loop(0, lv.ny // 2 // group)
        def _(i):
            for top, n in lv.blocks:
                rows = pl.ds(top, n)
                p = lv.hx + 2 * group * i
                xm, c = get(src, p - 1, rows, lv), get(src, p, rows, lv)
                prev = res(p - 1, get(src, p - 2, rows, lv), xm, c, top, n)
                prev = [jnp.where((yb > 0) | (i > 0), x, 0.0) for x in prev]
                keep = table_rows(table, 1, lv, top, n)
                for j in range(group):
                    x1, x2 = get(src, p + 1, rows, lv), get(src, p + 2, rows, lv)
                    even = res(p, xm, c, x1, top, n)
                    odd = res(p + 1, c, x1, x2, top, n)
                    for h in range(lv.parts):
                        pb[h, i * group + j, rows] = ((prev[h] + odd[h]) + (even[h] + even[h])) * keep
                    prev, xm, c, p = odd, x1, x2, p + 2

    def restricted_rows(i, lv, h=0):
        half = lv.nz // 2
        return ((pb[h, i, pl.ds(lv.z0 - 1, half, stride=2)] + pb[h, i, pl.ds(lv.z0 + 1, half, stride=2)])
                + 2.0 * pb[h, i, pl.ds(lv.z0, half, stride=2)])

    def weights(near, one, other):
        return jnp.where(near == 0, one, jnp.where((near == 1) | (near == -1), other, 0.0)).astype(F32)

    square = (LANES, LANES)
    eighth = 1.0 / (TILE * TILE)

    def restrict_level(src, rhs_ref, lv, table, coarse_rhs, coarse, group, step):
        restrict_planes(src, rhs_ref, lv, table, group)
        lane = lanes_of(square)
        w = jnp.where(lane < coarse.nx, weights(rows_of(square) - 2 * lane, 2.0 * eighth, eighth), 0.0)

        @pl.loop(0, coarse.ny // step)
        def _(i):
            got = [restricted_rows(i * step + j, lv) for j in range(step)]
            if lv.parts > 1:
                odds = [restricted_rows(i * step + j, lv, 1) for j in range(step)]
                got = [((odd + from_below(odd)) + 2.0 * even) * eighth for even, odd in zip(got, odds)]
            else:
                got = dot(stack(got), w)
                got = [got[j * coarse.nz:(j + 1) * coarse.nz] for j in range(step)]
            for j in range(step):
                coarse_rhs[coarse.hx + i * step + j, 0, coarse.own] = got[j]

    def prolong_planes(e, first, e_z0, e_top, e_rows, e_nx, chunk, n_chunks, lv):
        lane, below = lanes_of(square), rows_of(square)
        w = jnp.where(below < e_nx, weights(lane - 2 * below, 4.0, 2.0), 0.0)
        row = e_z0 - e_top - (lv.z0 - lv.top) // 2
        n = lv.rows // 2

        @pl.loop(0, n_chunks)
        def _(i):
            planes = pl.ds(first + i * chunk, chunk)
            got = e[planes, 0, pl.ds(e_top, e_rows)]
            if lv.parts == 1:
                got = dot(got.reshape(chunk * e_rows, LANES), w).reshape(chunk, e_rows, LANES)
            else:
                got = got * 4.0
            pz[pl.ds(i * chunk, chunk), pl.ds(0, e_rows)] = got

        @pl.loop(0, n_chunks)
        def _(i):
            for j in range(chunk):
                a = pz[i * chunk + j, pl.ds(row, n)]
                b = pz[i * chunk + j, pl.ds(row + 1, n)]
                pb[0, i * chunk + j, pl.ds(lv.top, n, stride=2)] = a
                pb[0, i * chunk + j, pl.ds(lv.top + 1, n, stride=2)] = 0.5 * (a + b)

    def correct(dst, lv, table, pairs):
        def load(at, rows):
            a = pb[0, at, rows]
            return [a, 0.5 * (a + from_above(a))] if lv.parts > 1 else [a]

        @pl.loop(0, lv.group * lv.count // (2 * pairs))
        def _(i):
            for top, n in lv.blocks:
                rows = pl.ds(top, n)
                a = load(i * pairs, rows)
                for j in range(pairs):
                    b = load(i * pairs + j + 1, rows)
                    p = lv.begin + 2 * (pairs * i + j)
                    between = every(lambda x, y: 0.5 * (x + y), a, b)
                    for q, add in ((p, a), (p + 1, between)):
                        keep = table_rows(table, valid(lv, q), lv, top, n)
                        put(dst, q, rows, every(lambda x, y: (x + y) * keep, get(dst, q, rows, lv), add))
                    a = b

    row_halo, halo = row_copies(), fine_copies()
    for copy in loads[:4]:
        copy.wait()
    half = TILE // 2
    upper = rows_of((TILE, LANES)) >= half

    @pl.loop(0, chip_y // TILE)
    def _(i):
        for j in range(TILE):
            y = i * TILE + j
            for side, row in enumerate((TILE, TILE + l0.nz - half)):
                send_z[side, y] = jnp.where(upper, stage_f[y, pl.ds(row - half, TILE)], stage_u[y, pl.ds(row, TILE)])
    begin(halo[4:])
    for copy in loads[4:]:
        copy.wait()
    for part in range(PARTS):
        for copy in partner_copies(part):
            copy.start()
    begin(row_halo)
    begin(halo[:4])
    for offset in around_me:
        pl.semaphore_signal(ready, inc=1, device_id=peer(offset), device_id_type=MESH)

    step = 4
    some = reach // 3

    @pl.loop(0, PARTS)
    def _(part):
        for copy in partner_copies(part):
            copy.wait_recv()

        @pl.loop(0, chunk // step)
        def _(i):
            for j in range(step):
                k = part * chunk + i * step + j
                for stage, buf, dst in ((stage_u, part_u, u0), (stage_f, part_f, f0)):
                    put(dst, l0.hx - cx * l0.wide + k, l0.own, split_x(stage[cx * (chip_y - reach) + k, inner], buf[k], cx))
    arrive(row_halo)
    outer_plane = l0.hx - l0.wide + cx * reach

    for buf, dst in ((recv_yu, u0), (recv_yf, f0)):
        for j in range(l0.wide):
            put(dst, outer_plane + j, l0.own, split_x(buf[0, j], buf[1, j], 0))
    arrive(halo)
    finish(row_halo)
    finish(halo)
    for part in range(PARTS):
        for copy in partner_copies(part):
            copy.wait_send()

    def put_rows(p, side, buf, k):
        row = l0.z0 + l0.nz if side else l0.z0 - half
        for h, part in enumerate(split_x(buf[0, k], buf[1, k], 0)):
            pltpu.store(u0.at[p, h, pl.ds(row, TILE)], part, mask=jnp.logical_not(upper))
            pltpu.store(f0.at[p, h, pl.ds(row - half, TILE)], part, mask=upper)

    @pl.loop(0, reach // some)
    def _(i):
        for j in range(some):
            for side in range(2):
                put_rows(l0.hx - cx * l0.wide + i * some + j, side, recv_z.at[side], i * some + j)
    for side in range(2):
        for j in range(l0.wide):
            put_rows(outer_plane + j, side, recv_d.at[side], j)
    sweep(u0, v0, f0, l0, mask0, cfg.stiffness)
    sweep(v0, u0, f0, l0, mask0)
    restrict_level(u0, f0, l0, mask0, g1, l1, 4, 4)

    exchange(1)
    first_sweep(a1, g1, l1, mask1)
    sweep(a1, b1, g1, l1, mask1)
    restrict_level(b1, g1, l1, mask1, g2, l2, 8, 8)
    exchange(2)
    first_sweep(a2, g2, l2, mask2)
    sweep(a2, b2, g2, l2, mask2)

    restrict_planes(b2, g2, l2, mask2, 4)
    ny3, nz3, width = l2.ny // 2, l2.nz // 2, l2.nx // 2
    near = rows_of(square) - 2 * (lanes_of(square) % width)
    got = dot(stack([restricted_rows(j, l2) for j in range(ny3)]), weights(near, 2.0 * eighth, eighth))
    tile = (TILE, LANES)
    lane = lanes_of(tile)
    block = lane // width
    blocks = LANES // width
    packed = got[:nz3]
    for j in range(1, ny3):
        packed = jnp.where(block == j, got[j * nz3:(j + 1) * nz3], packed)
    packed = roll(packed, width * cy)
    message[...] = packed
    slot = yb * n_z + cz
    slots[slot] = packed

    def gather_copy(k, at):
        return pltpu.make_async_remote_copy(
            src_ref=message, dst_ref=slots.at[at], send_sem=all_s.at[k], recv_sem=all_r.at[at], device_id=peer(offsets[k]), device_id_type=MESH)

    pl.semaphore_wait(ready, len(around_me))
    for k in range(total - 1):
        gather_copy(k, slot).start()
    for k, offset in enumerate(offsets):
        who = peer(offset)
        gather_copy(k, (who['sy'] * n_x + who['sx']) * n_z + who['sz']).wait_recv()

    tall = nz3 * n_z
    data = pl.ds(TILE, tall)
    for which in range(2):
        for y in range(TILE):
            for at in (0, TILE + tall):
                s3[which, y, pl.ds(at, TILE)] = jnp.zeros(tile, F32)
    live = lane < width * n_y

    @pl.loop(0, n_x)
    def _(core):
        for j in range(ny3):
            for z in range(n_z):
                acc = jnp.zeros(tile, F32)
                for t in range(n_y):
                    acc = jnp.where((block + 2 * blocks - t - j) % blocks == 0, slots[(t * n_x + core) * n_z + z], acc)
                acc = jnp.where(live, roll(acc, back(width * j)), 0.0)
                rows = pl.ds(TILE + nz3 * z, nz3)
                g3[core * ny3 + j, rows] = acc
                s3[0, core * ny3 + j, rows] = acc * NINTH

    long = (tall, LANES)
    along = lanes_of(long)
    x_first, x_last = along % width == 0, along % width == width - 1
    y_first, y_last = along < width, along >= width * (n_y - 1)

    def coarse_sweep(k, carry):
        old, new = k % 2, (k + 1) % 2
        lowest, highest = s3[old, 0, data], s3[old, TILE - 1, data]
        c = lowest
        ym = jnp.where(y_first, 0.0, roll(highest, width % LANES))
        beyond = jnp.where(y_last, 0.0, roll(lowest, back(width)))
        for y in range(TILE):
            yp = s3[old, y + 1, data] if y < TILE - 1 else beyond
            around = (ym + yp) + (s3[old, y, pl.ds(TILE - 1, tall)] + s3[old, y, pl.ds(TILE + 1, tall)])
            left = jnp.where(x_first, 0.0, roll(c, 1))
            right = jnp.where(x_last, 0.0, roll(c, LANES - 1))
            s3[new, y, data] = (around + (left + right) + 3.0 * c + g3[y, data]) * NINTH
            ym, c = c, yp
        return carry
    lax.fori_loop(0, COARSE_SWEEPS - 1, coarse_sweep, 0)

    first = (l2.begin - l2.hx) // 2
    for i in range(e3.shape[0]):
        y = yb * ny3 + (i + first)
        c = s3[(COARSE_SWEEPS - 1) % 2, (y + TILE) % TILE, pl.ds(pl.multiple_of(cz * nz3, TILE), 3 * TILE)]
        ok = (lanes_of(c.shape) < width) & (y >= 0) & (y < row_blocks * ny3)
        e3[i, 0] = jnp.where(ok, roll(c, back((y + TILE) // TILE * width + LANES - width)), 0.0)

    prolong_planes(e3, 0, TILE, 0, 3 * TILE, width, 6, 2, l2)
    correct(b2, l2, mask2, 5)
    sweep(b2, a2, g2, l2, mask2)
    sweep(a2, b2, g2, l2, mask2)
    prolong_planes(b2, l2.hx + (l1.begin - l1.hx) // 2, l2.z0, l2.top, l2.rows, l2.nx, 8, 2, l1)
    correct(b1, l1, mask1, 7)
    sweep(b1, a1, g1, l1, mask1)
    sweep(a1, b1, g1, l1, mask1)
    prolong_planes(b1, l1.hx + (l0.begin - l0.hx) // 2, l1.z0, l1.top, l1.rows, l1.nx, 8, 3, l0)
    correct(u0, l0, mask0, 4)
    sweep(u0, v0, f0, l0, mask0)

    def results(i):
        here, there = pl.ds(i * step, step), pl.ds(cx * l0.ny + i * step, step)
        return pltpu.make_async_remote_copy(
            src_ref=stage_f.at[here, inner], dst_ref=out.at[there], send_sem=out_sem.at[0, i], recv_sem=out_sem.at[1, i],
            device_id={'sx': 1 - cx}, device_id_type=MESH)

    @pl.loop(0, l0.ny // step)
    def _(i):
        for j in range(step):
            k = i * step + j
            p = l0.hx + k
            c = get(v0, p, l0.own, l0)
            around = neighbours(v0, p, get(v0, p - 1, l0.own, l0), c, get(v0, p + 1, l0.own, l0), l0, l0.z0, l0.nz)
            got = every(lambda x, y, g: (x + 3.0 * y + g) * (NINTH / cfg.stiffness), around, c, get(f0, p, l0.own, l0))
            out[cx * l0.ny + k], stage_f[k, inner] = merge_x(*got, cx)
        results(i).start()

    @pl.loop(0, l0.ny // step)
    def _(i):
        results(i).wait()
    drain(1)
    drain(2)

    for k in range(total - 1):
        gather_copy(k, slot).wait_send()


def write_out(held, out, sem):
    pltpu.make_async_copy(held, out, sem).start()
    pltpu.make_async_copy(held, out, sem).wait()


def local_cycle(rhs, start, counts, size):
    rhs, start = (jnp.transpose(x, (1, 2, 0)) for x in (rhs, start))
    n_x, n_y, n_z = counts
    chip_y, nz, nx = rhs.shape
    shapes = [(chip_y // n_x >> k, nz >> k, nx * n_x >> k) for k in range(3)]
    l0 = make_level(shapes[0], 6, 8, 4, nz + 8, 2, 8, (shapes[0][0] + 8) // 8, 4, 24)
    l1 = make_level(shapes[1], 8, 16, 8, shapes[1][1] + 16, 2, 14, (shapes[1][0] + 12) // 14, 5, 24)
    l2 = make_level(shapes[2], 8, 16, 8, shapes[2][1] + 16, 2, 10, (shapes[2][0] + 12) // 10, 6, 32)
    cfg = types.SimpleNamespace(levels=(l0, l1, l2), counts=counts, stiffness=float((size + 1) ** 2))
    total = n_x * n_y * n_z

    def vmem(*shape):
        return pltpu.VMEM(shape, F32)

    scratch = [vmem(lv.planes, lv.parts, lv.depth, LANES) for lv in (l0, l1, l2) for _ in range(3)]
    reach = l0.ny + l0.wide
    scratch += [vmem(12, 1, 3 * TILE, LANES), vmem(l1.ny + 8, l1.rows, LANES), vmem(2, l1.ny + 8, l0.depth, LANES)]
    scratch += [vmem(chip_y, l0.depth, LANES)] * 2 + [vmem(reach, nz, LANES)] * 2
    scratch += [vmem(2, TILE, l2.nz // 2 * n_z + 2 * TILE, LANES), vmem(TILE, l2.nz // 2 * n_z + 2 * TILE, LANES), vmem(total, TILE, LANES), vmem(TILE, LANES)]
    scratch += [vmem(3, lv.rows, LANES) for lv in (l0, l1, l2)]
    scratch += [vmem(2, chip_y, TILE, LANES), vmem(2, n_x, reach, TILE, LANES), vmem(2, 2, l0.wide, TILE, LANES)]
    scratch += [vmem(2, l0.wide, nz, LANES)] * 2
    sems = [(10,), (2, l0.ny // 4), (16,), (16,), (2, len(SIDES)), (2, len(SIDES)), (total,), (total,), (PARTS, 2), (PARTS, 2)]
    scratch += [pltpu.SemaphoreType.DMA(shape) for shape in sems] + [pltpu.SemaphoreType.REGULAR]
    got = pl.pallas_call(
        functools.partial(kernel, cfg),
        out_shape=pltpu.VMEM(rhs.shape, F32),
        in_specs=[pl.BlockSpec(memory_space=pl.ANY)] * 2,
        out_specs=pl.BlockSpec(memory_space=pltpu.VMEM),
        scratch_shapes=scratch,
        compiler_params=pltpu.CompilerParams(collective_id=0, has_side_effects=True, vmem_limit_bytes=60 * 2 ** 20),
    )(rhs, start)
    got = pl.pallas_call(
        write_out,
        out_shape=jax.ShapeDtypeStruct(rhs.shape, F32),
        in_specs=[pl.BlockSpec(memory_space=pltpu.VMEM)],
        out_specs=pl.BlockSpec(memory_space=pl.ANY),
        scratch_shapes=[pltpu.SemaphoreType.DMA],
    )(pltpu.with_memory_space_constraint(got, pltpu.VMEM))
    return jnp.transpose(got, (2, 0, 1))


def solution(mesh):
    counts = (mesh.shape['sx'], mesh.shape['sy'], mesh.shape['sz'])
    spec = P(('dp', 'sx'), 'sy', 'sz')

    def run(rhs_grid, u_start):
        size = rhs_grid.shape[0] // mesh.shape['dp']
        cycle = functools.partial(local_cycle, counts=counts, size=size)
        return jax.shard_map(cycle, mesh=mesh, in_specs=(spec, spec), out_specs=spec, check_vma=False)(rhs_grid, u_start)
    return run
```

```python
import functools
import types
import jax
import jax.numpy as jnp
from jax import lax
from jax.experimental import pallas as pl
from jax.experimental.pallas import tpu as pltpu
from jax.sharding import PartitionSpec as P

F32 = jnp.float32
MESH = pl.DeviceIdType.MESH
LANES = 128
TILE = 8
NINTH = 1.0 / 9.0
COARSE_SWEEPS = 16
PARTS = 3
OPPOSITE = (1, 0, 3, 2, 7, 6, 5, 4)
STEP_Y = (-1, 1, 0, 0, -1, -1, 1, 1)
STEP_Z = (0, 0, -1, 1, -1, 1, -1, 1)
SIDES = range(len(STEP_Y))


def make_level(shape, hx, z0, top, rows, begin, group, count, wide, block):
    ny, nz, nx = shape
    lv = types.SimpleNamespace(ny=ny, nz=nz, nx=nx, hx=hx, z0=z0, top=top, rows=rows, begin=begin, group=group, count=count, wide=wide)
    lv.planes = ny + 2 * hx
    lv.depth = nz + 2 * z0
    lv.parts = max(nx // LANES, 1)
    lv.own = pl.ds(z0, nz)
    lv.all = pl.ds(top, rows)
    lv.blocks = [(top + i, min(block, rows - i)) for i in range(0, rows, block)]
    return lv


def lanes_of(shape):
    return lax.broadcasted_iota(jnp.int32, shape, len(shape) - 1)


def rows_of(shape):
    return lax.broadcasted_iota(jnp.int32, shape, len(shape) - 2)


def roll(x, shift):
    return pltpu.roll(x, shift, 1)


def from_below(x):
    return jnp.where(lanes_of(x.shape) == 0, 0.0, roll(x, 1))


def from_above(x):
    return jnp.where(lanes_of(x.shape) == LANES - 1, 0.0, roll(x, LANES - 1))


def halves(x):
    return x[:, :LANES], x[:, LANES:]


def get(ref, p, rows, lv):
    return [ref[p, h, rows] for h in range(lv.parts)]


def put(ref, p, rows, values):
    for h, value in enumerate(values):
        ref[p, h, rows] = value


def every(f, *lists):
    return [f(*values) for values in zip(*lists)]


def join(*parts):
    return jnp.concatenate(parts, axis=1)


def stack(parts):
    return jnp.concatenate(parts, axis=0)


def back(shift):
    return (4 * LANES - shift) % LANES


def flag(condition):
    return jnp.where(condition, 1, 0)


def pick(x, index):
    return jnp.take_along_axis(x, index, axis=1, mode='promise_in_bounds')


def dot(x, w):
    return jnp.dot(x, w, precision=lax.Precision.HIGHEST, preferred_element_type=F32)


def kernel(cfg, rhs, start, out, *scratch):
    (u0, v0, f0, a1, b1, g1, a2, b2, g2, e3, pz, pb, stage_u, stage_f, part_u, part_f, s3, g3, slots, message, mask0, mask1, mask2,
     send_z, recv_z, recv_d, recv_yu, recv_yf,
     load_sem, out_sem, fine_s, fine_r, send_sem, recv_sem, all_s, all_r, part_s, part_r, ready) = scratch
    l0, l1, l2 = levels = cfg.levels
    masks = (mask0, mask1, mask2)
    n_x, n_y, n_z = cfg.counts
    cx, cy, cz = lax.axis_index('sx'), lax.axis_index('sy'), lax.axis_index('sz')
    total = n_x * n_y * n_z
    row_blocks = n_x * n_y
    yb = cy * n_x + cx

    inner = pl.ds(TILE, l0.nz)
    chip_y = n_x * l0.ny

    def load(planes, rows):
        shifted = pl.ds(rows.start + TILE, rows.size)
        k = len(loads)
        loads.append(pltpu.make_async_copy(start.at[planes, rows], stage_u.at[planes, shifted], load_sem.at[k]))
        loads.append(pltpu.make_async_copy(rhs.at[planes, rows], stage_f.at[planes, shifted], load_sem.at[k + 1]))
    loads = []
    between = pl.ds(TILE, l0.nz - 2 * TILE)
    for row in (0, l0.nz - TILE):
        load(pl.ds(0, chip_y), pl.ds(row, TILE))
    for plane in (0, chip_y - l0.wide):
        load(pl.ds(plane, l0.wide), between)
    load(pl.ds(l0.wide, chip_y - 2 * l0.wide), between)
    for copy in loads:
        copy.start()

    offsets = [(dz, dy, dx) for dz in range(n_z) for dy in range(n_y) for dx in range(n_x)][1:]
    offsets.sort(key=lambda o: -2 * (min(o[0], n_z - o[0]) + min(o[1], n_y - o[1])) - o[2])

    def peer(offset):
        return {name: lax.rem(at + d, n) for name, at, n, d in zip(('sz', 'sy', 'sx'), (cz, cy, cx), (n_z, n_y, n_x), offset)}

    def inside(step, at, count):
        if step == 0:
            return True
        return at > 0 if step < 0 else at < count - 1

    around_me = [o for o in offsets if o[0] in (0, 1, n_z - 1) and o[1] in (0, 1, n_y - 1)]
    barrier = pltpu.get_barrier_semaphore()
    for offset in around_me:
        pl.semaphore_signal(barrier, inc=1, device_id=peer(offset), device_id_type=MESH)
    outer = 2 * cx - 1
    has_outer = (cy + outer >= 0) & (cy + outer < n_y)

    def exists(d):
        return jnp.logical_and(inside(STEP_Y[d], yb, row_blocks), inside(STEP_Z[d], cz, n_z))

    def zero(ref):
        @pl.loop(0, ref.shape[0])
        def _(i):
            ref[i] = jnp.zeros(ref.shape[1:], F32)

    def span(step, first, n, wide, own):
        if step == 0:
            return pl.ds(first, n)
        if step < 0:
            return pl.ds(first if own else first - wide, wide)
        return pl.ds(first + n - wide if own else first + n, wide)

    def region(index, d, own):
        lv, arr = levels[index], (None, g1, g2)[index]
        return arr.at[span(STEP_Y[d], lv.hx, lv.ny, lv.wide, own), 0, span(STEP_Z[d], lv.z0, lv.nz, TILE, own)]

    def halo_copy(index, d, arriving):
        k = index - 1
        at = yb + STEP_Y[d]
        return pltpu.make_async_remote_copy(
            src_ref=region(index, d, not arriving), dst_ref=region(index, d if arriving else OPPOSITE[d], False),
            send_sem=send_sem.at[k, d], recv_sem=recv_sem.at[k, d if arriving else OPPOSITE[d]],
            device_id={'sx': at % n_x, 'sy': at // n_x, 'sz': cz + STEP_Z[d]}, device_id_type=MESH)

    def each(act):
        for d in (4, 5, 6, 7, 2, 3, 0, 1):
            @pl.when(exists(d))
            def _(d=d):
                act(d)

    def exchange(index):
        each(lambda d: halo_copy(index, d, False).start())
        each(lambda d: halo_copy(index, d, True).wait_recv())

    def drain(index):
        each(lambda d: halo_copy(index, d, False).wait_send())

    reach = l0.ny + l0.wide

    def fine_copies():
        got = []

        def add(sends, arrives, src, dst, arrival, k, theirs, **to):
            made = [pltpu.make_async_remote_copy(
                src_ref=a, dst_ref=b, send_sem=fine_s.at[k], recv_sem=fine_r.at[r], device_id=to, device_id_type=MESH)
                for a, b, r in ((src, dst, theirs[0]), (arrival, arrival, theirs[1]))]
            got.append((sends, arrives, *made))
        n = 0
        for z_side, z_step in enumerate((-1, 1)):
            for y_side, y_step in enumerate((-1, 1)):
                edge = pl.ds(0 if y_step < 0 else chip_y - l0.wide, l0.wide)
                to_z = jnp.logical_and(inside(y_step, cy, n_y), inside(z_step, cz, n_z))
                in_z = jnp.logical_and(has_outer, inside(z_step, cz, n_z))
                add(to_z, in_z, send_z.at[z_side, edge], recv_d.at[1 - z_side, cx], recv_d.at[z_side, y_side], n,
                    (8 + 2 * (1 - z_side) + cx, 8 + 2 * z_side + y_side), sx=1 - y_side, sy=cy + y_step, sz=cz + z_step)
                n += 1
        for z_side, z_step in enumerate((-1, 1)):
            for core in range(n_x):
                there = inside(z_step, cz, n_z)
                add(there, there, send_z.at[z_side, pl.ds(core * (chip_y - reach), reach)], recv_z.at[1 - z_side, cx],
                    recv_z.at[z_side, core], n, (12 + 2 * (1 - z_side) + cx, 12 + 2 * z_side + core), sx=core, sz=cz + z_step)
                n += 1
        return got

    def row_copies():
        got = []
        for y_side, y_step in enumerate((-1, 1)):
            edge = pl.ds(0 if y_step < 0 else chip_y - l0.wide, l0.wide)
            for k, (stage, buf) in enumerate(((stage_u, recv_yu), (stage_f, recv_yf))):
                made = [pltpu.make_async_remote_copy(
                    src_ref=a, dst_ref=b, send_sem=fine_s.at[8 + 2 * y_side + k], recv_sem=fine_r.at[2 * r + k],
                    device_id={'sx': 1 - y_side, 'sy': cy + y_step}, device_id_type=MESH)
                    for a, b, r in ((stage.at[edge, inner], buf.at[cx], cx), (buf.at[y_side], buf.at[y_side], y_side))]
                got.append((inside(y_step, cy, n_y), has_outer, *made))
        return got

    chunk = reach // PARTS

    def partner_copies(part):
        other = pl.ds((1 - cx) * (chip_y - reach) + part * chunk, chunk)
        return [pltpu.make_async_remote_copy(
            src_ref=stage.at[other, inner], dst_ref=buf.at[pl.ds(part * chunk, chunk)], send_sem=part_s.at[part, k],
            recv_sem=part_r.at[part, k], device_id={'sx': 1 - cx}, device_id_type=MESH)
            for k, (stage, buf) in enumerate(((stage_u, part_u), (stage_f, part_f)))]

    def begin(copies):
        for sends, _, copy, _ in copies:
            @pl.when(sends)
            def _(copy=copy):
                copy.start()

    def arrive(copies):
        for _, arrives, _, copy in copies:
            @pl.when(arrives)
            def _(copy=copy):
                copy.wait_recv()

    def finish(copies):
        for sends, _, copy, _ in copies:
            @pl.when(sends)
            def _(copy=copy):
                copy.wait_send()

    @pl.when(jnp.logical_not(has_outer))
    def _():
        for buf in (recv_yu, recv_yf, recv_d):
            for k in range(2):
                zero(buf.at[k])
    for z_side, z_step in enumerate((-1, 1)):
        @pl.when(jnp.logical_not(inside(z_step, cz, n_z)))
        def _(z_side=z_side):
            for core in range(n_x):
                zero(recv_z.at[z_side, core])
            zero(recv_d.at[z_side])
    for index in (1, 2):
        for d in SIDES:
            @pl.when(jnp.logical_not(exists(d)))
            def _(index=index, d=d):
                zero(region(index, d, False))

    for lv, arrays in ((l0, (u0, v0)), (l1, (a1, b1)), (l2, (a2, b2))):
        for arr in arrays:
            for plane, outside in ((lv.hx - 1, yb == 0), (lv.hx + lv.ny, yb == row_blocks - 1)):
                @pl.when(outside)
                def _(arr=arr, lv=lv, plane=plane):
                    put(arr, plane, lv.all, [jnp.zeros((lv.rows, LANES), F32)] * lv.parts)

    for lv, table in zip(levels, masks):
        shape = (lv.rows, LANES)
        z = rows_of(shape) + (lv.top - lv.z0) + cz * lv.nz
        ok = (z >= 0) & (z < n_z * lv.nz) & (lanes_of(shape) < lv.nx)
        table[0] = jnp.zeros(shape, F32)
        table[1] = jnp.where(ok, 1.0, 0.0).astype(F32)
        table[2] = jnp.where(ok, NINTH, 0.0).astype(F32)

    def valid(lv, p):
        y = p + (yb * lv.ny - lv.hx)
        return flag((y >= 0) & (y < row_blocks * lv.ny))

    middle = LANES // 2

    def towards(core):
        return 1 + (LANES - 2) * core

    def split_x(first, second, core):
        lane = lanes_of(first.shape)
        near, far = roll(second, towards(core)), roll(first, towards(1 - core))
        spot = 2 * (lane % middle) + lane // middle
        return [pick(jnp.where(lane % 2 == core, first, near), spot), pick(jnp.where(lane % 2 == core, far, second), spot)]

    def merge_x(first, second, core):
        lane = lanes_of(first.shape)
        spot = lane // 2 + middle * (lane % 2)
        first, second = pick(first, spot), pick(second, spot)
        return (jnp.where(lane % 2 == core, first, roll(second, towards(core))),
                jnp.where(lane % 2 == core, roll(first, towards(1 - core)), second))

    pl.semaphore_wait(barrier, len(around_me))

    def across(c, lv):
        if lv.parts > 1:
            even, odd = c
            return [odd + from_below(odd), even + from_above(even)]
        if lv.nx == LANES:
            return [from_below(c[0]) + from_above(c[0])]
        return [roll(c[0], 1) + roll(c[0], LANES - 1)]

    def neighbours(src, p, xm, c, xp, lv, top, n):
        zm, zp = get(src, p, pl.ds(top - 1, n), lv), get(src, p, pl.ds(top + 1, n), lv)
        return every(lambda a, b, d, e, f: ((a + b) + (d + e)) + f, xm, xp, zm, zp, across(c, lv))

    def table_rows(table, k, lv, top, n):
        return table[k, pl.ds(top - lv.top, n)]

    def sweep(src, dst, rhs_ref, lv, table, scale=None):
        @pl.loop(0, lv.count)
        def _(g):
            base = lv.begin + g * lv.group
            for top, n in lv.blocks:
                rows = pl.ds(top, n)
                xm, c = get(src, base - 1, rows, lv), get(src, base, rows, lv)
                for j in range(lv.group):
                    p = base + j
                    xp = get(src, p + 1, rows, lv)
                    t = every(lambda a, b: a + 3.0 * b, neighbours(src, p, xm, c, xp, lv, top, n), c)
                    if scale is not None:
                        t = [x * scale for x in t]
                    keep = table_rows(table, 2 * valid(lv, p), lv, top, n)
                    put(dst, p, rows, every(lambda a, b: (a + b) * keep, t, get(rhs_ref, p, rows, lv)))
                    xm, c = c, xp

    def first_sweep(dst, rhs_ref, lv, table):
        @pl.loop(0, lv.count)
        def _(g):
            for j in range(lv.group):
                p = lv.begin + g * lv.group + j
                dst[p, 0, lv.all] = rhs_ref[p, 0, lv.all] * table[2 * valid(lv, p)]

    def restrict_planes(src, rhs_ref, lv, table, group):
        def res(p, xm, c, xp, top, n):
            return every(lambda a, b, d: a + b - 6.0 * d, neighbours(src, p, xm, c, xp, lv, top, n), get(rhs_ref, p, pl.ds(top, n), lv), c)

        @pl.loop(0, lv.ny // 2 // group)
        def _(i):
            for top, n in lv.blocks:
                rows = pl.ds(top, n)
                p = lv.hx + 2 * group * i
                xm, c = get(src, p - 1, rows, lv), get(src, p, rows, lv)
                prev = res(p - 1, get(src, p - 2, rows, lv), xm, c, top, n)
                prev = [jnp.where((yb > 0) | (i > 0), x, 0.0) for x in prev]
                keep = table_rows(table, 1, lv, top, n)
                for j in range(group):
                    x1, x2 = get(src, p + 1, rows, lv), get(src, p + 2, rows, lv)
                    even = res(p, xm, c, x1, top, n)
                    odd = res(p + 1, c, x1, x2, top, n)
                    for h in range(lv.parts):
                        pb[h, i * group + j, rows] = ((prev[h] + odd[h]) + (even[h] + even[h])) * keep
                    prev, xm, c, p = odd, x1, x2, p + 2

    def restricted_rows(i, lv, h=0):
        half = lv.nz // 2
        return ((pb[h, i, pl.ds(lv.z0 - 1, half, stride=2)] + pb[h, i, pl.ds(lv.z0 + 1, half, stride=2)])
                + 2.0 * pb[h, i, pl.ds(lv.z0, half, stride=2)])

    def weights(near, one, other):
        return jnp.where(near == 0, one, jnp.where((near == 1) | (near == -1), other, 0.0)).astype(F32)

    square = (LANES, LANES)
    eighth = 1.0 / (TILE * TILE)

    def restrict_level(src, rhs_ref, lv, table, coarse_rhs, coarse, group, step):
        restrict_planes(src, rhs_ref, lv, table, group)
        lane = lanes_of(square)
        w = jnp.where(lane < coarse.nx, weights(rows_of(square) - 2 * lane, 2.0 * eighth, eighth), 0.0)

        @pl.loop(0, coarse.ny // step)
        def _(i):
            got = [restricted_rows(i * step + j, lv) for j in range(step)]
            if lv.parts > 1:
                odds = [restricted_rows(i * step + j, lv, 1) for j in range(step)]
                got = [((odd + from_below(odd)) + 2.0 * even) * eighth for even, odd in zip(got, odds)]
            else:
                got = dot(stack(got), w)
                got = [got[j * coarse.nz:(j + 1) * coarse.nz] for j in range(step)]
            for j in range(step):
                coarse_rhs[coarse.hx + i * step + j, 0, coarse.own] = got[j]

    def prolong_planes(e, first, e_z0, e_top, e_rows, e_nx, chunk, n_chunks, lv):
        lane, below = lanes_of(square), rows_of(square)
        w = jnp.where(below < e_nx, weights(lane - 2 * below, 4.0, 2.0), 0.0)
        row = e_z0 - e_top - (lv.z0 - lv.top) // 2
        n = lv.rows // 2

        @pl.loop(0, n_chunks)
        def _(i):
            planes = pl.ds(first + i * chunk, chunk)
            got = e[planes, 0, pl.ds(e_top, e_rows)]
            if lv.parts == 1:
                got = dot(got.reshape(chunk * e_rows, LANES), w).reshape(chunk, e_rows, LANES)
            else:
                got = got * 4.0
            pz[pl.ds(i * chunk, chunk), pl.ds(0, e_rows)] = got

        @pl.loop(0, n_chunks)
        def _(i):
            for j in range(chunk):
                a = pz[i * chunk + j, pl.ds(row, n)]
                b = pz[i * chunk + j, pl.ds(row + 1, n)]
                pb[0, i * chunk + j, pl.ds(lv.top, n, stride=2)] = a
                pb[0, i * chunk + j, pl.ds(lv.top + 1, n, stride=2)] = 0.5 * (a + b)

    def correct(dst, lv, table, pairs):
        def load(at, rows):
            a = pb[0, at, rows]
            return [a, 0.5 * (a + from_above(a))] if lv.parts > 1 else [a]

        @pl.loop(0, lv.group * lv.count // (2 * pairs))
        def _(i):
            for top, n in lv.blocks:
                rows = pl.ds(top, n)
                a = load(i * pairs, rows)
                for j in range(pairs):
                    b = load(i * pairs + j + 1, rows)
                    p = lv.begin + 2 * (pairs * i + j)
                    between = every(lambda x, y: 0.5 * (x + y), a, b)
                    for q, add in ((p, a), (p + 1, between)):
                        keep = table_rows(table, valid(lv, q), lv, top, n)
                        put(dst, q, rows, every(lambda x, y: (x + y) * keep, get(dst, q, rows, lv), add))
                    a = b

    row_halo, halo = row_copies(), fine_copies()
    for copy in loads[:4]:
        copy.wait()
    half = TILE // 2
    upper = rows_of((TILE, LANES)) >= half

    @pl.loop(0, chip_y // TILE)
    def _(i):
        for j in range(TILE):
            y = i * TILE + j
            for side, row in enumerate((TILE, TILE + l0.nz - half)):
                send_z[side, y] = jnp.where(upper, stage_f[y, pl.ds(row - half, TILE)], stage_u[y, pl.ds(row, TILE)])
    begin(halo[4:])
    for copy in loads[4:]:
        copy.wait()
    for part in range(PARTS):
        for copy in partner_copies(part):
            copy.start()
    begin(row_halo)
    begin(halo[:4])
    for offset in around_me:
        pl.semaphore_signal(ready, inc=1, device_id=peer(offset), device_id_type=MESH)

    step = 4
    some = reach // 3

    @pl.loop(0, PARTS)
    def _(part):
        for copy in partner_copies(part):
            copy.wait_recv()

        @pl.loop(0, chunk // step)
        def _(i):
            for j in range(step):
                k = part * chunk + i * step + j
                for stage, buf, dst in ((stage_u, part_u, u0), (stage_f, part_f, f0)):
                    p = l0.hx - cx * l0.wide + k
                    dst[p, cx, l0.own], dst[p, 1 - cx, l0.own] = split_x(stage[cx * (chip_y - reach) + k, inner], buf[k], cx)
    arrive(row_halo)
    outer_plane = l0.hx - l0.wide + cx * reach

    for buf, dst in ((recv_yu, u0), (recv_yf, f0)):
        for j in range(l0.wide):
            put(dst, outer_plane + j, l0.own, split_x(buf[0, j], buf[1, j], 0))
    arrive(halo)
    finish(row_halo)
    finish(halo)
    for part in range(PARTS):
        for copy in partner_copies(part):
            copy.wait_send()

    def put_rows(p, side, buf, k):
        row = l0.z0 + l0.nz if side else l0.z0 - half
        for h, part in enumerate(split_x(buf[0, k], buf[1, k], 0)):
            pltpu.store(u0.at[p, h, pl.ds(row, TILE)], part, mask=jnp.logical_not(upper))
            pltpu.store(f0.at[p, h, pl.ds(row - half, TILE)], part, mask=upper)

    @pl.loop(0, reach // some)
    def _(i):
        for j in range(some):
            for side in range(2):
                put_rows(l0.hx - cx * l0.wide + i * some + j, side, recv_z.at[side], i * some + j)
    for side in range(2):
        for j in range(l0.wide):
            put_rows(outer_plane + j, side, recv_d.at[side], j)
    sweep(u0, v0, f0, l0, mask0, cfg.stiffness)
    sweep(v0, u0, f0, l0, mask0)
    restrict_level(u0, f0, l0, mask0, g1, l1, 4, 4)

    exchange(1)
    first_sweep(a1, g1, l1, mask1)
    sweep(a1, b1, g1, l1, mask1)
    restrict_level(b1, g1, l1, mask1, g2, l2, 8, 8)
    exchange(2)
    first_sweep(a2, g2, l2, mask2)
    sweep(a2, b2, g2, l2, mask2)

    restrict_planes(b2, g2, l2, mask2, 4)
    ny3, nz3, width = l2.ny // 2, l2.nz // 2, l2.nx // 2
    near = rows_of(square) - 2 * (lanes_of(square) % width)
    got = dot(stack([restricted_rows(j, l2) for j in range(ny3)]), weights(near, 2.0 * eighth, eighth))
    tile = (TILE, LANES)
    lane = lanes_of(tile)
    block = lane // width
    blocks = LANES // width
    packed = got[:nz3]
    for j in range(1, ny3):
        packed = jnp.where(block == j, got[j * nz3:(j + 1) * nz3], packed)
    packed = roll(packed, width * cy)
    message[...] = packed
    slot = yb * n_z + cz
    slots[slot] = packed

    def gather_copy(k, at):
        return pltpu.make_async_remote_copy(
            src_ref=message, dst_ref=slots.at[at], send_sem=all_s.at[k], recv_sem=all_r.at[at], device_id=peer(offsets[k]), device_id_type=MESH)

    pl.semaphore_wait(ready, len(around_me))
    for k in range(total - 1):
        gather_copy(k, slot).start()
    for k, offset in enumerate(offsets):
        who = peer(offset)
        gather_copy(k, (who['sy'] * n_x + who['sx']) * n_z + who['sz']).wait_recv()

    tall = nz3 * n_z
    data = pl.ds(TILE, tall)
    for which in range(2):
        for y in range(TILE):
            for at in (0, TILE + tall):
                s3[which, y, pl.ds(at, TILE)] = jnp.zeros(tile, F32)
    live = lane < width * n_y

    @pl.loop(0, n_x)
    def _(core):
        for j in range(ny3):
            for z in range(n_z):
                acc = jnp.zeros(tile, F32)
                for t in range(n_y):
                    acc = jnp.where((block + 2 * blocks - t - j) % blocks == 0, slots[(t * n_x + core) * n_z + z], acc)
                acc = jnp.where(live, roll(acc, back(width * j)), 0.0)
                rows = pl.ds(TILE + nz3 * z, nz3)
                g3[core * ny3 + j, rows] = acc
                s3[0, core * ny3 + j, rows] = acc * NINTH

    long = (tall, LANES)
    along = lanes_of(long)
    x_first, x_last = along % width == 0, along % width == width - 1
    y_first, y_last = along < width, along >= width * (n_y - 1)

    def coarse_sweep(k, carry):
        old, new = k % 2, (k + 1) % 2
        lowest, highest = s3[old, 0, data], s3[old, TILE - 1, data]
        c = lowest
        ym = jnp.where(y_first, 0.0, roll(highest, width % LANES))
        beyond = jnp.where(y_last, 0.0, roll(lowest, back(width)))
        for y in range(TILE):
            yp = s3[old, y + 1, data] if y < TILE - 1 else beyond
            around = (ym + yp) + (s3[old, y, pl.ds(TILE - 1, tall)] + s3[old, y, pl.ds(TILE + 1, tall)])
            left = jnp.where(x_first, 0.0, roll(c, 1))
            right = jnp.where(x_last, 0.0, roll(c, LANES - 1))
            s3[new, y, data] = (around + (left + right) + 3.0 * c + g3[y, data]) * NINTH
            ym, c = c, yp
        return carry
    lax.fori_loop(0, COARSE_SWEEPS - 1, coarse_sweep, 0)

    first = (l2.begin - l2.hx) // 2
    for i in range(e3.shape[0]):
        y = yb * ny3 + (i + first)
        c = s3[(COARSE_SWEEPS - 1) % 2, (y + TILE) % TILE, pl.ds(pl.multiple_of(cz * nz3, TILE), 3 * TILE)]
        ok = (lanes_of(c.shape) < width) & (y >= 0) & (y < row_blocks * ny3)
        e3[i, 0] = jnp.where(ok, roll(c, back((y + TILE) // TILE * width + LANES - width)), 0.0)

    prolong_planes(e3, 0, TILE, 0, 3 * TILE, width, 6, 2, l2)
    correct(b2, l2, mask2, 5)
    sweep(b2, a2, g2, l2, mask2)
    sweep(a2, b2, g2, l2, mask2)
    prolong_planes(b2, l2.hx + (l1.begin - l1.hx) // 2, l2.z0, l2.top, l2.rows, l2.nx, 8, 2, l1)
    correct(b1, l1, mask1, 7)
    sweep(b1, a1, g1, l1, mask1)
    sweep(a1, b1, g1, l1, mask1)
    prolong_planes(b1, l1.hx + (l0.begin - l0.hx) // 2, l1.z0, l1.top, l1.rows, l1.nx, 8, 3, l0)
    correct(u0, l0, mask0, 4)
    sweep(u0, v0, f0, l0, mask0)

    def results(i):
        here, there = pl.ds(i * step, step), pl.ds(cx * l0.ny + i * step, step)
        return pltpu.make_async_remote_copy(
            src_ref=stage_f.at[here, inner], dst_ref=out.at[there], send_sem=out_sem.at[0, i], recv_sem=out_sem.at[1, i],
            device_id={'sx': 1 - cx}, device_id_type=MESH)

    @pl.loop(0, l0.ny // step)
    def _(i):
        for j in range(step):
            k = i * step + j
            p = l0.hx + k
            c = get(v0, p, l0.own, l0)
            around = neighbours(v0, p, get(v0, p - 1, l0.own, l0), c, get(v0, p + 1, l0.own, l0), l0, l0.z0, l0.nz)
            got = every(lambda x, y, g: (x + 3.0 * y + g) * (NINTH / cfg.stiffness), around, c, get(f0, p, l0.own, l0))
            got = [jnp.where(cx == 0, got[0], got[1]), jnp.where(cx == 0, got[1], got[0])]
            out[cx * l0.ny + k], stage_f[k, inner] = merge_x(*got, cx)
        results(i).start()

    @pl.loop(0, l0.ny // step)
    def _(i):
        results(i).wait()
    drain(1)
    drain(2)

    for k in range(total - 1):
        gather_copy(k, slot).wait_send()


def write_out(held, out, sem):
    pltpu.make_async_copy(held, out, sem).start()
    pltpu.make_async_copy(held, out, sem).wait()


def local_cycle(rhs, start, counts, size):
    rhs, start = (jnp.transpose(x, (1, 2, 0)) for x in (rhs, start))
    n_x, n_y, n_z = counts
    chip_y, nz, nx = rhs.shape
    shapes = [(chip_y // n_x >> k, nz >> k, nx * n_x >> k) for k in range(3)]
    l0 = make_level(shapes[0], 6, 8, 4, nz + 8, 2, 8, (shapes[0][0] + 8) // 8, 4, 24)
    l1 = make_level(shapes[1], 8, 16, 8, shapes[1][1] + 16, 2, 14, (shapes[1][0] + 12) // 14, 5, 24)
    l2 = make_level(shapes[2], 8, 16, 8, shapes[2][1] + 16, 2, 10, (shapes[2][0] + 12) // 10, 6, 32)
    cfg = types.SimpleNamespace(levels=(l0, l1, l2), counts=counts, stiffness=float((size + 1) ** 2))
    total = n_x * n_y * n_z

    def vmem(*shape):
        return pltpu.VMEM(shape, F32)

    scratch = [vmem(lv.planes, lv.parts, lv.depth, LANES) for lv in (l0, l1, l2) for _ in range(3)]
    reach = l0.ny + l0.wide
    scratch += [vmem(12, 1, 3 * TILE, LANES), vmem(l1.ny + 8, l1.rows, LANES), vmem(2, l1.ny + 8, l0.depth, LANES)]
    scratch += [vmem(chip_y, l0.depth, LANES)] * 2 + [vmem(reach, nz, LANES)] * 2
    scratch += [vmem(2, TILE, l2.nz // 2 * n_z + 2 * TILE, LANES), vmem(TILE, l2.nz // 2 * n_z + 2 * TILE, LANES), vmem(total, TILE, LANES), vmem(TILE, LANES)]
    scratch += [vmem(3, lv.rows, LANES) for lv in (l0, l1, l2)]
    scratch += [vmem(2, chip_y, TILE, LANES), vmem(2, n_x, reach, TILE, LANES), vmem(2, 2, l0.wide, TILE, LANES)]
    scratch += [vmem(2, l0.wide, nz, LANES)] * 2
    sems = [(10,), (2, l0.ny // 4), (16,), (16,), (2, len(SIDES)), (2, len(SIDES)), (total,), (total,), (PARTS, 2), (PARTS, 2)]
    scratch += [pltpu.SemaphoreType.DMA(shape) for shape in sems] + [pltpu.SemaphoreType.REGULAR]
    got = pl.pallas_call(
        functools.partial(kernel, cfg),
        out_shape=pltpu.VMEM(rhs.shape, F32),
        in_specs=[pl.BlockSpec(memory_space=pl.ANY)] * 2,
        out_specs=pl.BlockSpec(memory_space=pltpu.VMEM),
        scratch_shapes=scratch,
        compiler_params=pltpu.CompilerParams(collective_id=0, has_side_effects=True, vmem_limit_bytes=60 * 2 ** 20),
    )(rhs, start)
    got = pl.pallas_call(
        write_out,
        out_shape=jax.ShapeDtypeStruct(rhs.shape, F32),
        in_specs=[pl.BlockSpec(memory_space=pltpu.VMEM)],
        out_specs=pl.BlockSpec(memory_space=pl.ANY),
        scratch_shapes=[pltpu.SemaphoreType.DMA],
    )(pltpu.with_memory_space_constraint(got, pltpu.VMEM))
    return jnp.transpose(got, (2, 0, 1))


def solution(mesh):
    counts = (mesh.shape['sx'], mesh.shape['sy'], mesh.shape['sz'])
    spec = P(('dp', 'sx'), 'sy', 'sz')

    def run(rhs_grid, u_start):
        size = rhs_grid.shape[0] // mesh.shape['dp']
        cycle = functools.partial(local_cycle, counts=counts, size=size)
        return jax.shard_map(cycle, mesh=mesh, in_specs=(spec, spec), out_specs=spec, check_vma=False)(rhs_grid, u_start)
    return run
```

```python
import functools
import types
import jax
import jax.numpy as jnp
from jax import lax
from jax.experimental import pallas as pl
from jax.experimental.pallas import tpu as pltpu
from jax.sharding import PartitionSpec as P

F32 = jnp.float32
MESH = pl.DeviceIdType.MESH
LANES = 128
TILE = 8
NINTH = 1.0 / 9.0
COARSE_SWEEPS = 16
PARTS = 3
OPPOSITE = (1, 0, 3, 2, 7, 6, 5, 4)
STEP_Y = (-1, 1, 0, 0, -1, -1, 1, 1)
STEP_Z = (0, 0, -1, 1, -1, 1, -1, 1)
SIDES = range(len(STEP_Y))


def make_level(shape, hx, z0, top, rows, begin, group, count, wide, block):
    ny, nz, nx = shape
    lv = types.SimpleNamespace(ny=ny, nz=nz, nx=nx, hx=hx, z0=z0, top=top, rows=rows, begin=begin, group=group, count=count, wide=wide)
    lv.planes = ny + 2 * hx
    lv.depth = nz + 2 * z0
    lv.parts = max(nx // LANES, 1)
    lv.own = pl.ds(z0, nz)
    lv.all = pl.ds(top, rows)
    lv.blocks = [(top + i, min(block, rows - i)) for i in range(0, rows, block)]
    return lv


def lanes_of(shape):
    return lax.broadcasted_iota(jnp.int32, shape, len(shape) - 1)


def rows_of(shape):
    return lax.broadcasted_iota(jnp.int32, shape, len(shape) - 2)


def roll(x, shift):
    return pltpu.roll(x, shift, 1)


def from_below(x):
    return jnp.where(lanes_of(x.shape) == 0, 0.0, roll(x, 1))


def from_above(x):
    return jnp.where(lanes_of(x.shape) == LANES - 1, 0.0, roll(x, LANES - 1))


def halves(x):
    return x[:, :LANES], x[:, LANES:]


def get(ref, p, rows, lv):
    return [ref[p, h, rows] for h in range(lv.parts)]


def put(ref, p, rows, values):
    for h, value in enumerate(values):
        ref[p, h, rows] = value


def every(f, *lists):
    return [f(*values) for values in zip(*lists)]


def join(*parts):
    return jnp.concatenate(parts, axis=1)


def stack(parts):
    return jnp.concatenate(parts, axis=0)


def back(shift):
    return (4 * LANES - shift) % LANES


def flag(condition):
    return jnp.where(condition, 1, 0)


def pick(x, index):
    return jnp.take_along_axis(x, index, axis=1, mode='promise_in_bounds')


def dot(x, w):
    return jnp.dot(x, w, precision=lax.Precision.HIGHEST, preferred_element_type=F32)


def kernel(cfg, rhs, start, out, *scratch):
    (u0, v0, f0, a1, b1, g1, a2, b2, g2, e3, pz, pb, stage_u, stage_f, part_u, part_f, sorted_u, sorted_f, edge_u, edge_f, s3, g3, slots, message, mask0, mask1, mask2,
     send_z, recv_z, recv_d, recv_yu, recv_yf,
     load_sem, out_sem, fine_s, fine_r, send_sem, recv_sem, all_s, all_r, part_s, part_r, ready) = scratch
    l0, l1, l2 = levels = cfg.levels
    masks = (mask0, mask1, mask2)
    n_x, n_y, n_z = cfg.counts
    cx, cy, cz = lax.axis_index('sx'), lax.axis_index('sy'), lax.axis_index('sz')
    total = n_x * n_y * n_z
    row_blocks = n_x * n_y
    yb = cy * n_x + cx

    inner = pl.ds(TILE, l0.nz)
    chip_y = n_x * l0.ny

    def load(planes, rows):
        shifted = pl.ds(rows.start + TILE, rows.size)
        k = len(loads)
        loads.append(pltpu.make_async_copy(start.at[planes, rows], stage_u.at[planes, shifted], load_sem.at[k]))
        loads.append(pltpu.make_async_copy(rhs.at[planes, rows], stage_f.at[planes, shifted], load_sem.at[k + 1]))
    loads = []
    between = pl.ds(TILE, l0.nz - 2 * TILE)
    for row in (0, l0.nz - TILE):
        load(pl.ds(0, chip_y), pl.ds(row, TILE))
    for plane in (0, chip_y - l0.wide):
        load(pl.ds(plane, l0.wide), between)
    load(pl.ds(l0.wide, chip_y - 2 * l0.wide), between)
    for copy in loads:
        copy.start()

    offsets = [(dz, dy, dx) for dz in range(n_z) for dy in range(n_y) for dx in range(n_x)][1:]
    offsets.sort(key=lambda o: -2 * (min(o[0], n_z - o[0]) + min(o[1], n_y - o[1])) - o[2])

    def peer(offset):
        return {name: lax.rem(at + d, n) for name, at, n, d in zip(('sz', 'sy', 'sx'), (cz, cy, cx), (n_z, n_y, n_x), offset)}

    def inside(step, at, count):
        if step == 0:
            return True
        return at > 0 if step < 0 else at < count - 1

    around_me = [o for o in offsets if o[0] in (0, 1, n_z - 1) and o[1] in (0, 1, n_y - 1)]
    barrier = pltpu.get_barrier_semaphore()
    for offset in around_me:
        pl.semaphore_signal(barrier, inc=1, device_id=peer(offset), device_id_type=MESH)
    outer = 2 * cx - 1
    has_outer = (cy + outer >= 0) & (cy + outer < n_y)

    def exists(d):
        return jnp.logical_and(inside(STEP_Y[d], yb, row_blocks), inside(STEP_Z[d], cz, n_z))

    def zero(ref):
        @pl.loop(0, ref.shape[0])
        def _(i):
            ref[i] = jnp.zeros(ref.shape[1:], F32)

    def span(step, first, n, wide, own):
        if step == 0:
            return pl.ds(first, n)
        if step < 0:
            return pl.ds(first if own else first - wide, wide)
        return pl.ds(first + n - wide if own else first + n, wide)

    def region(index, d, own):
        lv, arr = levels[index], (None, g1, g2)[index]
        return arr.at[span(STEP_Y[d], lv.hx, lv.ny, lv.wide, own), 0, span(STEP_Z[d], lv.z0, lv.nz, TILE, own)]

    def halo_copy(index, d, arriving):
        k = index - 1
        at = yb + STEP_Y[d]
        return pltpu.make_async_remote_copy(
            src_ref=region(index, d, not arriving), dst_ref=region(index, d if arriving else OPPOSITE[d], False),
            send_sem=send_sem.at[k, d], recv_sem=recv_sem.at[k, d if arriving else OPPOSITE[d]],
            device_id={'sx': at % n_x, 'sy': at // n_x, 'sz': cz + STEP_Z[d]}, device_id_type=MESH)

    def each(act):
        for d in (4, 5, 6, 7, 2, 3, 0, 1):
            @pl.when(exists(d))
            def _(d=d):
                act(d)

    def exchange(index):
        each(lambda d: halo_copy(index, d, False).start())
        each(lambda d: halo_copy(index, d, True).wait_recv())

    def drain(index):
        each(lambda d: halo_copy(index, d, False).wait_send())

    reach = l0.ny + l0.wide

    def fine_copies():
        got = []

        def add(sends, arrives, src, dst, arrival, k, theirs, **to):
            made = [pltpu.make_async_remote_copy(
                src_ref=a, dst_ref=b, send_sem=fine_s.at[k], recv_sem=fine_r.at[r], device_id=to, device_id_type=MESH)
                for a, b, r in ((src, dst, theirs[0]), (arrival, arrival, theirs[1]))]
            got.append((sends, arrives, *made))
        n = 0
        for z_side, z_step in enumerate((-1, 1)):
            for y_side, y_step in enumerate((-1, 1)):
                edge = pl.ds(0 if y_step < 0 else chip_y - l0.wide, l0.wide)
                to_z = jnp.logical_and(inside(y_step, cy, n_y), inside(z_step, cz, n_z))
                in_z = jnp.logical_and(has_outer, inside(z_step, cz, n_z))
                add(to_z, in_z, send_z.at[z_side, edge], recv_d.at[1 - z_side, cx], recv_d.at[z_side, y_side], n,
                    (8 + 2 * (1 - z_side) + cx, 8 + 2 * z_side + y_side), sx=1 - y_side, sy=cy + y_step, sz=cz + z_step)
                n += 1
        for z_side, z_step in enumerate((-1, 1)):
            for core in range(n_x):
                there = inside(z_step, cz, n_z)
                add(there, there, send_z.at[z_side, pl.ds(core * (chip_y - reach), reach)], recv_z.at[1 - z_side, cx],
                    recv_z.at[z_side, core], n, (12 + 2 * (1 - z_side) + cx, 12 + 2 * z_side + core), sx=core, sz=cz + z_step)
                n += 1
        return got

    def row_copies():
        got = []
        for y_side, y_step in enumerate((-1, 1)):
            for k, (edges, buf) in enumerate(((edge_u, recv_yu), (edge_f, recv_yf))):
                made = [pltpu.make_async_remote_copy(
                    src_ref=a, dst_ref=b, send_sem=fine_s.at[8 + 2 * y_side + k], recv_sem=fine_r.at[2 * r + k],
                    device_id={'sx': 1 - y_side, 'sy': cy + y_step}, device_id_type=MESH)
                    for a, b, r in ((edges.at[y_side], buf.at[cx], cx), (buf.at[y_side], buf.at[y_side], y_side))]
                got.append((inside(y_step, cy, n_y), has_outer, *made))
        return got

    chunk = reach // PARTS

    def partner_copies(part):
        other = pl.ds((1 - cx) * (chip_y - reach) + part * chunk, chunk)
        return [pltpu.make_async_remote_copy(
            src_ref=src.at[other], dst_ref=buf.at[pl.ds(part * chunk, chunk)], send_sem=part_s.at[part, k],
            recv_sem=part_r.at[part, k], device_id={'sx': 1 - cx}, device_id_type=MESH)
            for k, (src, buf) in enumerate(((sorted_u, part_u), (sorted_f, part_f)))]

    def begin(copies):
        for sends, _, copy, _ in copies:
            @pl.when(sends)
            def _(copy=copy):
                copy.start()

    def arrive(copies):
        for _, arrives, _, copy in copies:
            @pl.when(arrives)
            def _(copy=copy):
                copy.wait_recv()

    def finish(copies):
        for sends, _, copy, _ in copies:
            @pl.when(sends)
            def _(copy=copy):
                copy.wait_send()

    @pl.when(jnp.logical_not(has_outer))
    def _():
        for buf in (recv_yu, recv_yf, recv_d):
            for k in range(2):
                zero(buf.at[k])
    for z_side, z_step in enumerate((-1, 1)):
        @pl.when(jnp.logical_not(inside(z_step, cz, n_z)))
        def _(z_side=z_side):
            for core in range(n_x):
                zero(recv_z.at[z_side, core])
            zero(recv_d.at[z_side])
    for index in (1, 2):
        for d in SIDES:
            @pl.when(jnp.logical_not(exists(d)))
            def _(index=index, d=d):
                zero(region(index, d, False))

    for lv, arrays in ((l0, (u0, v0)), (l1, (a1, b1)), (l2, (a2, b2))):
        for arr in arrays:
            for plane, outside in ((lv.hx - 1, yb == 0), (lv.hx + lv.ny, yb == row_blocks - 1)):
                @pl.when(outside)
                def _(arr=arr, lv=lv, plane=plane):
                    put(arr, plane, lv.all, [jnp.zeros((lv.rows, LANES), F32)] * lv.parts)

    for lv, table in zip(levels, masks):
        shape = (lv.rows, LANES)
        z = rows_of(shape) + (lv.top - lv.z0) + cz * lv.nz
        ok = (z >= 0) & (z < n_z * lv.nz) & (lanes_of(shape) < lv.nx)
        table[0] = jnp.zeros(shape, F32)
        table[1] = jnp.where(ok, 1.0, 0.0).astype(F32)
        table[2] = jnp.where(ok, NINTH, 0.0).astype(F32)

    def valid(lv, p):
        y = p + (yb * lv.ny - lv.hx)
        return flag((y >= 0) & (y < row_blocks * lv.ny))

    middle = LANES // 2

    def sort_x(x):
        lane = lanes_of(x.shape)
        return pick(x, 2 * (lane % middle) + (lane // middle + cx) % 2)

    def split_x(first, second, core):
        here = lanes_of(first.shape) // middle == core
        return [jnp.where(here, first, second), roll(jnp.where(here, second, first), middle)]

    def merge_x(even, odd, core):
        here = lanes_of(even.shape) // middle == core
        odd = roll(odd, middle)
        return jnp.where(here, even, odd), jnp.where(here, odd, even)

    pl.semaphore_wait(barrier, len(around_me))

    def across(c, lv):
        if lv.parts > 1:
            even, odd = c
            return [odd + from_below(odd), even + from_above(even)]
        if lv.nx == LANES:
            return [from_below(c[0]) + from_above(c[0])]
        return [roll(c[0], 1) + roll(c[0], LANES - 1)]

    def neighbours(src, p, xm, c, xp, lv, top, n):
        zm, zp = get(src, p, pl.ds(top - 1, n), lv), get(src, p, pl.ds(top + 1, n), lv)
        return every(lambda a, b, d, e, f: ((a + b) + (d + e)) + f, xm, xp, zm, zp, across(c, lv))

    def table_rows(table, k, lv, top, n):
        return table[k, pl.ds(top - lv.top, n)]

    def sweep(src, dst, rhs_ref, lv, table, scale=None):
        @pl.loop(0, lv.count)
        def _(g):
            base = lv.begin + g * lv.group
            for top, n in lv.blocks:
                rows = pl.ds(top, n)
                xm, c = get(src, base - 1, rows, lv), get(src, base, rows, lv)
                for j in range(lv.group):
                    p = base + j
                    xp = get(src, p + 1, rows, lv)
                    t = every(lambda a, b: a + 3.0 * b, neighbours(src, p, xm, c, xp, lv, top, n), c)
                    if scale is not None:
                        t = [x * scale for x in t]
                    keep = table_rows(table, 2 * valid(lv, p), lv, top, n)
                    put(dst, p, rows, every(lambda a, b: (a + b) * keep, t, get(rhs_ref, p, rows, lv)))
                    xm, c = c, xp

    def first_sweep(dst, rhs_ref, lv, table):
        @pl.loop(0, lv.count)
        def _(g):
            for j in range(lv.group):
                p = lv.begin + g * lv.group + j
                dst[p, 0, lv.all] = rhs_ref[p, 0, lv.all] * table[2 * valid(lv, p)]

    def restrict_planes(src, rhs_ref, lv, table, group):
        def res(p, xm, c, xp, top, n):
            return every(lambda a, b, d: a + b - 6.0 * d, neighbours(src, p, xm, c, xp, lv, top, n), get(rhs_ref, p, pl.ds(top, n), lv), c)

        @pl.loop(0, lv.ny // 2 // group)
        def _(i):
            for top, n in lv.blocks:
                rows = pl.ds(top, n)
                p = lv.hx + 2 * group * i
                xm, c = get(src, p - 1, rows, lv), get(src, p, rows, lv)
                prev = res(p - 1, get(src, p - 2, rows, lv), xm, c, top, n)
                prev = [jnp.where((yb > 0) | (i > 0), x, 0.0) for x in prev]
                keep = table_rows(table, 1, lv, top, n)
                for j in range(group):
                    x1, x2 = get(src, p + 1, rows, lv), get(src, p + 2, rows, lv)
                    even = res(p, xm, c, x1, top, n)
                    odd = res(p + 1, c, x1, x2, top, n)
                    for h in range(lv.parts):
                        pb[h, i * group + j, rows] = ((prev[h] + odd[h]) + (even[h] + even[h])) * keep
                    prev, xm, c, p = odd, x1, x2, p + 2

    def restricted_rows(i, lv, h=0):
        half = lv.nz // 2
        return ((pb[h, i, pl.ds(lv.z0 - 1, half, stride=2)] + pb[h, i, pl.ds(lv.z0 + 1, half, stride=2)])
                + 2.0 * pb[h, i, pl.ds(lv.z0, half, stride=2)])

    def weights(near, one, other):
        return jnp.where(near == 0, one, jnp.where((near == 1) | (near == -1), other, 0.0)).astype(F32)

    square = (LANES, LANES)
    eighth = 1.0 / (TILE * TILE)

    def restrict_level(src, rhs_ref, lv, table, coarse_rhs, coarse, group, step):
        restrict_planes(src, rhs_ref, lv, table, group)
        lane = lanes_of(square)
        w = jnp.where(lane < coarse.nx, weights(rows_of(square) - 2 * lane, 2.0 * eighth, eighth), 0.0)

        @pl.loop(0, coarse.ny // step)
        def _(i):
            got = [restricted_rows(i * step + j, lv) for j in range(step)]
            if lv.parts > 1:
                odds = [restricted_rows(i * step + j, lv, 1) for j in range(step)]
                got = [((odd + from_below(odd)) + 2.0 * even) * eighth for even, odd in zip(got, odds)]
            else:
                got = dot(stack(got), w)
                got = [got[j * coarse.nz:(j + 1) * coarse.nz] for j in range(step)]
            for j in range(step):
                coarse_rhs[coarse.hx + i * step + j, 0, coarse.own] = got[j]

    def prolong_planes(e, first, e_z0, e_top, e_rows, e_nx, chunk, n_chunks, lv):
        lane, below = lanes_of(square), rows_of(square)
        w = jnp.where(below < e_nx, weights(lane - 2 * below, 4.0, 2.0), 0.0)
        row = e_z0 - e_top - (lv.z0 - lv.top) // 2
        n = lv.rows // 2

        @pl.loop(0, n_chunks)
        def _(i):
            planes = pl.ds(first + i * chunk, chunk)
            got = e[planes, 0, pl.ds(e_top, e_rows)]
            if lv.parts == 1:
                got = dot(got.reshape(chunk * e_rows, LANES), w).reshape(chunk, e_rows, LANES)
            else:
                got = got * 4.0
            pz[pl.ds(i * chunk, chunk), pl.ds(0, e_rows)] = got

        @pl.loop(0, n_chunks)
        def _(i):
            for j in range(chunk):
                a = pz[i * chunk + j, pl.ds(row, n)]
                b = pz[i * chunk + j, pl.ds(row + 1, n)]
                pb[0, i * chunk + j, pl.ds(lv.top, n, stride=2)] = a
                pb[0, i * chunk + j, pl.ds(lv.top + 1, n, stride=2)] = 0.5 * (a + b)

    def correct(dst, lv, table, pairs):
        def load(at, rows):
            a = pb[0, at, rows]
            return [a, 0.5 * (a + from_above(a))] if lv.parts > 1 else [a]

        @pl.loop(0, lv.group * lv.count // (2 * pairs))
        def _(i):
            for top, n in lv.blocks:
                rows = pl.ds(top, n)
                a = load(i * pairs, rows)
                for j in range(pairs):
                    b = load(i * pairs + j + 1, rows)
                    p = lv.begin + 2 * (pairs * i + j)
                    between = every(lambda x, y: 0.5 * (x + y), a, b)
                    for q, add in ((p, a), (p + 1, between)):
                        keep = table_rows(table, valid(lv, q), lv, top, n)
                        put(dst, q, rows, every(lambda x, y: (x + y) * keep, get(dst, q, rows, lv), add))
                    a = b

    row_halo, halo = row_copies(), fine_copies()
    for copy in loads[:4]:
        copy.wait()
    half = TILE // 2
    upper = rows_of((TILE, LANES)) >= half

    @pl.loop(0, chip_y // TILE)
    def _(i):
        for j in range(TILE):
            y = i * TILE + j
            for side, row in enumerate((TILE, TILE + l0.nz - half)):
                send_z[side, y] = sort_x(jnp.where(upper, stage_f[y, pl.ds(row - half, TILE)], stage_u[y, pl.ds(row, TILE)]))
    begin(halo[4:])
    for copy in loads[4:]:
        copy.wait()
    step = 4

    for side, plane in enumerate((0, chip_y - l0.wide)):
        for j in range(l0.wide):
            edge_u[side, j] = sort_x(stage_u[plane + j, inner])
            edge_f[side, j] = sort_x(stage_f[plane + j, inner])
    begin(row_halo)

    def sort_planes(first, n):
        @pl.loop(0, n // step)
        def _(i):
            for j in range(step):
                y = first + i * step + j
                sorted_u[y] = sort_x(stage_u[y, inner])
                sorted_f[y] = sort_x(stage_f[y, inner])

    @pl.loop(0, PARTS)
    def _(part):
        sort_planes((1 - cx) * (chip_y - reach) + part * chunk, chunk)
        for copy in partner_copies(part):
            copy.start()
    begin(halo[:4])
    sort_planes(cx * reach, chip_y - reach)
    for offset in around_me:
        pl.semaphore_signal(ready, inc=1, device_id=peer(offset), device_id_type=MESH)

    some = reach // 3

    @pl.loop(0, PARTS)
    def _(part):
        for copy in partner_copies(part):
            copy.wait_recv()

        @pl.loop(0, chunk // step)
        def _(i):
            for j in range(step):
                k = part * chunk + i * step + j
                for src, buf, dst in ((sorted_u, part_u, u0), (sorted_f, part_f, f0)):
                    put(dst, l0.hx - cx * l0.wide + k, l0.own, split_x(src[cx * (chip_y - reach) + k], buf[k], cx))
    arrive(row_halo)
    outer_plane = l0.hx - l0.wide + cx * reach

    for buf, dst in ((recv_yu, u0), (recv_yf, f0)):
        for j in range(l0.wide):
            put(dst, outer_plane + j, l0.own, split_x(buf[0, j], buf[1, j], 0))
    arrive(halo)
    finish(row_halo)
    finish(halo)
    for part in range(PARTS):
        for copy in partner_copies(part):
            copy.wait_send()

    def put_rows(p, side, buf, k):
        row = l0.z0 + l0.nz if side else l0.z0 - half
        for h, part in enumerate(split_x(buf[0, k], buf[1, k], 0)):
            pltpu.store(u0.at[p, h, pl.ds(row, TILE)], part, mask=jnp.logical_not(upper))
            pltpu.store(f0.at[p, h, pl.ds(row - half, TILE)], part, mask=upper)

    @pl.loop(0, reach // some)
    def _(i):
        for j in range(some):
            for side in range(2):
                put_rows(l0.hx - cx * l0.wide + i * some + j, side, recv_z.at[side], i * some + j)
    for side in range(2):
        for j in range(l0.wide):
            put_rows(outer_plane + j, side, recv_d.at[side], j)
    sweep(u0, v0, f0, l0, mask0, cfg.stiffness)
    sweep(v0, u0, f0, l0, mask0)
    restrict_level(u0, f0, l0, mask0, g1, l1, 4, 4)

    exchange(1)
    first_sweep(a1, g1, l1, mask1)
    sweep(a1, b1, g1, l1, mask1)
    restrict_level(b1, g1, l1, mask1, g2, l2, 8, 8)
    exchange(2)
    first_sweep(a2, g2, l2, mask2)
    sweep(a2, b2, g2, l2, mask2)

    restrict_planes(b2, g2, l2, mask2, 4)
    ny3, nz3, width = l2.ny // 2, l2.nz // 2, l2.nx // 2
    near = rows_of(square) - 2 * (lanes_of(square) % width)
    got = dot(stack([restricted_rows(j, l2) for j in range(ny3)]), weights(near, 2.0 * eighth, eighth))
    tile = (TILE, LANES)
    lane = lanes_of(tile)
    block = lane // width
    blocks = LANES // width
    packed = got[:nz3]
    for j in range(1, ny3):
        packed = jnp.where(block == j, got[j * nz3:(j + 1) * nz3], packed)
    packed = roll(packed, width * cy)
    message[...] = packed
    slot = yb * n_z + cz
    slots[slot] = packed

    def gather_copy(k, at):
        return pltpu.make_async_remote_copy(
            src_ref=message, dst_ref=slots.at[at], send_sem=all_s.at[k], recv_sem=all_r.at[at], device_id=peer(offsets[k]), device_id_type=MESH)

    pl.semaphore_wait(ready, len(around_me))
    for k in range(total - 1):
        gather_copy(k, slot).start()
    for k, offset in enumerate(offsets):
        who = peer(offset)
        gather_copy(k, (who['sy'] * n_x + who['sx']) * n_z + who['sz']).wait_recv()

    tall = nz3 * n_z
    data = pl.ds(TILE, tall)
    for which in range(2):
        for y in range(TILE):
            for at in (0, TILE + tall):
                s3[which, y, pl.ds(at, TILE)] = jnp.zeros(tile, F32)
    live = lane < width * n_y

    @pl.loop(0, n_x)
    def _(core):
        for j in range(ny3):
            for z in range(n_z):
                acc = jnp.zeros(tile, F32)
                for t in range(n_y):
                    acc = jnp.where((block + 2 * blocks - t - j) % blocks == 0, slots[(t * n_x + core) * n_z + z], acc)
                acc = jnp.where(live, roll(acc, back(width * j)), 0.0)
                rows = pl.ds(TILE + nz3 * z, nz3)
                g3[core * ny3 + j, rows] = acc
                s3[0, core * ny3 + j, rows] = acc * NINTH

    long = (tall, LANES)
    along = lanes_of(long)
    x_first, x_last = along % width == 0, along % width == width - 1
    y_first, y_last = along < width, along >= width * (n_y - 1)

    def coarse_sweep(k, carry):
        old, new = k % 2, (k + 1) % 2
        lowest, highest = s3[old, 0, data], s3[old, TILE - 1, data]
        c = lowest
        ym = jnp.where(y_first, 0.0, roll(highest, width % LANES))
        beyond = jnp.where(y_last, 0.0, roll(lowest, back(width)))
        for y in range(TILE):
            yp = s3[old, y + 1, data] if y < TILE - 1 else beyond
            around = (ym + yp) + (s3[old, y, pl.ds(TILE - 1, tall)] + s3[old, y, pl.ds(TILE + 1, tall)])
            left = jnp.where(x_first, 0.0, roll(c, 1))
            right = jnp.where(x_last, 0.0, roll(c, LANES - 1))
            s3[new, y, data] = (around + (left + right) + 3.0 * c + g3[y, data]) * NINTH
            ym, c = c, yp
        return carry
    lax.fori_loop(0, COARSE_SWEEPS - 1, coarse_sweep, 0)

    first = (l2.begin - l2.hx) // 2
    for i in range(e3.shape[0]):
        y = yb * ny3 + (i + first)
        c = s3[(COARSE_SWEEPS - 1) % 2, (y + TILE) % TILE, pl.ds(pl.multiple_of(cz * nz3, TILE), 3 * TILE)]
        ok = (lanes_of(c.shape) < width) & (y >= 0) & (y < row_blocks * ny3)
        e3[i, 0] = jnp.where(ok, roll(c, back((y + TILE) // TILE * width + LANES - width)), 0.0)

    prolong_planes(e3, 0, TILE, 0, 3 * TILE, width, 6, 2, l2)
    correct(b2, l2, mask2, 5)
    sweep(b2, a2, g2, l2, mask2)
    sweep(a2, b2, g2, l2, mask2)
    prolong_planes(b2, l2.hx + (l1.begin - l1.hx) // 2, l2.z0, l2.top, l2.rows, l2.nx, 8, 2, l1)
    correct(b1, l1, mask1, 7)
    sweep(b1, a1, g1, l1, mask1)
    sweep(a1, b1, g1, l1, mask1)
    prolong_planes(b1, l1.hx + (l0.begin - l0.hx) // 2, l1.z0, l1.top, l1.rows, l1.nx, 8, 3, l0)
    correct(u0, l0, mask0, 4)
    sweep(u0, v0, f0, l0, mask0)

    def results(i):
        here, there = pl.ds(i * step, step), pl.ds(cx * l0.ny + i * step, step)
        return pltpu.make_async_remote_copy(
            src_ref=stage_f.at[here, inner], dst_ref=out.at[there], send_sem=out_sem.at[0, i], recv_sem=out_sem.at[1, i],
            device_id={'sx': 1 - cx}, device_id_type=MESH)

    @pl.loop(0, l0.ny // step)
    def _(i):
        for j in range(step):
            k = i * step + j
            p = l0.hx + k
            c = get(v0, p, l0.own, l0)
            around = neighbours(v0, p, get(v0, p - 1, l0.own, l0), c, get(v0, p + 1, l0.own, l0), l0, l0.z0, l0.nz)
            got = every(lambda x, y, g: (x + 3.0 * y + g) * (NINTH / cfg.stiffness), around, c, get(f0, p, l0.own, l0))
            out[cx * l0.ny + k], stage_f[k, inner] = merge_x(*got, cx)
        results(i).start()

    @pl.loop(0, l0.ny // step)
    def _(i):
        results(i).wait()
    drain(1)
    drain(2)

    for k in range(total - 1):
        gather_copy(k, slot).wait_send()


def write_out(held, out, rows, sem):
    def copy_out(i):
        planes = pl.ds(i * TILE, TILE)
        return pltpu.make_async_copy(rows.at[planes], out.at[planes], sem.at[i])

    @pl.loop(0, held.shape[0] // TILE)
    def _(i):
        for j in range(TILE):
            x = held[i * TILE + j]
            lane = lanes_of(x.shape)
            rows[i * TILE + j] = pick(x, lane // 2 + LANES // 2 * ((lane + lax.axis_index('sx')) % 2))
        copy_out(i).start()

    @pl.loop(0, held.shape[0] // TILE)
    def _(i):
        copy_out(i).wait()


def local_cycle(rhs, start, counts, size):
    rhs, start = (jnp.transpose(x, (1, 2, 0)) for x in (rhs, start))
    n_x, n_y, n_z = counts
    chip_y, nz, nx = rhs.shape
    shapes = [(chip_y // n_x >> k, nz >> k, nx * n_x >> k) for k in range(3)]
    l0 = make_level(shapes[0], 6, 8, 4, nz + 8, 2, 8, (shapes[0][0] + 8) // 8, 4, 24)
    l1 = make_level(shapes[1], 8, 16, 8, shapes[1][1] + 16, 2, 14, (shapes[1][0] + 12) // 14, 5, 24)
    l2 = make_level(shapes[2], 8, 16, 8, shapes[2][1] + 16, 2, 10, (shapes[2][0] + 12) // 10, 6, 32)
    cfg = types.SimpleNamespace(levels=(l0, l1, l2), counts=counts, stiffness=float((size + 1) ** 2))
    total = n_x * n_y * n_z

    def vmem(*shape):
        return pltpu.VMEM(shape, F32)

    scratch = [vmem(lv.planes, lv.parts, lv.depth, LANES) for lv in (l0, l1, l2) for _ in range(3)]
    reach = l0.ny + l0.wide
    scratch += [vmem(12, 1, 3 * TILE, LANES), vmem(l1.ny + 8, l1.rows, LANES), vmem(2, l1.ny + 8, l0.depth, LANES)]
    scratch += [vmem(chip_y, l0.depth, LANES)] * 2 + [vmem(reach, nz, LANES)] * 2 + [vmem(chip_y, nz, LANES)] * 2
    scratch += [vmem(2, l0.wide, nz, LANES)] * 2
    scratch += [vmem(2, TILE, l2.nz // 2 * n_z + 2 * TILE, LANES), vmem(TILE, l2.nz // 2 * n_z + 2 * TILE, LANES), vmem(total, TILE, LANES), vmem(TILE, LANES)]
    scratch += [vmem(3, lv.rows, LANES) for lv in (l0, l1, l2)]
    scratch += [vmem(2, chip_y, TILE, LANES), vmem(2, n_x, reach, TILE, LANES), vmem(2, 2, l0.wide, TILE, LANES)]
    scratch += [vmem(2, l0.wide, nz, LANES)] * 2
    sems = [(10,), (2, l0.ny // 4), (16,), (16,), (2, len(SIDES)), (2, len(SIDES)), (total,), (total,), (PARTS, 2), (PARTS, 2)]
    scratch += [pltpu.SemaphoreType.DMA(shape) for shape in sems] + [pltpu.SemaphoreType.REGULAR]
    got = pl.pallas_call(
        functools.partial(kernel, cfg),
        out_shape=pltpu.VMEM(rhs.shape, F32),
        in_specs=[pl.BlockSpec(memory_space=pl.ANY)] * 2,
        out_specs=pl.BlockSpec(memory_space=pltpu.VMEM),
        scratch_shapes=scratch,
        compiler_params=pltpu.CompilerParams(collective_id=0, has_side_effects=True, vmem_limit_bytes=60 * 2 ** 20),
    )(rhs, start)
    got = pl.pallas_call(
        write_out,
        out_shape=jax.ShapeDtypeStruct(rhs.shape, F32),
        in_specs=[pl.BlockSpec(memory_space=pltpu.VMEM)],
        out_specs=pl.BlockSpec(memory_space=pl.ANY),
        scratch_shapes=[vmem(*rhs.shape), pltpu.SemaphoreType.DMA((chip_y // TILE,))],
    )(pltpu.with_memory_space_constraint(got, pltpu.VMEM))
    return jnp.transpose(got, (2, 0, 1))


def solution(mesh):
    counts = (mesh.shape['sx'], mesh.shape['sy'], mesh.shape['sz'])
    spec = P(('dp', 'sx'), 'sy', 'sz')

    def run(rhs_grid, u_start):
        size = rhs_grid.shape[0] // mesh.shape['dp']
        cycle = functools.partial(local_cycle, counts=counts, size=size)
        return jax.shard_map(cycle, mesh=mesh, in_specs=(spec, spec), out_specs=spec, check_vma=False)(rhs_grid, u_start)
    return run
```

```python
import functools
import types
import jax
import jax.numpy as jnp
from jax import lax
from jax.experimental import pallas as pl
from jax.experimental.pallas import tpu as pltpu
from jax.sharding import PartitionSpec as P

F32 = jnp.float32
MESH = pl.DeviceIdType.MESH
LANES = 128
TILE = 8
NINTH = 1.0 / 9.0
COARSE_SWEEPS = 16
PARTS = 3
OPPOSITE = (1, 0, 3, 2, 7, 6, 5, 4)
STEP_Y = (-1, 1, 0, 0, -1, -1, 1, 1)
STEP_Z = (0, 0, -1, 1, -1, 1, -1, 1)
SIDES = range(len(STEP_Y))


def make_level(shape, hx, z0, top, rows, begin, group, count, wide, block):
    ny, nz, nx = shape
    lv = types.SimpleNamespace(ny=ny, nz=nz, nx=nx, hx=hx, z0=z0, top=top, rows=rows, begin=begin, group=group, count=count, wide=wide)
    lv.planes = ny + 2 * hx
    lv.depth = nz + 2 * z0
    lv.parts = max(nx // LANES, 1)
    lv.own = pl.ds(z0, nz)
    lv.all = pl.ds(top, rows)
    lv.block = block
    lv.blocks = cut(lv, top, rows)
    return lv


def cut(lv, top, rows):
    return [(top + i, min(lv.block, rows - i)) for i in range(0, rows, lv.block)]


def lanes_of(shape):
    return lax.broadcasted_iota(jnp.int32, shape, len(shape) - 1)


def rows_of(shape):
    return lax.broadcasted_iota(jnp.int32, shape, len(shape) - 2)


def roll(x, shift):
    return pltpu.roll(x, shift, 1)


def from_below(x):
    return jnp.where(lanes_of(x.shape) == 0, 0.0, roll(x, 1))


def from_above(x):
    return jnp.where(lanes_of(x.shape) == LANES - 1, 0.0, roll(x, LANES - 1))


def halves(x):
    return x[:, :LANES], x[:, LANES:]


def get(ref, p, rows, lv):
    return [ref[p, h, rows] for h in range(lv.parts)]


def put(ref, p, rows, values):
    for h, value in enumerate(values):
        ref[p, h, rows] = value


def every(f, *lists):
    return [f(*values) for values in zip(*lists)]


def join(*parts):
    return jnp.concatenate(parts, axis=1)


def stack(parts):
    return jnp.concatenate(parts, axis=0)


def back(shift):
    return (4 * LANES - shift) % LANES


def flag(condition):
    return jnp.where(condition, 1, 0)


def pick(x, index):
    return jnp.take_along_axis(x, index, axis=1, mode='promise_in_bounds')


def dot(x, w):
    return jnp.dot(x, w, precision=lax.Precision.HIGHEST, preferred_element_type=F32)


def kernel(cfg, rhs, start, out, *scratch):
    (u0, v0, f0, w0, a1, b1, g1, a2, b2, g2, e3, pz, pb, stage_u, stage_f, part_u, part_f, sorted_u, sorted_f, edge_u, edge_f, s3, g3, slots, message, mask0, mask1, mask2,
     send_z, recv_z, recv_d, recv_yu, recv_yf,
     load_sem, out_sem, fine_s, fine_r, send_sem, recv_sem, all_s, all_r, part_s, part_r, ready) = scratch
    l0, l1, l2 = levels = cfg.levels
    masks = (mask0, mask1, mask2)
    n_x, n_y, n_z = cfg.counts
    cx, cy, cz = lax.axis_index('sx'), lax.axis_index('sy'), lax.axis_index('sz')
    total = n_x * n_y * n_z
    row_blocks = n_x * n_y
    yb = cy * n_x + cx

    inner = pl.ds(TILE, l0.nz)
    chip_y = n_x * l0.ny

    def load(planes, rows):
        shifted = pl.ds(rows.start + TILE, rows.size)
        k = len(loads)
        loads.append(pltpu.make_async_copy(start.at[planes, rows], stage_u.at[planes, shifted], load_sem.at[k]))
        loads.append(pltpu.make_async_copy(rhs.at[planes, rows], stage_f.at[planes, shifted], load_sem.at[k + 1]))
    loads = []
    between = pl.ds(TILE, l0.nz - 2 * TILE)
    for row in (0, l0.nz - TILE):
        load(pl.ds(0, chip_y), pl.ds(row, TILE))
    for plane in (0, chip_y - l0.wide):
        load(pl.ds(plane, l0.wide), between)
    load(pl.ds(l0.wide, chip_y - 2 * l0.wide), between)
    for copy in loads:
        copy.start()

    offsets = [(dz, dy, dx) for dz in range(n_z) for dy in range(n_y) for dx in range(n_x)][1:]
    offsets.sort(key=lambda o: -2 * (min(o[0], n_z - o[0]) + min(o[1], n_y - o[1])) - o[2])

    def peer(offset):
        return {name: lax.rem(at + d, n) for name, at, n, d in zip(('sz', 'sy', 'sx'), (cz, cy, cx), (n_z, n_y, n_x), offset)}

    def inside(step, at, count):
        if step == 0:
            return True
        return at > 0 if step < 0 else at < count - 1

    around_me = [o for o in offsets if o[0] in (0, 1, n_z - 1) and o[1] in (0, 1, n_y - 1)]
    barrier = pltpu.get_barrier_semaphore()
    for offset in around_me:
        pl.semaphore_signal(barrier, inc=1, device_id=peer(offset), device_id_type=MESH)
    outer = 2 * cx - 1
    has_outer = (cy + outer >= 0) & (cy + outer < n_y)

    def exists(d):
        return jnp.logical_and(inside(STEP_Y[d], yb, row_blocks), inside(STEP_Z[d], cz, n_z))

    def zero(ref):
        @pl.loop(0, ref.shape[0])
        def _(i):
            ref[i] = jnp.zeros(ref.shape[1:], F32)

    def span(step, first, n, wide, own):
        if step == 0:
            return pl.ds(first, n)
        if step < 0:
            return pl.ds(first if own else first - wide, wide)
        return pl.ds(first + n - wide if own else first + n, wide)

    def region(index, d, own):
        lv, arr = levels[index], (None, g1, g2)[index]
        return arr.at[span(STEP_Y[d], lv.hx, lv.ny, lv.wide, own), 0, span(STEP_Z[d], lv.z0, lv.nz, TILE, own)]

    def halo_copy(index, d, arriving):
        k = index - 1
        at = yb + STEP_Y[d]
        return pltpu.make_async_remote_copy(
            src_ref=region(index, d, not arriving), dst_ref=region(index, d if arriving else OPPOSITE[d], False),
            send_sem=send_sem.at[k, d], recv_sem=recv_sem.at[k, d if arriving else OPPOSITE[d]],
            device_id={'sx': at % n_x, 'sy': at // n_x, 'sz': cz + STEP_Z[d]}, device_id_type=MESH)

    def each(act):
        for d in (4, 5, 6, 7, 2, 3, 0, 1):
            @pl.when(exists(d))
            def _(d=d):
                act(d)

    def exchange(index):
        each(lambda d: halo_copy(index, d, False).start())
        each(lambda d: halo_copy(index, d, True).wait_recv())

    def drain(index):
        each(lambda d: halo_copy(index, d, False).wait_send())

    reach = l0.ny + l0.wide

    def fine_copies():
        got = []

        def add(sends, arrives, src, dst, arrival, k, theirs, **to):
            made = [pltpu.make_async_remote_copy(
                src_ref=a, dst_ref=b, send_sem=fine_s.at[k], recv_sem=fine_r.at[r], device_id=to, device_id_type=MESH)
                for a, b, r in ((src, dst, theirs[0]), (arrival, arrival, theirs[1]))]
            got.append((sends, arrives, *made))
        n = 0
        for z_side, z_step in enumerate((-1, 1)):
            for y_side, y_step in enumerate((-1, 1)):
                edge = pl.ds(0 if y_step < 0 else chip_y - l0.wide, l0.wide)
                to_z = jnp.logical_and(inside(y_step, cy, n_y), inside(z_step, cz, n_z))
                in_z = jnp.logical_and(has_outer, inside(z_step, cz, n_z))
                add(to_z, in_z, send_z.at[z_side, edge], recv_d.at[1 - z_side, cx], recv_d.at[z_side, y_side], n,
                    (8 + 2 * (1 - z_side) + cx, 8 + 2 * z_side + y_side), sx=1 - y_side, sy=cy + y_step, sz=cz + z_step)
                n += 1
        for z_side, z_step in enumerate((-1, 1)):
            for core in range(n_x):
                there = inside(z_step, cz, n_z)
                add(there, there, send_z.at[z_side, pl.ds(core * (chip_y - reach), reach)], recv_z.at[1 - z_side, cx],
                    recv_z.at[z_side, core], n, (12 + 2 * (1 - z_side) + cx, 12 + 2 * z_side + core), sx=core, sz=cz + z_step)
                n += 1
        return got

    def row_copies():
        got = []
        for y_side, y_step in enumerate((-1, 1)):
            for k, (edges, buf) in enumerate(((edge_u, recv_yu), (edge_f, recv_yf))):
                made = [pltpu.make_async_remote_copy(
                    src_ref=a, dst_ref=b, send_sem=fine_s.at[8 + 2 * y_side + k], recv_sem=fine_r.at[2 * r + k],
                    device_id={'sx': 1 - y_side, 'sy': cy + y_step}, device_id_type=MESH)
                    for a, b, r in ((edges.at[y_side], buf.at[cx], cx), (buf.at[y_side], buf.at[y_side], y_side))]
                got.append((inside(y_step, cy, n_y), has_outer, *made))
        return got

    chunk = reach // PARTS

    def partner_copies(part):
        other = pl.ds((1 - cx) * (chip_y - reach) + part * chunk, chunk)
        return [pltpu.make_async_remote_copy(
            src_ref=src.at[other], dst_ref=buf.at[pl.ds(part * chunk, chunk)], send_sem=part_s.at[part, k],
            recv_sem=part_r.at[part, k], device_id={'sx': 1 - cx}, device_id_type=MESH)
            for k, (src, buf) in enumerate(((sorted_u, part_u), (sorted_f, part_f)))]

    def begin(copies):
        for sends, _, copy, _ in copies:
            @pl.when(sends)
            def _(copy=copy):
                copy.start()

    def arrive(copies):
        for _, arrives, _, copy in copies:
            @pl.when(arrives)
            def _(copy=copy):
                copy.wait_recv()

    def finish(copies):
        for sends, _, copy, _ in copies:
            @pl.when(sends)
            def _(copy=copy):
                copy.wait_send()

    @pl.when(jnp.logical_not(has_outer))
    def _():
        for buf in (recv_yu, recv_yf, recv_d):
            for k in range(2):
                zero(buf.at[k])
    for z_side, z_step in enumerate((-1, 1)):
        @pl.when(jnp.logical_not(inside(z_step, cz, n_z)))
        def _(z_side=z_side):
            for core in range(n_x):
                zero(recv_z.at[z_side, core])
            zero(recv_d.at[z_side])
    for index in (1, 2):
        for d in SIDES:
            @pl.when(jnp.logical_not(exists(d)))
            def _(index=index, d=d):
                zero(region(index, d, False))

    for lv, arrays in ((l0, (u0, v0, w0)), (l1, (a1, b1)), (l2, (a2, b2))):
        for arr in arrays:
            for plane, outside in ((lv.hx - 1, yb == 0), (lv.hx + lv.ny, yb == row_blocks - 1)):
                @pl.when(outside)
                def _(arr=arr, lv=lv, plane=plane):
                    put(arr, plane, lv.all, [jnp.zeros((lv.rows, LANES), F32)] * lv.parts)

    for lv, table in zip(levels, masks):
        shape = (lv.rows, LANES)
        z = rows_of(shape) + (lv.top - lv.z0) + cz * lv.nz
        ok = (z >= 0) & (z < n_z * lv.nz) & (lanes_of(shape) < lv.nx)
        table[0] = jnp.zeros(shape, F32)
        table[1] = jnp.where(ok, 1.0, 0.0).astype(F32)
        table[2] = jnp.where(ok, NINTH, 0.0).astype(F32)

    def valid(lv, p):
        y = p + (yb * lv.ny - lv.hx)
        return flag((y >= 0) & (y < row_blocks * lv.ny))

    middle = LANES // 2

    def sort_x(x):
        lane = lanes_of(x.shape)
        return pick(x, 2 * (lane % middle) + (lane // middle + cx) % 2)

    def split_x(first, second, core):
        here = lanes_of(first.shape) // middle == core
        return [jnp.where(here, first, second), roll(jnp.where(here, second, first), middle)]

    def merge_x(even, odd, core):
        here = lanes_of(even.shape) // middle == core
        odd = roll(odd, middle)
        return jnp.where(here, even, odd), jnp.where(here, odd, even)

    pl.semaphore_wait(barrier, len(around_me))

    def across(c, lv):
        if lv.parts > 1:
            even, odd = c
            return [odd + from_below(odd), even + from_above(even)]
        if lv.nx == LANES:
            return [from_below(c[0]) + from_above(c[0])]
        return [roll(c[0], 1) + roll(c[0], LANES - 1)]

    def neighbours(src, p, xm, c, xp, lv, top, n):
        zm, zp = get(src, p, pl.ds(top - 1, n), lv), get(src, p, pl.ds(top + 1, n), lv)
        return every(lambda a, b, d, e, f: ((a + b) + (d + e)) + f, xm, xp, zm, zp, across(c, lv))

    def table_rows(table, k, lv, top, n):
        return table[k, pl.ds(top - lv.top, n)]

    def sweep(src, dst, rhs_ref, lv, table, scale=None, blocks=None, first=None, count=None):
        @pl.loop(0, count or lv.count)
        def _(g):
            base = (lv.begin if first is None else first) + g * lv.group
            for top, n in blocks or lv.blocks:
                rows = pl.ds(top, n)
                xm, c = get(src, base - 1, rows, lv), get(src, base, rows, lv)
                for j in range(lv.group):
                    p = base + j
                    xp = get(src, p + 1, rows, lv)
                    t = every(lambda a, b: a + 3.0 * b, neighbours(src, p, xm, c, xp, lv, top, n), c)
                    if scale is not None:
                        t = [x * scale for x in t]
                    keep = table_rows(table, 2 * valid(lv, p), lv, top, n)
                    put(dst, p, rows, every(lambda a, b: (a + b) * keep, t, get(rhs_ref, p, rows, lv)))
                    xm, c = c, xp

    def first_sweep(dst, rhs_ref, lv, table):
        @pl.loop(0, lv.count)
        def _(g):
            for j in range(lv.group):
                p = lv.begin + g * lv.group + j
                dst[p, 0, lv.all] = rhs_ref[p, 0, lv.all] * table[2 * valid(lv, p)]

    def restrict_planes(src, rhs_ref, lv, table, group):
        def res(p, xm, c, xp, top, n):
            return every(lambda a, b, d: a + b - 6.0 * d, neighbours(src, p, xm, c, xp, lv, top, n), get(rhs_ref, p, pl.ds(top, n), lv), c)

        @pl.loop(0, lv.ny // 2 // group)
        def _(i):
            for top, n in lv.blocks:
                rows = pl.ds(top, n)
                p = lv.hx + 2 * group * i
                xm, c = get(src, p - 1, rows, lv), get(src, p, rows, lv)
                prev = res(p - 1, get(src, p - 2, rows, lv), xm, c, top, n)
                prev = [jnp.where((yb > 0) | (i > 0), x, 0.0) for x in prev]
                keep = table_rows(table, 1, lv, top, n)
                for j in range(group):
                    x1, x2 = get(src, p + 1, rows, lv), get(src, p + 2, rows, lv)
                    even = res(p, xm, c, x1, top, n)
                    odd = res(p + 1, c, x1, x2, top, n)
                    for h in range(lv.parts):
                        pb[h, i * group + j, rows] = ((prev[h] + odd[h]) + (even[h] + even[h])) * keep
                    prev, xm, c, p = odd, x1, x2, p + 2

    def restricted_rows(i, lv, h=0):
        half = lv.nz // 2
        return ((pb[h, i, pl.ds(lv.z0 - 1, half, stride=2)] + pb[h, i, pl.ds(lv.z0 + 1, half, stride=2)])
                + 2.0 * pb[h, i, pl.ds(lv.z0, half, stride=2)])

    def weights(near, one, other):
        return jnp.where(near == 0, one, jnp.where((near == 1) | (near == -1), other, 0.0)).astype(F32)

    square = (LANES, LANES)
    eighth = 1.0 / (TILE * TILE)

    def restrict_level(src, rhs_ref, lv, table, coarse_rhs, coarse, group, step):
        restrict_planes(src, rhs_ref, lv, table, group)
        lane = lanes_of(square)
        w = jnp.where(lane < coarse.nx, weights(rows_of(square) - 2 * lane, 2.0 * eighth, eighth), 0.0)

        @pl.loop(0, coarse.ny // step)
        def _(i):
            got = [restricted_rows(i * step + j, lv) for j in range(step)]
            if lv.parts > 1:
                odds = [restricted_rows(i * step + j, lv, 1) for j in range(step)]
                got = [((odd + from_below(odd)) + 2.0 * even) * eighth for even, odd in zip(got, odds)]
            else:
                got = dot(stack(got), w)
                got = [got[j * coarse.nz:(j + 1) * coarse.nz] for j in range(step)]
            for j in range(step):
                coarse_rhs[coarse.hx + i * step + j, 0, coarse.own] = got[j]

    def prolong_planes(e, first, e_z0, e_top, e_rows, e_nx, chunk, n_chunks, lv):
        lane, below = lanes_of(square), rows_of(square)
        w = jnp.where(below < e_nx, weights(lane - 2 * below, 4.0, 2.0), 0.0)
        row = e_z0 - e_top - (lv.z0 - lv.top) // 2
        n = lv.rows // 2

        @pl.loop(0, n_chunks)
        def _(i):
            planes = pl.ds(first + i * chunk, chunk)
            got = e[planes, 0, pl.ds(e_top, e_rows)]
            if lv.parts == 1:
                got = dot(got.reshape(chunk * e_rows, LANES), w).reshape(chunk, e_rows, LANES)
            else:
                got = got * 4.0
            pz[pl.ds(i * chunk, chunk), pl.ds(0, e_rows)] = got

        @pl.loop(0, n_chunks)
        def _(i):
            for j in range(chunk):
                a = pz[i * chunk + j, pl.ds(row, n)]
                b = pz[i * chunk + j, pl.ds(row + 1, n)]
                pb[0, i * chunk + j, pl.ds(lv.top, n, stride=2)] = a
                pb[0, i * chunk + j, pl.ds(lv.top + 1, n, stride=2)] = 0.5 * (a + b)

    def correct(dst, lv, table, pairs):
        def load(at, rows):
            a = pb[0, at, rows]
            return [a, 0.5 * (a + from_above(a))] if lv.parts > 1 else [a]

        @pl.loop(0, lv.group * lv.count // (2 * pairs))
        def _(i):
            for top, n in lv.blocks:
                rows = pl.ds(top, n)
                a = load(i * pairs, rows)
                for j in range(pairs):
                    b = load(i * pairs + j + 1, rows)
                    p = lv.begin + 2 * (pairs * i + j)
                    between = every(lambda x, y: 0.5 * (x + y), a, b)
                    for q, add in ((p, a), (p + 1, between)):
                        keep = table_rows(table, valid(lv, q), lv, top, n)
                        put(dst, q, rows, every(lambda x, y: (x + y) * keep, get(dst, q, rows, lv), add))
                    a = b

    row_halo, halo = row_copies(), fine_copies()
    for copy in loads[:4]:
        copy.wait()
    half = TILE // 2
    upper = rows_of((TILE, LANES)) >= half

    @pl.loop(0, chip_y // TILE)
    def _(i):
        for j in range(TILE):
            y = i * TILE + j
            for side, row in enumerate((TILE, TILE + l0.nz - half)):
                send_z[side, y] = sort_x(jnp.where(upper, stage_f[y, pl.ds(row - half, TILE)], stage_u[y, pl.ds(row, TILE)]))
    begin(halo[4:])
    for copy in loads[4:]:
        copy.wait()
    step = 4

    for side, plane in enumerate((0, chip_y - l0.wide)):
        for j in range(l0.wide):
            edge_u[side, j] = sort_x(stage_u[plane + j, inner])
            edge_f[side, j] = sort_x(stage_f[plane + j, inner])
    begin(row_halo)

    def sort_planes(first, n):
        @pl.loop(0, n // step)
        def _(i):
            for j in range(step):
                y = first + i * step + j
                sorted_u[y] = sort_x(stage_u[y, inner])
                sorted_f[y] = sort_x(stage_f[y, inner])

    @pl.loop(0, PARTS)
    def _(part):
        sort_planes((1 - cx) * (chip_y - reach) + part * chunk, chunk)
        for copy in partner_copies(part):
            copy.start()
    begin(halo[:4])
    sort_planes(cx * reach, chip_y - reach)
    for offset in around_me:
        pl.semaphore_signal(ready, inc=1, device_id=peer(offset), device_id_type=MESH)

    some = reach // 3

    @pl.loop(0, PARTS)
    def _(part):
        for copy in partner_copies(part):
            copy.wait_recv()

        @pl.loop(0, chunk // step)
        def _(i):
            for j in range(step):
                k = part * chunk + i * step + j
                for src, buf, dst in ((sorted_u, part_u, u0), (sorted_f, part_f, f0)):
                    put(dst, l0.hx - cx * l0.wide + k, l0.own, split_x(src[cx * (chip_y - reach) + k], buf[k], cx))
    stages = ((u0, v0, cfg.stiffness), (v0, w0, None))
    for k, (src, dst, scale) in enumerate(stages):
        sweep(src, dst, f0, l0, mask0, scale, cut(l0, l0.z0 + k + 1, l0.nz - 2 * (k + 1)))
    arrive(row_halo)
    outer_plane = l0.hx - l0.wide + cx * reach

    for buf, dst in ((recv_yu, u0), (recv_yf, f0)):
        for j in range(l0.wide):
            put(dst, outer_plane + j, l0.own, split_x(buf[0, j], buf[1, j], 0))
    arrive(halo)
    finish(row_halo)
    finish(halo)
    for part in range(PARTS):
        for copy in partner_copies(part):
            copy.wait_send()

    def put_rows(p, side, buf, k):
        row = l0.z0 + l0.nz if side else l0.z0 - half
        for h, part in enumerate(split_x(buf[0, k], buf[1, k], 0)):
            pltpu.store(u0.at[p, h, pl.ds(row, TILE)], part, mask=jnp.logical_not(upper))
            pltpu.store(f0.at[p, h, pl.ds(row - half, TILE)], part, mask=upper)

    @pl.loop(0, reach // some)
    def _(i):
        for j in range(some):
            for side in range(2):
                put_rows(l0.hx - cx * l0.wide + i * some + j, side, recv_z.at[side], i * some + j)
    for side in range(2):
        for j in range(l0.wide):
            put_rows(outer_plane + j, side, recv_d.at[side], j)
    for k, (src, dst, scale) in enumerate(stages):
        ring = l0.wide + 1
        sweep(src, dst, f0, l0, mask0, scale, [(l0.top + k, ring), (l0.z0 + l0.nz - 1 - k, ring)])
        sweep(src, dst, f0, l0, mask0, scale, first=l0.begin + cx * l0.ny, count=1)
    restrict_level(w0, f0, l0, mask0, g1, l1, 4, 4)

    exchange(1)
    first_sweep(a1, g1, l1, mask1)
    sweep(a1, b1, g1, l1, mask1)
    restrict_level(b1, g1, l1, mask1, g2, l2, 8, 8)
    exchange(2)
    first_sweep(a2, g2, l2, mask2)
    sweep(a2, b2, g2, l2, mask2)

    restrict_planes(b2, g2, l2, mask2, 4)
    ny3, nz3, width = l2.ny // 2, l2.nz // 2, l2.nx // 2
    near = rows_of(square) - 2 * (lanes_of(square) % width)
    got = dot(stack([restricted_rows(j, l2) for j in range(ny3)]), weights(near, 2.0 * eighth, eighth))
    tile = (TILE, LANES)
    lane = lanes_of(tile)
    block = lane // width
    blocks = LANES // width
    packed = got[:nz3]
    for j in range(1, ny3):
        packed = jnp.where(block == j, got[j * nz3:(j + 1) * nz3], packed)
    packed = roll(packed, width * cy)
    message[...] = packed
    slot = yb * n_z + cz
    slots[slot] = packed

    def gather_copy(k, at):
        return pltpu.make_async_remote_copy(
            src_ref=message, dst_ref=slots.at[at], send_sem=all_s.at[k], recv_sem=all_r.at[at], device_id=peer(offsets[k]), device_id_type=MESH)

    pl.semaphore_wait(ready, len(around_me))
    for k in range(total - 1):
        gather_copy(k, slot).start()
    for k, offset in enumerate(offsets):
        who = peer(offset)
        gather_copy(k, (who['sy'] * n_x + who['sx']) * n_z + who['sz']).wait_recv()

    tall = nz3 * n_z
    data = pl.ds(TILE, tall)
    for which in range(2):
        for y in range(TILE):
            for at in (0, TILE + tall):
                s3[which, y, pl.ds(at, TILE)] = jnp.zeros(tile, F32)
    live = lane < width * n_y

    @pl.loop(0, n_x)
    def _(core):
        for j in range(ny3):
            for z in range(n_z):
                acc = jnp.zeros(tile, F32)
                for t in range(n_y):
                    acc = jnp.where((block + 2 * blocks - t - j) % blocks == 0, slots[(t * n_x + core) * n_z + z], acc)
                acc = jnp.where(live, roll(acc, back(width * j)), 0.0)
                rows = pl.ds(TILE + nz3 * z, nz3)
                g3[core * ny3 + j, rows] = acc
                s3[0, core * ny3 + j, rows] = acc * NINTH

    long = (tall, LANES)
    along = lanes_of(long)
    x_first, x_last = along % width == 0, along % width == width - 1
    y_first, y_last = along < width, along >= width * (n_y - 1)

    def coarse_sweep(k, carry):
        old, new = k % 2, (k + 1) % 2
        lowest, highest = s3[old, 0, data], s3[old, TILE - 1, data]
        c = lowest
        ym = jnp.where(y_first, 0.0, roll(highest, width % LANES))
        beyond = jnp.where(y_last, 0.0, roll(lowest, back(width)))
        for y in range(TILE):
            yp = s3[old, y + 1, data] if y < TILE - 1 else beyond
            around = (ym + yp) + (s3[old, y, pl.ds(TILE - 1, tall)] + s3[old, y, pl.ds(TILE + 1, tall)])
            left = jnp.where(x_first, 0.0, roll(c, 1))
            right = jnp.where(x_last, 0.0, roll(c, LANES - 1))
            s3[new, y, data] = (around + (left + right) + 3.0 * c + g3[y, data]) * NINTH
            ym, c = c, yp
        return carry
    lax.fori_loop(0, COARSE_SWEEPS - 1, coarse_sweep, 0)

    first = (l2.begin - l2.hx) // 2
    for i in range(e3.shape[0]):
        y = yb * ny3 + (i + first)
        c = s3[(COARSE_SWEEPS - 1) % 2, (y + TILE) % TILE, pl.ds(pl.multiple_of(cz * nz3, TILE), 3 * TILE)]
        ok = (lanes_of(c.shape) < width) & (y >= 0) & (y < row_blocks * ny3)
        e3[i, 0] = jnp.where(ok, roll(c, back((y + TILE) // TILE * width + LANES - width)), 0.0)

    prolong_planes(e3, 0, TILE, 0, 3 * TILE, width, 6, 2, l2)
    correct(b2, l2, mask2, 5)
    sweep(b2, a2, g2, l2, mask2)
    sweep(a2, b2, g2, l2, mask2)
    prolong_planes(b2, l2.hx + (l1.begin - l1.hx) // 2, l2.z0, l2.top, l2.rows, l2.nx, 8, 2, l1)
    correct(b1, l1, mask1, 7)
    sweep(b1, a1, g1, l1, mask1)
    sweep(a1, b1, g1, l1, mask1)
    prolong_planes(b1, l1.hx + (l0.begin - l0.hx) // 2, l1.z0, l1.top, l1.rows, l1.nx, 8, 3, l0)
    correct(w0, l0, mask0, 4)
    sweep(w0, v0, f0, l0, mask0)

    def results(i):
        here, there = pl.ds(i * step, step), pl.ds(cx * l0.ny + i * step, step)
        return pltpu.make_async_remote_copy(
            src_ref=stage_f.at[here, inner], dst_ref=out.at[there], send_sem=out_sem.at[0, i], recv_sem=out_sem.at[1, i],
            device_id={'sx': 1 - cx}, device_id_type=MESH)

    @pl.loop(0, l0.ny // step)
    def _(i):
        for j in range(step):
            k = i * step + j
            p = l0.hx + k
            c = get(v0, p, l0.own, l0)
            around = neighbours(v0, p, get(v0, p - 1, l0.own, l0), c, get(v0, p + 1, l0.own, l0), l0, l0.z0, l0.nz)
            got = every(lambda x, y, g: (x + 3.0 * y + g) * (NINTH / cfg.stiffness), around, c, get(f0, p, l0.own, l0))
            out[cx * l0.ny + k], stage_f[k, inner] = merge_x(*got, cx)
        results(i).start()

    @pl.loop(0, l0.ny // step)
    def _(i):
        results(i).wait()
    drain(1)
    drain(2)

    for k in range(total - 1):
        gather_copy(k, slot).wait_send()


def write_out(held, out, rows, sem):
    def copy_out(i):
        planes = pl.ds(i * TILE, TILE)
        return pltpu.make_async_copy(rows.at[planes], out.at[planes], sem.at[i])

    @pl.loop(0, held.shape[0] // TILE)
    def _(i):
        for j in range(TILE):
            x = held[i * TILE + j]
            lane = lanes_of(x.shape)
            rows[i * TILE + j] = pick(x, lane // 2 + LANES // 2 * ((lane + lax.axis_index('sx')) % 2))
        copy_out(i).start()

    @pl.loop(0, held.shape[0] // TILE)
    def _(i):
        copy_out(i).wait()


def local_cycle(rhs, start, counts, size):
    rhs, start = (jnp.transpose(x, (1, 2, 0)) for x in (rhs, start))
    n_x, n_y, n_z = counts
    chip_y, nz, nx = rhs.shape
    shapes = [(chip_y // n_x >> k, nz >> k, nx * n_x >> k) for k in range(3)]
    l0 = make_level(shapes[0], 6, 8, 4, nz + 8, 2, 8, (shapes[0][0] + 8) // 8, 4, nz + 8)
    l1 = make_level(shapes[1], 8, 16, 8, shapes[1][1] + 16, 2, 14, (shapes[1][0] + 12) // 14, 5, 48)
    l2 = make_level(shapes[2], 8, 16, 8, shapes[2][1] + 16, 2, 10, (shapes[2][0] + 12) // 10, 6, 32)
    cfg = types.SimpleNamespace(levels=(l0, l1, l2), counts=counts, stiffness=float((size + 1) ** 2))
    total = n_x * n_y * n_z

    def vmem(*shape):
        return pltpu.VMEM(shape, F32)

    scratch = [vmem(lv.planes, lv.parts, lv.depth, LANES) for lv, n in ((l0, 4), (l1, 3), (l2, 3)) for _ in range(n)]
    reach = l0.ny + l0.wide
    scratch += [vmem(12, 1, 3 * TILE, LANES), vmem(l1.ny + 8, l1.rows, LANES), vmem(2, l1.ny + 8, l0.depth, LANES)]
    scratch += [vmem(chip_y, l0.depth, LANES)] * 2 + [vmem(reach, nz, LANES)] * 2 + [vmem(chip_y, nz, LANES)] * 2
    scratch += [vmem(2, l0.wide, nz, LANES)] * 2
    scratch += [vmem(2, TILE, l2.nz // 2 * n_z + 2 * TILE, LANES), vmem(TILE, l2.nz // 2 * n_z + 2 * TILE, LANES), vmem(total, TILE, LANES), vmem(TILE, LANES)]
    scratch += [vmem(3, lv.rows, LANES) for lv in (l0, l1, l2)]
    scratch += [vmem(2, chip_y, TILE, LANES), vmem(2, n_x, reach, TILE, LANES), vmem(2, 2, l0.wide, TILE, LANES)]
    scratch += [vmem(2, l0.wide, nz, LANES)] * 2
    sems = [(10,), (2, l0.ny // 4), (16,), (16,), (2, len(SIDES)), (2, len(SIDES)), (total,), (total,), (PARTS, 2), (PARTS, 2)]
    scratch += [pltpu.SemaphoreType.DMA(shape) for shape in sems] + [pltpu.SemaphoreType.REGULAR]
    got = pl.pallas_call(
        functools.partial(kernel, cfg),
        out_shape=pltpu.VMEM(rhs.shape, F32),
        in_specs=[pl.BlockSpec(memory_space=pl.ANY)] * 2,
        out_specs=pl.BlockSpec(memory_space=pltpu.VMEM),
        scratch_shapes=scratch,
        compiler_params=pltpu.CompilerParams(collective_id=0, has_side_effects=True, vmem_limit_bytes=60 * 2 ** 20),
    )(rhs, start)
    got = pl.pallas_call(
        write_out,
        out_shape=jax.ShapeDtypeStruct(rhs.shape, F32),
        in_specs=[pl.BlockSpec(memory_space=pltpu.VMEM)],
        out_specs=pl.BlockSpec(memory_space=pl.ANY),
        scratch_shapes=[vmem(*rhs.shape), pltpu.SemaphoreType.DMA((chip_y // TILE,))],
    )(pltpu.with_memory_space_constraint(got, pltpu.VMEM))
    return jnp.transpose(got, (2, 0, 1))


def solution(mesh):
    counts = (mesh.shape['sx'], mesh.shape['sy'], mesh.shape['sz'])
    spec = P(('dp', 'sx'), 'sy', 'sz')

    def run(rhs_grid, u_start):
        size = rhs_grid.shape[0] // mesh.shape['dp']
        cycle = functools.partial(local_cycle, counts=counts, size=size)
        return jax.shard_map(cycle, mesh=mesh, in_specs=(spec, spec), out_specs=spec, check_vma=False)(rhs_grid, u_start)
    return run
```

```python
import functools
import types
import jax
import jax.numpy as jnp
from jax import lax
from jax.experimental import pallas as pl
from jax.experimental.pallas import tpu as pltpu
from jax.sharding import PartitionSpec as P

F32 = jnp.float32
MESH = pl.DeviceIdType.MESH
LANES = 128
TILE = 8
NINTH = 1.0 / 9.0
COARSE_SWEEPS = 16
PARTS = 3
OPPOSITE = (1, 0, 3, 2, 7, 6, 5, 4)
STEP_Y = (-1, 1, 0, 0, -1, -1, 1, 1)
STEP_Z = (0, 0, -1, 1, -1, 1, -1, 1)
SIDES = range(len(STEP_Y))


def make_level(shape, hx, z0, top, rows, begin, group, count, wide, block):
    ny, nz, nx = shape
    lv = types.SimpleNamespace(ny=ny, nz=nz, nx=nx, hx=hx, z0=z0, top=top, rows=rows, begin=begin, group=group, count=count, wide=wide)
    lv.planes = ny + 2 * hx
    lv.depth = nz + 2 * z0
    lv.parts = max(nx // LANES, 1)
    lv.own = pl.ds(z0, nz)
    lv.all = pl.ds(top, rows)
    lv.block = block
    lv.blocks = cut(lv, top, rows)
    return lv


def cut(lv, top, rows):
    return [(top + i, min(lv.block, rows - i)) for i in range(0, rows, lv.block)]


def lanes_of(shape):
    return lax.broadcasted_iota(jnp.int32, shape, len(shape) - 1)


def rows_of(shape):
    return lax.broadcasted_iota(jnp.int32, shape, len(shape) - 2)


def roll(x, shift):
    return pltpu.roll(x, shift, 1)


def from_below(x):
    return jnp.where(lanes_of(x.shape) == 0, 0.0, roll(x, 1))


def from_above(x):
    return jnp.where(lanes_of(x.shape) == LANES - 1, 0.0, roll(x, LANES - 1))


def halves(x):
    return x[:, :LANES], x[:, LANES:]


def get(ref, p, rows, lv):
    return [ref[p, h, rows] for h in range(lv.parts)]


def put(ref, p, rows, values):
    for h, value in enumerate(values):
        ref[p, h, rows] = value


def every(f, *lists):
    return [f(*values) for values in zip(*lists)]


def join(*parts):
    return jnp.concatenate(parts, axis=1)


def stack(parts):
    return jnp.concatenate(parts, axis=0)


def back(shift):
    return (4 * LANES - shift) % LANES


def flag(condition):
    return jnp.where(condition, 1, 0)


def pick(x, index):
    return jnp.take_along_axis(x, index, axis=1, mode='promise_in_bounds')


def dot(x, w):
    return jnp.dot(x, w, precision=lax.Precision.HIGHEST, preferred_element_type=F32)


def kernel(cfg, rhs, start, out, *scratch):
    (u0, v0, f0, w0, a1, b1, g1, a2, b2, g2, e3, pz, pb, stage_u, stage_f, part_u, part_f, sorted_u, sorted_f, edge_u, edge_f, s3, g3, slots, message, mask0, mask1, mask2,
     send_z, recv_z, recv_d, recv_yu, recv_yf,
     load_sem, out_sem, fine_s, fine_r, send_sem, recv_sem, all_s, all_r, part_s, part_r, ready) = scratch
    l0, l1, l2 = levels = cfg.levels
    masks = (mask0, mask1, mask2)
    n_x, n_y, n_z = cfg.counts
    cx, cy, cz = lax.axis_index('sx'), lax.axis_index('sy'), lax.axis_index('sz')
    total = n_x * n_y * n_z
    row_blocks = n_x * n_y
    yb = cy * n_x + cx

    inner = pl.ds(TILE, l0.nz)
    chip_y = n_x * l0.ny

    def load(planes, rows):
        shifted = pl.ds(rows.start + TILE, rows.size)
        k = len(loads)
        loads.append(pltpu.make_async_copy(start.at[planes, rows], stage_u.at[planes, shifted], load_sem.at[k]))
        loads.append(pltpu.make_async_copy(rhs.at[planes, rows], stage_f.at[planes, shifted], load_sem.at[k + 1]))
    loads = []
    between = pl.ds(TILE, l0.nz - 2 * TILE)
    for row in (0, l0.nz - TILE):
        load(pl.ds(0, chip_y), pl.ds(row, TILE))
    for plane in (0, chip_y - l0.wide):
        load(pl.ds(plane, l0.wide), between)
    load(pl.ds(l0.wide, chip_y - 2 * l0.wide), between)
    for copy in loads:
        copy.start()

    offsets = [(dz, dy, dx) for dz in range(n_z) for dy in range(n_y) for dx in range(n_x)][1:]
    offsets.sort(key=lambda o: -2 * (min(o[0], n_z - o[0]) + min(o[1], n_y - o[1])) - o[2])

    def peer(offset):
        return {name: lax.rem(at + d, n) for name, at, n, d in zip(('sz', 'sy', 'sx'), (cz, cy, cx), (n_z, n_y, n_x), offset)}

    def inside(step, at, count):
        if step == 0:
            return True
        return at > 0 if step < 0 else at < count - 1

    around_me = [o for o in offsets if o[0] in (0, 1, n_z - 1) and o[1] in (0, 1, n_y - 1)]
    barrier = pltpu.get_barrier_semaphore()
    for offset in around_me:
        pl.semaphore_signal(barrier, inc=1, device_id=peer(offset), device_id_type=MESH)
    outer = 2 * cx - 1
    has_outer = (cy + outer >= 0) & (cy + outer < n_y)

    def exists(d):
        return jnp.logical_and(inside(STEP_Y[d], yb, row_blocks), inside(STEP_Z[d], cz, n_z))

    def zero(ref):
        @pl.loop(0, ref.shape[0])
        def _(i):
            ref[i] = jnp.zeros(ref.shape[1:], F32)

    def span(step, first, n, wide, own):
        if step == 0:
            return pl.ds(first, n)
        if step < 0:
            return pl.ds(first if own else first - wide, wide)
        return pl.ds(first + n - wide if own else first + n, wide)

    def region(index, d, own):
        lv, arr = levels[index], (None, g1, g2)[index]
        return arr.at[span(STEP_Y[d], lv.hx, lv.ny, lv.wide, own), 0, span(STEP_Z[d], lv.z0, lv.nz, TILE, own)]

    def halo_copy(index, d, arriving):
        k = index - 1
        at = yb + STEP_Y[d]
        return pltpu.make_async_remote_copy(
            src_ref=region(index, d, not arriving), dst_ref=region(index, d if arriving else OPPOSITE[d], False),
            send_sem=send_sem.at[k, d], recv_sem=recv_sem.at[k, d if arriving else OPPOSITE[d]],
            device_id={'sx': at % n_x, 'sy': at // n_x, 'sz': cz + STEP_Z[d]}, device_id_type=MESH)

    def each(act):
        for d in (4, 5, 6, 7, 2, 3, 0, 1):
            @pl.when(exists(d))
            def _(d=d):
                act(d)

    def exchange(index):
        each(lambda d: halo_copy(index, d, False).start())
        each(lambda d: halo_copy(index, d, True).wait_recv())

    def drain(index):
        each(lambda d: halo_copy(index, d, False).wait_send())

    reach = l0.ny + l0.wide

    def fine_copies():
        got = []

        def add(sends, arrives, src, dst, arrival, k, theirs, **to):
            made = [pltpu.make_async_remote_copy(
                src_ref=a, dst_ref=b, send_sem=fine_s.at[k], recv_sem=fine_r.at[r], device_id=to, device_id_type=MESH)
                for a, b, r in ((src, dst, theirs[0]), (arrival, arrival, theirs[1]))]
            got.append((sends, arrives, *made))
        n = 0
        for z_side, z_step in enumerate((-1, 1)):
            for y_side, y_step in enumerate((-1, 1)):
                edge = pl.ds(0 if y_step < 0 else chip_y - l0.wide, l0.wide)
                to_z = jnp.logical_and(inside(y_step, cy, n_y), inside(z_step, cz, n_z))
                in_z = jnp.logical_and(has_outer, inside(z_step, cz, n_z))
                add(to_z, in_z, send_z.at[z_side, edge], recv_d.at[1 - z_side, cx], recv_d.at[z_side, y_side], n,
                    (8 + 2 * (1 - z_side) + cx, 8 + 2 * z_side + y_side), sx=1 - y_side, sy=cy + y_step, sz=cz + z_step)
                n += 1
        for z_side, z_step in enumerate((-1, 1)):
            for core in range(n_x):
                there = inside(z_step, cz, n_z)
                add(there, there, send_z.at[z_side, pl.ds(core * (chip_y - reach), reach)], recv_z.at[1 - z_side, cx],
                    recv_z.at[z_side, core], n, (12 + 2 * (1 - z_side) + cx, 12 + 2 * z_side + core), sx=core, sz=cz + z_step)
                n += 1
        return got

    def row_copies():
        got = []
        for y_side, y_step in enumerate((-1, 1)):
            for k, (edges, buf) in enumerate(((edge_u, recv_yu), (edge_f, recv_yf))):
                made = [pltpu.make_async_remote_copy(
                    src_ref=a, dst_ref=b, send_sem=fine_s.at[8 + 2 * y_side + k], recv_sem=fine_r.at[2 * r + k],
                    device_id={'sx': 1 - y_side, 'sy': cy + y_step}, device_id_type=MESH)
                    for a, b, r in ((edges.at[y_side], buf.at[cx], cx), (buf.at[y_side], buf.at[y_side], y_side))]
                got.append((inside(y_step, cy, n_y), has_outer, *made))
        return got

    chunk = reach // PARTS

    def partner_copies(part):
        other = pl.ds((1 - cx) * (chip_y - reach) + part * chunk, chunk)
        return [pltpu.make_async_remote_copy(
            src_ref=src.at[other], dst_ref=buf.at[pl.ds(part * chunk, chunk)], send_sem=part_s.at[part, k],
            recv_sem=part_r.at[part, k], device_id={'sx': 1 - cx}, device_id_type=MESH)
            for k, (src, buf) in enumerate(((sorted_u, part_u), (sorted_f, part_f)))]

    def begin(copies):
        for sends, _, copy, _ in copies:
            @pl.when(sends)
            def _(copy=copy):
                copy.start()

    def arrive(copies):
        for _, arrives, _, copy in copies:
            @pl.when(arrives)
            def _(copy=copy):
                copy.wait_recv()

    def finish(copies):
        for sends, _, copy, _ in copies:
            @pl.when(sends)
            def _(copy=copy):
                copy.wait_send()

    @pl.when(jnp.logical_not(has_outer))
    def _():
        for buf in (recv_yu, recv_yf, recv_d):
            for k in range(2):
                zero(buf.at[k])
    for z_side, z_step in enumerate((-1, 1)):
        @pl.when(jnp.logical_not(inside(z_step, cz, n_z)))
        def _(z_side=z_side):
            for core in range(n_x):
                zero(recv_z.at[z_side, core])
            zero(recv_d.at[z_side])
    for index in (1, 2):
        for d in SIDES:
            @pl.when(jnp.logical_not(exists(d)))
            def _(index=index, d=d):
                zero(region(index, d, False))

    for lv, arrays in ((l0, (u0, v0, w0)), (l1, (a1, b1)), (l2, (a2, b2))):
        for arr in arrays:
            for plane, outside in ((lv.hx - 1, yb == 0), (lv.hx + lv.ny, yb == row_blocks - 1)):
                @pl.when(outside)
                def _(arr=arr, lv=lv, plane=plane):
                    put(arr, plane, lv.all, [jnp.zeros((lv.rows, LANES), F32)] * lv.parts)

    for lv, table in zip(levels, masks):
        shape = (lv.rows, LANES)
        z = rows_of(shape) + (lv.top - lv.z0) + cz * lv.nz
        ok = (z >= 0) & (z < n_z * lv.nz) & (lanes_of(shape) < lv.nx)
        table[0] = jnp.zeros(shape, F32)
        table[1] = jnp.where(ok, 1.0, 0.0).astype(F32)
        table[2] = jnp.where(ok, NINTH, 0.0).astype(F32)

    def valid(lv, p):
        y = p + (yb * lv.ny - lv.hx)
        return flag((y >= 0) & (y < row_blocks * lv.ny))

    middle = LANES // 2

    def sort_x(x):
        lane = lanes_of(x.shape)
        return pick(x, 2 * (lane % middle) + (lane // middle + cx) % 2)

    def split_x(first, second, core):
        here = lanes_of(first.shape) // middle == core
        return [jnp.where(here, first, second), roll(jnp.where(here, second, first), middle)]

    def merge_x(even, odd, core):
        here = lanes_of(even.shape) // middle == core
        odd = roll(odd, middle)
        return jnp.where(here, even, odd), jnp.where(here, odd, even)

    pl.semaphore_wait(barrier, len(around_me))

    def across(c, lv):
        if lv.parts > 1:
            even, odd = c
            return [odd + from_below(odd), even + from_above(even)]
        if lv.nx == LANES:
            return [from_below(c[0]) + from_above(c[0])]
        return [roll(c[0], 1) + roll(c[0], LANES - 1)]

    def neighbours(src, p, xm, c, xp, lv, top, n):
        zm, zp = get(src, p, pl.ds(top - 1, n), lv), get(src, p, pl.ds(top + 1, n), lv)
        return every(lambda a, b, d, e, f: ((a + b) + (d + e)) + f, xm, xp, zm, zp, across(c, lv))

    def table_rows(table, k, lv, top, n):
        return table[k, pl.ds(top - lv.top, n)]

    def sweep(src, dst, rhs_ref, lv, table, scale=None, blocks=None, first=None, count=None, group=None):
        group = group or lv.group

        @pl.loop(0, count or lv.count)
        def _(g):
            base = (lv.begin if first is None else first) + g * group
            for top, n in blocks or lv.blocks:
                rows = pl.ds(top, n)
                xm, c = get(src, base - 1, rows, lv), get(src, base, rows, lv)
                for j in range(group):
                    p = base + j
                    xp = get(src, p + 1, rows, lv)
                    t = every(lambda a, b: a + 3.0 * b, neighbours(src, p, xm, c, xp, lv, top, n), c)
                    if scale is not None:
                        t = [x * scale for x in t]
                    keep = table_rows(table, 2 * valid(lv, p), lv, top, n)
                    put(dst, p, rows, every(lambda a, b: (a + b) * keep, t, get(rhs_ref, p, rows, lv)))
                    xm, c = c, xp

    def first_sweep(dst, rhs_ref, lv, table):
        @pl.loop(0, lv.count)
        def _(g):
            for j in range(lv.group):
                p = lv.begin + g * lv.group + j
                dst[p, 0, lv.all] = rhs_ref[p, 0, lv.all] * table[2 * valid(lv, p)]

    def restrict_planes(src, rhs_ref, lv, table, group):
        def res(p, xm, c, xp, top, n):
            return every(lambda a, b, d: a + b - 6.0 * d, neighbours(src, p, xm, c, xp, lv, top, n), get(rhs_ref, p, pl.ds(top, n), lv), c)

        @pl.loop(0, lv.ny // 2 // group)
        def _(i):
            for top, n in lv.blocks:
                rows = pl.ds(top, n)
                p = lv.hx + 2 * group * i
                xm, c = get(src, p - 1, rows, lv), get(src, p, rows, lv)
                prev = res(p - 1, get(src, p - 2, rows, lv), xm, c, top, n)
                prev = [jnp.where((yb > 0) | (i > 0), x, 0.0) for x in prev]
                keep = table_rows(table, 1, lv, top, n)
                for j in range(group):
                    x1, x2 = get(src, p + 1, rows, lv), get(src, p + 2, rows, lv)
                    even = res(p, xm, c, x1, top, n)
                    odd = res(p + 1, c, x1, x2, top, n)
                    for h in range(lv.parts):
                        pb[h, i * group + j, rows] = ((prev[h] + odd[h]) + (even[h] + even[h])) * keep
                    prev, xm, c, p = odd, x1, x2, p + 2

    def restricted_rows(i, lv, h=0):
        half = lv.nz // 2
        return ((pb[h, i, pl.ds(lv.z0 - 1, half, stride=2)] + pb[h, i, pl.ds(lv.z0 + 1, half, stride=2)])
                + 2.0 * pb[h, i, pl.ds(lv.z0, half, stride=2)])

    def weights(near, one, other):
        return jnp.where(near == 0, one, jnp.where((near == 1) | (near == -1), other, 0.0)).astype(F32)

    square = (LANES, LANES)
    eighth = 1.0 / (TILE * TILE)

    def restrict_level(src, rhs_ref, lv, table, coarse_rhs, coarse, group, step):
        restrict_planes(src, rhs_ref, lv, table, group)
        lane = lanes_of(square)
        w = jnp.where(lane < coarse.nx, weights(rows_of(square) - 2 * lane, 2.0 * eighth, eighth), 0.0)

        @pl.loop(0, coarse.ny // step)
        def _(i):
            got = [restricted_rows(i * step + j, lv) for j in range(step)]
            if lv.parts > 1:
                odds = [restricted_rows(i * step + j, lv, 1) for j in range(step)]
                got = [((odd + from_below(odd)) + 2.0 * even) * eighth for even, odd in zip(got, odds)]
            else:
                got = dot(stack(got), w)
                got = [got[j * coarse.nz:(j + 1) * coarse.nz] for j in range(step)]
            for j in range(step):
                coarse_rhs[coarse.hx + i * step + j, 0, coarse.own] = got[j]

    def prolong_planes(e, first, e_z0, e_top, e_rows, e_nx, chunk, n_chunks, lv):
        lane, below = lanes_of(square), rows_of(square)
        w = jnp.where(below < e_nx, weights(lane - 2 * below, 4.0, 2.0), 0.0)
        row = e_z0 - e_top - (lv.z0 - lv.top) // 2
        n = lv.rows // 2

        @pl.loop(0, n_chunks)
        def _(i):
            planes = pl.ds(first + i * chunk, chunk)
            got = e[planes, 0, pl.ds(e_top, e_rows)]
            if lv.parts == 1:
                got = dot(got.reshape(chunk * e_rows, LANES), w).reshape(chunk, e_rows, LANES)
            else:
                got = got * 4.0
            pz[pl.ds(i * chunk, chunk), pl.ds(0, e_rows)] = got

        @pl.loop(0, n_chunks)
        def _(i):
            for j in range(chunk):
                a = pz[i * chunk + j, pl.ds(row, n)]
                b = pz[i * chunk + j, pl.ds(row + 1, n)]
                pb[0, i * chunk + j, pl.ds(lv.top, n, stride=2)] = a
                pb[0, i * chunk + j, pl.ds(lv.top + 1, n, stride=2)] = 0.5 * (a + b)

    def correct(dst, lv, table, pairs):
        def load(at, rows):
            a = pb[0, at, rows]
            return [a, 0.5 * (a + from_above(a))] if lv.parts > 1 else [a]

        @pl.loop(0, lv.group * lv.count // (2 * pairs))
        def _(i):
            for top, n in lv.blocks:
                rows = pl.ds(top, n)
                a = load(i * pairs, rows)
                for j in range(pairs):
                    b = load(i * pairs + j + 1, rows)
                    p = lv.begin + 2 * (pairs * i + j)
                    between = every(lambda x, y: 0.5 * (x + y), a, b)
                    for q, add in ((p, a), (p + 1, between)):
                        keep = table_rows(table, valid(lv, q), lv, top, n)
                        put(dst, q, rows, every(lambda x, y: (x + y) * keep, get(dst, q, rows, lv), add))
                    a = b

    row_halo, halo = row_copies(), fine_copies()
    for copy in loads[:4]:
        copy.wait()
    half = TILE // 2
    upper = rows_of((TILE, LANES)) >= half

    batch = chip_y // 2
    many = rows_of((batch * TILE, LANES)) % TILE >= half

    @pl.loop(0, chip_y // batch)
    def _(i):
        planes = pl.ds(i * batch, batch)
        for side, row in enumerate((TILE, TILE + l0.nz - half)):
            f, u = (x.reshape(batch * TILE, LANES) for x in (stage_f[planes, pl.ds(row - half, TILE)], stage_u[planes, pl.ds(row, TILE)]))
            send_z[side, planes] = sort_x(jnp.where(many, f, u)).reshape(batch, TILE, LANES)
    begin(halo[4:])
    for copy in loads[4:]:
        copy.wait()
    step = 4

    for side, plane in enumerate((0, chip_y - l0.wide)):
        for j in range(l0.wide):
            edge_u[side, j] = sort_x(stage_u[plane + j, inner])
            edge_f[side, j] = sort_x(stage_f[plane + j, inner])
    begin(row_halo)

    def sort_planes(first, n):
        @pl.loop(0, n // step)
        def _(i):
            for j in range(step):
                y = first + i * step + j
                sorted_u[y] = sort_x(stage_u[y, inner])
                sorted_f[y] = sort_x(stage_f[y, inner])

    @pl.loop(0, PARTS)
    def _(part):
        sort_planes((1 - cx) * (chip_y - reach) + part * chunk, chunk)
        for copy in partner_copies(part):
            copy.start()
    begin(halo[:4])
    sort_planes(cx * reach, chip_y - reach)
    for offset in around_me:
        pl.semaphore_signal(ready, inc=1, device_id=peer(offset), device_id_type=MESH)

    some = reach // 3

    @pl.loop(0, PARTS)
    def _(part):
        for copy in partner_copies(part):
            copy.wait_recv()

        @pl.loop(0, chunk // step)
        def _(i):
            for j in range(step):
                k = part * chunk + i * step + j
                for src, buf, dst in ((sorted_u, part_u, u0), (sorted_f, part_f, f0)):
                    put(dst, l0.hx - cx * l0.wide + k, l0.own, split_x(src[cx * (chip_y - reach) + k], buf[k], cx))
    stages = ((u0, v0, cfg.stiffness), (v0, w0, None))
    for k, (src, dst, scale) in enumerate(stages):
        sweep(src, dst, f0, l0, mask0, scale, cut(l0, l0.z0 + k + 1, l0.nz - 2 * (k + 1)))
    arrive(row_halo)
    outer_plane = l0.hx - l0.wide + cx * reach

    for buf, dst in ((recv_yu, u0), (recv_yf, f0)):
        for j in range(l0.wide):
            put(dst, outer_plane + j, l0.own, split_x(buf[0, j], buf[1, j], 0))
    arrive(halo)
    finish(row_halo)
    finish(halo)
    for part in range(PARTS):
        for copy in partner_copies(part):
            copy.wait_send()

    def put_rows(p, side, buf, k):
        row = l0.z0 + l0.nz if side else l0.z0 - half
        for h, part in enumerate(split_x(buf[0, k], buf[1, k], 0)):
            pltpu.store(u0.at[p, h, pl.ds(row, TILE)], part, mask=jnp.logical_not(upper))
            pltpu.store(f0.at[p, h, pl.ds(row - half, TILE)], part, mask=upper)

    @pl.loop(0, reach // some)
    def _(i):
        for j in range(some):
            for side in range(2):
                put_rows(l0.hx - cx * l0.wide + i * some + j, side, recv_z.at[side], i * some + j)
    for side in range(2):
        for j in range(l0.wide):
            put_rows(outer_plane + j, side, recv_d.at[side], j)
    for k, (src, dst, scale) in enumerate(stages):
        ring = l0.wide + 1
        sweep(src, dst, f0, l0, mask0, scale, [(l0.top + k, ring), (l0.z0 + l0.nz - 1 - k, ring)], count=2, group=20)
        sweep(src, dst, f0, l0, mask0, scale, first=l0.begin + cx * l0.ny, count=1)
    restrict_level(w0, f0, l0, mask0, g1, l1, 4, 4)

    exchange(1)
    first_sweep(a1, g1, l1, mask1)
    sweep(a1, b1, g1, l1, mask1)
    restrict_level(b1, g1, l1, mask1, g2, l2, 8, 8)
    exchange(2)
    first_sweep(a2, g2, l2, mask2)
    sweep(a2, b2, g2, l2, mask2)

    restrict_planes(b2, g2, l2, mask2, 4)
    ny3, nz3, width = l2.ny // 2, l2.nz // 2, l2.nx // 2
    near = rows_of(square) - 2 * (lanes_of(square) % width)
    got = dot(stack([restricted_rows(j, l2) for j in range(ny3)]), weights(near, 2.0 * eighth, eighth))
    tile = (TILE, LANES)
    lane = lanes_of(tile)
    block = lane // width
    blocks = LANES // width
    packed = got[:nz3]
    for j in range(1, ny3):
        packed = jnp.where(block == j, got[j * nz3:(j + 1) * nz3], packed)
    packed = roll(packed, width * cy)
    message[...] = packed
    slot = yb * n_z + cz
    slots[slot] = packed

    def gather_copy(k, at):
        return pltpu.make_async_remote_copy(
            src_ref=message, dst_ref=slots.at[at], send_sem=all_s.at[k], recv_sem=all_r.at[at], device_id=peer(offsets[k]), device_id_type=MESH)

    pl.semaphore_wait(ready, len(around_me))
    for k in range(total - 1):
        gather_copy(k, slot).start()
    for k, offset in enumerate(offsets):
        who = peer(offset)
        gather_copy(k, (who['sy'] * n_x + who['sx']) * n_z + who['sz']).wait_recv()

    tall = nz3 * n_z
    data = pl.ds(TILE, tall)
    for which in range(2):
        for y in range(TILE):
            for at in (0, TILE + tall):
                s3[which, y, pl.ds(at, TILE)] = jnp.zeros(tile, F32)
    live = lane < width * n_y

    @pl.loop(0, n_x)
    def _(core):
        for j in range(ny3):
            for z in range(n_z):
                acc = jnp.zeros(tile, F32)
                for t in range(n_y):
                    acc = jnp.where((block + 2 * blocks - t - j) % blocks == 0, slots[(t * n_x + core) * n_z + z], acc)
                acc = jnp.where(live, roll(acc, back(width * j)), 0.0)
                rows = pl.ds(TILE + nz3 * z, nz3)
                g3[core * ny3 + j, rows] = acc
                s3[0, core * ny3 + j, rows] = acc * NINTH

    long = (tall, LANES)
    along = lanes_of(long)
    x_first, x_last = along % width == 0, along % width == width - 1
    y_first, y_last = along < width, along >= width * (n_y - 1)

    def coarse_sweep(k, carry):
        old, new = k % 2, (k + 1) % 2
        lowest, highest = s3[old, 0, data], s3[old, TILE - 1, data]
        c = lowest
        ym = jnp.where(y_first, 0.0, roll(highest, width % LANES))
        beyond = jnp.where(y_last, 0.0, roll(lowest, back(width)))
        for y in range(TILE):
            yp = s3[old, y + 1, data] if y < TILE - 1 else beyond
            around = (ym + yp) + (s3[old, y, pl.ds(TILE - 1, tall)] + s3[old, y, pl.ds(TILE + 1, tall)])
            left = jnp.where(x_first, 0.0, roll(c, 1))
            right = jnp.where(x_last, 0.0, roll(c, LANES - 1))
            s3[new, y, data] = (around + (left + right) + 3.0 * c + g3[y, data]) * NINTH
            ym, c = c, yp
        return carry
    lax.fori_loop(0, COARSE_SWEEPS - 1, coarse_sweep, 0)

    first = (l2.begin - l2.hx) // 2
    for i in range(e3.shape[0]):
        y = yb * ny3 + (i + first)
        c = s3[(COARSE_SWEEPS - 1) % 2, (y + TILE) % TILE, pl.ds(pl.multiple_of(cz * nz3, TILE), 3 * TILE)]
        ok = (lanes_of(c.shape) < width) & (y >= 0) & (y < row_blocks * ny3)
        e3[i, 0] = jnp.where(ok, roll(c, back((y + TILE) // TILE * width + LANES - width)), 0.0)

    prolong_planes(e3, 0, TILE, 0, 3 * TILE, width, 6, 2, l2)
    correct(b2, l2, mask2, 5)
    sweep(b2, a2, g2, l2, mask2)
    sweep(a2, b2, g2, l2, mask2)
    prolong_planes(b2, l2.hx + (l1.begin - l1.hx) // 2, l2.z0, l2.top, l2.rows, l2.nx, 8, 2, l1)
    correct(b1, l1, mask1, 7)
    sweep(b1, a1, g1, l1, mask1)
    sweep(a1, b1, g1, l1, mask1)
    prolong_planes(b1, l1.hx + (l0.begin - l0.hx) // 2, l1.z0, l1.top, l1.rows, l1.nx, 8, 3, l0)
    correct(w0, l0, mask0, 4)
    sweep(w0, v0, f0, l0, mask0)

    def results(i):
        here, there = pl.ds(i * step, step), pl.ds(cx * l0.ny + i * step, step)
        return pltpu.make_async_remote_copy(
            src_ref=stage_f.at[here, inner], dst_ref=out.at[there], send_sem=out_sem.at[0, i], recv_sem=out_sem.at[1, i],
            device_id={'sx': 1 - cx}, device_id_type=MESH)

    @pl.loop(0, l0.ny // step)
    def _(i):
        for j in range(step):
            k = i * step + j
            p = l0.hx + k
            c = get(v0, p, l0.own, l0)
            around = neighbours(v0, p, get(v0, p - 1, l0.own, l0), c, get(v0, p + 1, l0.own, l0), l0, l0.z0, l0.nz)
            got = every(lambda x, y, g: (x + 3.0 * y + g) * (NINTH / cfg.stiffness), around, c, get(f0, p, l0.own, l0))
            out[cx * l0.ny + k], stage_f[k, inner] = merge_x(*got, cx)
        results(i).start()

    @pl.loop(0, l0.ny // step)
    def _(i):
        results(i).wait()
    drain(1)
    drain(2)

    for k in range(total - 1):
        gather_copy(k, slot).wait_send()


def write_out(held, out, rows, sem):
    batch = 2 * TILE

    def copy_out(i):
        planes = pl.ds(i * batch, batch)
        return pltpu.make_async_copy(rows.at[planes], out.at[planes], sem.at[i])

    @pl.loop(0, held.shape[0] // batch)
    def _(i):
        for j in range(batch):
            x = held[i * batch + j]
            lane = lanes_of(x.shape)
            rows[i * batch + j] = pick(x, lane // 2 + LANES // 2 * ((lane + lax.axis_index('sx')) % 2))
        copy_out(i).start()

    @pl.loop(0, held.shape[0] // batch)
    def _(i):
        copy_out(i).wait()


def local_cycle(rhs, start, counts, size):
    rhs, start = (jnp.transpose(x, (1, 2, 0)) for x in (rhs, start))
    n_x, n_y, n_z = counts
    chip_y, nz, nx = rhs.shape
    shapes = [(chip_y // n_x >> k, nz >> k, nx * n_x >> k) for k in range(3)]
    l0 = make_level(shapes[0], 6, 8, 4, nz + 8, 2, 8, (shapes[0][0] + 8) // 8, 4, nz + 8)
    l1 = make_level(shapes[1], 8, 16, 8, shapes[1][1] + 16, 2, 14, (shapes[1][0] + 12) // 14, 5, 48)
    l2 = make_level(shapes[2], 8, 16, 8, shapes[2][1] + 16, 2, 10, (shapes[2][0] + 12) // 10, 6, 32)
    cfg = types.SimpleNamespace(levels=(l0, l1, l2), counts=counts, stiffness=float((size + 1) ** 2))
    total = n_x * n_y * n_z

    def vmem(*shape):
        return pltpu.VMEM(shape, F32)

    scratch = [vmem(lv.planes, lv.parts, lv.depth, LANES) for lv, n in ((l0, 4), (l1, 3), (l2, 3)) for _ in range(n)]
    reach = l0.ny + l0.wide
    scratch += [vmem(12, 1, 3 * TILE, LANES), vmem(l1.ny + 8, l1.rows, LANES), vmem(2, l1.ny + 8, l0.depth, LANES)]
    scratch += [vmem(chip_y, l0.depth, LANES)] * 2 + [vmem(reach, nz, LANES)] * 2 + [vmem(chip_y, nz, LANES)] * 2
    scratch += [vmem(2, l0.wide, nz, LANES)] * 2
    scratch += [vmem(2, TILE, l2.nz // 2 * n_z + 2 * TILE, LANES), vmem(TILE, l2.nz // 2 * n_z + 2 * TILE, LANES), vmem(total, TILE, LANES), vmem(TILE, LANES)]
    scratch += [vmem(3, lv.rows, LANES) for lv in (l0, l1, l2)]
    scratch += [vmem(2, chip_y, TILE, LANES), vmem(2, n_x, reach, TILE, LANES), vmem(2, 2, l0.wide, TILE, LANES)]
    scratch += [vmem(2, l0.wide, nz, LANES)] * 2
    sems = [(10,), (2, l0.ny // 4), (16,), (16,), (2, len(SIDES)), (2, len(SIDES)), (total,), (total,), (PARTS, 2), (PARTS, 2)]
    scratch += [pltpu.SemaphoreType.DMA(shape) for shape in sems] + [pltpu.SemaphoreType.REGULAR]
    got = pl.pallas_call(
        functools.partial(kernel, cfg),
        out_shape=pltpu.VMEM(rhs.shape, F32),
        in_specs=[pl.BlockSpec(memory_space=pl.ANY)] * 2,
        out_specs=pl.BlockSpec(memory_space=pltpu.VMEM),
        scratch_shapes=scratch,
        compiler_params=pltpu.CompilerParams(collective_id=0, has_side_effects=True, vmem_limit_bytes=60 * 2 ** 20),
    )(rhs, start)
    got = pl.pallas_call(
        write_out,
        out_shape=jax.ShapeDtypeStruct(rhs.shape, F32),
        in_specs=[pl.BlockSpec(memory_space=pltpu.VMEM)],
        out_specs=pl.BlockSpec(memory_space=pl.ANY),
        scratch_shapes=[vmem(*rhs.shape), pltpu.SemaphoreType.DMA((chip_y // TILE,))],
    )(pltpu.with_memory_space_constraint(got, pltpu.VMEM))
    return jnp.transpose(got, (2, 0, 1))


def solution(mesh):
    counts = (mesh.shape['sx'], mesh.shape['sy'], mesh.shape['sz'])
    spec = P(('dp', 'sx'), 'sy', 'sz')

    def run(rhs_grid, u_start):
        size = rhs_grid.shape[0] // mesh.shape['dp']
        cycle = functools.partial(local_cycle, counts=counts, size=size)
        return jax.shard_map(cycle, mesh=mesh, in_specs=(spec, spec), out_specs=spec, check_vma=False)(rhs_grid, u_start)
    return run
```

```python
import functools
import types
import jax
import jax.numpy as jnp
from jax import lax
from jax.experimental import pallas as pl
from jax.experimental.pallas import tpu as pltpu
from jax.sharding import PartitionSpec as P

F32 = jnp.float32
MESH = pl.DeviceIdType.MESH
LANES = 128
TILE = 8
NINTH = 1.0 / 9.0
COARSE_SWEEPS = 16
PARTS = 3
OPPOSITE = (1, 0, 3, 2, 7, 6, 5, 4)
STEP_Y = (-1, 1, 0, 0, -1, -1, 1, 1)
STEP_Z = (0, 0, -1, 1, -1, 1, -1, 1)
SIDES = range(len(STEP_Y))


def make_level(shape, hx, z0, top, rows, begin, group, count, wide, block):
    ny, nz, nx = shape
    lv = types.SimpleNamespace(ny=ny, nz=nz, nx=nx, hx=hx, z0=z0, top=top, rows=rows, begin=begin, group=group, count=count, wide=wide)
    lv.planes = ny + 2 * hx
    lv.depth = nz + 2 * z0
    lv.parts = max(nx // LANES, 1)
    lv.own = pl.ds(z0, nz)
    lv.all = pl.ds(top, rows)
    lv.block = block
    lv.blocks = cut(lv, top, rows)
    return lv


def cut(lv, top, rows):
    return [(top + i, min(lv.block, rows - i)) for i in range(0, rows, lv.block)]


def lanes_of(shape):
    return lax.broadcasted_iota(jnp.int32, shape, len(shape) - 1)


def rows_of(shape):
    return lax.broadcasted_iota(jnp.int32, shape, len(shape) - 2)


def roll(x, shift):
    return pltpu.roll(x, shift, 1)


def ends(n):
    lane = lanes_of((n, LANES))
    return lane == 0, lane == LANES - 1, jnp.zeros((n, LANES), F32)


def from_below(x, outer):
    return lax.select(outer[0], outer[2], roll(x, 1))


def from_above(x, outer):
    return lax.select(outer[1], outer[2], roll(x, LANES - 1))


def halves(x):
    return x[:, :LANES], x[:, LANES:]


def get(ref, p, rows, lv):
    return [ref[p, h, rows] for h in range(lv.parts)]


def put(ref, p, rows, values):
    for h, value in enumerate(values):
        ref[p, h, rows] = value


def every(f, *lists):
    return [f(*values) for values in zip(*lists)]


def join(*parts):
    return jnp.concatenate(parts, axis=1)


def stack(parts):
    return jnp.concatenate(parts, axis=0)


def back(shift):
    return (4 * LANES - shift) % LANES


def flag(condition):
    return jnp.where(condition, 1, 0)


def pick(x, index):
    return jnp.take_along_axis(x, index, axis=1, mode='promise_in_bounds')


def dot(x, w):
    return jnp.dot(x, w, precision=lax.Precision.HIGHEST, preferred_element_type=F32)


def kernel(cfg, rhs, start, out, *scratch):
    (u0, v0, f0, w0, a1, b1, g1, a2, b2, g2, e3, pz, pb, stage_u, stage_f, part_u, part_f, sorted_u, sorted_f, edge_u, edge_f, s3, g3, slots, message, mask0, mask1, mask2,
     send_z, recv_z, recv_d, recv_yu, recv_yf,
     load_sem, out_sem, fine_s, fine_r, send_sem, recv_sem, all_s, all_r, part_s, part_r, ready) = scratch
    l0, l1, l2 = levels = cfg.levels
    masks = (mask0, mask1, mask2)
    n_x, n_y, n_z = cfg.counts
    cx, cy, cz = lax.axis_index('sx'), lax.axis_index('sy'), lax.axis_index('sz')
    total = n_x * n_y * n_z
    row_blocks = n_x * n_y
    yb = cy * n_x + cx

    inner = pl.ds(TILE, l0.nz)
    chip_y = n_x * l0.ny

    def load(planes, rows):
        shifted = pl.ds(rows.start + TILE, rows.size)
        k = len(loads)
        loads.append(pltpu.make_async_copy(start.at[planes, rows], stage_u.at[planes, shifted], load_sem.at[k]))
        loads.append(pltpu.make_async_copy(rhs.at[planes, rows], stage_f.at[planes, shifted], load_sem.at[k + 1]))
    loads = []
    between = pl.ds(TILE, l0.nz - 2 * TILE)
    for row in (0, l0.nz - TILE):
        load(pl.ds(0, chip_y), pl.ds(row, TILE))
    for plane in (0, chip_y - l0.wide):
        load(pl.ds(plane, l0.wide), between)
    load(pl.ds(l0.wide, chip_y - 2 * l0.wide), between)
    for copy in loads:
        copy.start()

    offsets = [(dz, dy, dx) for dz in range(n_z) for dy in range(n_y) for dx in range(n_x)][1:]
    offsets.sort(key=lambda o: -2 * (min(o[0], n_z - o[0]) + min(o[1], n_y - o[1])) - o[2])

    def peer(offset):
        return {name: lax.rem(at + d, n) for name, at, n, d in zip(('sz', 'sy', 'sx'), (cz, cy, cx), (n_z, n_y, n_x), offset)}

    def inside(step, at, count):
        if step == 0:
            return True
        return at > 0 if step < 0 else at < count - 1

    around_me = [o for o in offsets if o[0] in (0, 1, n_z - 1) and o[1] in (0, 1, n_y - 1)]
    barrier = pltpu.get_barrier_semaphore()
    for offset in around_me:
        pl.semaphore_signal(barrier, inc=1, device_id=peer(offset), device_id_type=MESH)
    outer = 2 * cx - 1
    has_outer = (cy + outer >= 0) & (cy + outer < n_y)

    def exists(d):
        return jnp.logical_and(inside(STEP_Y[d], yb, row_blocks), inside(STEP_Z[d], cz, n_z))

    def zero(ref):
        @pl.loop(0, ref.shape[0])
        def _(i):
            ref[i] = jnp.zeros(ref.shape[1:], F32)

    def span(step, first, n, wide, own):
        if step == 0:
            return pl.ds(first, n)
        if step < 0:
            return pl.ds(first if own else first - wide, wide)
        return pl.ds(first + n - wide if own else first + n, wide)

    def region(index, d, own):
        lv, arr = levels[index], (None, g1, g2)[index]
        return arr.at[span(STEP_Y[d], lv.hx, lv.ny, lv.wide, own), 0, span(STEP_Z[d], lv.z0, lv.nz, TILE, own)]

    def halo_copy(index, d, arriving):
        k = index - 1
        at = yb + STEP_Y[d]
        return pltpu.make_async_remote_copy(
            src_ref=region(index, d, not arriving), dst_ref=region(index, d if arriving else OPPOSITE[d], False),
            send_sem=send_sem.at[k, d], recv_sem=recv_sem.at[k, d if arriving else OPPOSITE[d]],
            device_id={'sx': at % n_x, 'sy': at // n_x, 'sz': cz + STEP_Z[d]}, device_id_type=MESH)

    def each(act):
        for d in (2, 3, 4, 5, 6, 7, 0, 1):
            @pl.when(exists(d))
            def _(d=d):
                act(d)

    def exchange(index):
        each(lambda d: halo_copy(index, d, False).start())
        each(lambda d: halo_copy(index, d, True).wait_recv())

    def drain(index):
        each(lambda d: halo_copy(index, d, False).wait_send())

    reach = l0.ny + l0.wide

    def fine_copies():
        got = []

        def add(sends, arrives, src, dst, arrival, k, theirs, **to):
            made = [pltpu.make_async_remote_copy(
                src_ref=a, dst_ref=b, send_sem=fine_s.at[k], recv_sem=fine_r.at[r], device_id=to, device_id_type=MESH)
                for a, b, r in ((src, dst, theirs[0]), (arrival, arrival, theirs[1]))]
            got.append((sends, arrives, *made))
        n = 0
        for z_side, z_step in enumerate((-1, 1)):
            for y_side, y_step in enumerate((-1, 1)):
                edge = pl.ds(0 if y_step < 0 else chip_y - l0.wide, l0.wide)
                to_z = jnp.logical_and(inside(y_step, cy, n_y), inside(z_step, cz, n_z))
                in_z = jnp.logical_and(has_outer, inside(z_step, cz, n_z))
                add(to_z, in_z, send_z.at[z_side, edge], recv_d.at[1 - z_side, cx], recv_d.at[z_side, y_side], n,
                    (8 + 2 * (1 - z_side) + cx, 8 + 2 * z_side + y_side), sx=1 - y_side, sy=cy + y_step, sz=cz + z_step)
                n += 1
        for z_side, z_step in enumerate((-1, 1)):
            for core in range(n_x):
                there = inside(z_step, cz, n_z)
                add(there, there, send_z.at[z_side, pl.ds(core * (chip_y - reach), reach)], recv_z.at[1 - z_side, cx],
                    recv_z.at[z_side, core], n, (12 + 2 * (1 - z_side) + cx, 12 + 2 * z_side + core), sx=core, sz=cz + z_step)
                n += 1
        return got

    def row_copies():
        got = []
        for y_side, y_step in enumerate((-1, 1)):
            for k, (edges, buf) in enumerate(((edge_u, recv_yu), (edge_f, recv_yf))):
                made = [pltpu.make_async_remote_copy(
                    src_ref=a, dst_ref=b, send_sem=fine_s.at[8 + 2 * y_side + k], recv_sem=fine_r.at[2 * r + k],
                    device_id={'sx': 1 - y_side, 'sy': cy + y_step}, device_id_type=MESH)
                    for a, b, r in ((edges.at[y_side], buf.at[cx], cx), (buf.at[y_side], buf.at[y_side], y_side))]
                got.append((inside(y_step, cy, n_y), has_outer, *made))
        return got

    chunk = reach // PARTS

    def partner_copies(part):
        other = pl.ds((1 - cx) * (chip_y - reach) + part * chunk, chunk)
        return [pltpu.make_async_remote_copy(
            src_ref=src.at[other], dst_ref=buf.at[pl.ds(part * chunk, chunk)], send_sem=part_s.at[part, k],
            recv_sem=part_r.at[part, k], device_id={'sx': 1 - cx}, device_id_type=MESH)
            for k, (src, buf) in enumerate(((sorted_u, part_u), (sorted_f, part_f)))]

    def begin(copies):
        for sends, _, copy, _ in copies:
            @pl.when(sends)
            def _(copy=copy):
                copy.start()

    def arrive(copies):
        for _, arrives, _, copy in copies:
            @pl.when(arrives)
            def _(copy=copy):
                copy.wait_recv()

    def finish(copies):
        for sends, _, copy, _ in copies:
            @pl.when(sends)
            def _(copy=copy):
                copy.wait_send()

    @pl.when(jnp.logical_not(has_outer))
    def _():
        for buf in (recv_yu, recv_yf, recv_d):
            for k in range(2):
                zero(buf.at[k])
    for z_side, z_step in enumerate((-1, 1)):
        @pl.when(jnp.logical_not(inside(z_step, cz, n_z)))
        def _(z_side=z_side):
            for core in range(n_x):
                zero(recv_z.at[z_side, core])
            zero(recv_d.at[z_side])
    for index in (1, 2):
        for d in SIDES:
            @pl.when(jnp.logical_not(exists(d)))
            def _(index=index, d=d):
                zero(region(index, d, False))

    for lv, arrays in ((l0, (u0, v0, w0)), (l1, (a1, b1)), (l2, (a2, b2))):
        for arr in arrays:
            for plane, outside in ((lv.hx - 1, yb == 0), (lv.hx + lv.ny, yb == row_blocks - 1)):
                @pl.when(outside)
                def _(arr=arr, lv=lv, plane=plane):
                    put(arr, plane, lv.all, [jnp.zeros((lv.rows, LANES), F32)] * lv.parts)

    for lv, table in zip(levels, masks):
        shape = (lv.rows, LANES)
        z = rows_of(shape) + (lv.top - lv.z0) + cz * lv.nz
        ok = (z >= 0) & (z < n_z * lv.nz) & (lanes_of(shape) < lv.nx)
        table[0] = jnp.zeros(shape, F32)
        table[1] = jnp.where(ok, 1.0, 0.0).astype(F32)
        table[2] = jnp.where(ok, NINTH, 0.0).astype(F32)

    def valid(lv, p):
        y = p + (yb * lv.ny - lv.hx)
        return flag((y >= 0) & (y < row_blocks * lv.ny))

    middle = LANES // 2

    def sort_x(x):
        lane = lanes_of(x.shape)
        return pick(x, 2 * (lane % middle) + (lane // middle + cx) % 2)

    def split_x(first, second, core):
        here = lanes_of(first.shape) // middle == core
        return [jnp.where(here, first, second), roll(jnp.where(here, second, first), middle)]

    def merge_x(even, odd, core):
        here = lanes_of(even.shape) // middle == core
        odd = roll(odd, middle)
        return jnp.where(here, even, odd), jnp.where(here, odd, even)

    pl.semaphore_wait(barrier, len(around_me))

    def across(c, lv, outer):
        if lv.parts > 1:
            even, odd = c
            return [odd + from_below(odd, outer), even + from_above(even, outer)]
        if lv.nx == LANES:
            return [from_below(c[0], outer) + from_above(c[0], outer)]
        return [roll(c[0], 1) + roll(c[0], LANES - 1)]

    def neighbours(src, p, xm, c, xp, lv, top, n, outer):
        zm, zp = get(src, p, pl.ds(top - 1, n), lv), get(src, p, pl.ds(top + 1, n), lv)
        return every(lambda a, b, d, e, f: ((a + b) + (d + e)) + f, xm, xp, zm, zp, across(c, lv, outer))

    def table_rows(table, k, lv, top, n):
        return table[k, pl.ds(top - lv.top, n)]

    def sweep(src, dst, rhs_ref, lv, table, scale=None, blocks=None, first=None, count=None, group=None):
        group, blocks = group or lv.group, blocks or lv.blocks
        outers = {n: ends(n) for _, n in blocks}

        @pl.loop(0, count or lv.count)
        def _(g):
            base = (lv.begin if first is None else first) + g * group
            for top, n in blocks:
                rows = pl.ds(top, n)
                xm, c = get(src, base - 1, rows, lv), get(src, base, rows, lv)
                for j in range(group):
                    p = base + j
                    xp = get(src, p + 1, rows, lv)
                    t = every(lambda a, b: a + 3.0 * b, neighbours(src, p, xm, c, xp, lv, top, n, outers[n]), c)
                    if scale is not None:
                        t = [x * scale for x in t]
                    keep = table_rows(table, 2 * valid(lv, p), lv, top, n)
                    put(dst, p, rows, every(lambda a, b: (a + b) * keep, t, get(rhs_ref, p, rows, lv)))
                    xm, c = c, xp

    def first_sweep(dst, rhs_ref, lv, table):
        @pl.loop(0, lv.count)
        def _(g):
            for j in range(lv.group):
                p = lv.begin + g * lv.group + j
                dst[p, 0, lv.all] = rhs_ref[p, 0, lv.all] * table[2 * valid(lv, p)]

    def restrict_planes(src, rhs_ref, lv, table, group):
        outers = {n: ends(n) for _, n in lv.blocks}

        def res(p, xm, c, xp, top, n):
            return every(lambda a, b, d: a + b - 6.0 * d, neighbours(src, p, xm, c, xp, lv, top, n, outers[n]), get(rhs_ref, p, pl.ds(top, n), lv), c)

        @pl.loop(0, lv.ny // 2 // group)
        def _(i):
            for top, n in lv.blocks:
                rows = pl.ds(top, n)
                p = lv.hx + 2 * group * i
                xm, c = get(src, p - 1, rows, lv), get(src, p, rows, lv)
                prev = res(p - 1, get(src, p - 2, rows, lv), xm, c, top, n)
                prev = [jnp.where((yb > 0) | (i > 0), x, 0.0) for x in prev]
                keep = table_rows(table, 1, lv, top, n)
                for j in range(group):
                    x1, x2 = get(src, p + 1, rows, lv), get(src, p + 2, rows, lv)
                    even = res(p, xm, c, x1, top, n)
                    odd = res(p + 1, c, x1, x2, top, n)
                    for h in range(lv.parts):
                        pb[h, i * group + j, rows] = ((prev[h] + odd[h]) + (even[h] + even[h])) * keep
                    prev, xm, c, p = odd, x1, x2, p + 2

    def restricted_rows(i, lv, h=0):
        half = lv.nz // 2
        return ((pb[h, i, pl.ds(lv.z0 - 1, half, stride=2)] + pb[h, i, pl.ds(lv.z0 + 1, half, stride=2)])
                + 2.0 * pb[h, i, pl.ds(lv.z0, half, stride=2)])

    def weights(near, one, other):
        return jnp.where(near == 0, one, jnp.where((near == 1) | (near == -1), other, 0.0)).astype(F32)

    square = (LANES, LANES)
    eighth = 1.0 / (TILE * TILE)

    def restrict_level(src, rhs_ref, lv, table, coarse_rhs, coarse, group, step):
        restrict_planes(src, rhs_ref, lv, table, group)
        lane = lanes_of(square)
        outer = ends(coarse.nz)
        w = jnp.where(lane < coarse.nx, weights(rows_of(square) - 2 * lane, 2.0 * eighth, eighth), 0.0)

        @pl.loop(0, coarse.ny // step)
        def _(i):
            got = [restricted_rows(i * step + j, lv) for j in range(step)]
            if lv.parts > 1:
                odds = [restricted_rows(i * step + j, lv, 1) for j in range(step)]
                got = [((odd + from_below(odd, outer)) + 2.0 * even) * eighth for even, odd in zip(got, odds)]
            else:
                got = dot(stack(got), w)
                got = [got[j * coarse.nz:(j + 1) * coarse.nz] for j in range(step)]
            for j in range(step):
                coarse_rhs[coarse.hx + i * step + j, 0, coarse.own] = got[j]

    def prolong_planes(e, first, e_z0, e_top, e_rows, e_nx, chunk, n_chunks, lv):
        lane, below = lanes_of(square), rows_of(square)
        w = jnp.where(below < e_nx, weights(lane - 2 * below, 4.0, 2.0), 0.0)
        row = e_z0 - e_top - (lv.z0 - lv.top) // 2
        n = lv.rows // 2

        @pl.loop(0, n_chunks)
        def _(i):
            planes = pl.ds(first + i * chunk, chunk)
            got = e[planes, 0, pl.ds(e_top, e_rows)]
            if lv.parts == 1:
                got = dot(got.reshape(chunk * e_rows, LANES), w).reshape(chunk, e_rows, LANES)
            else:
                got = got * 4.0
            pz[pl.ds(i * chunk, chunk), pl.ds(0, e_rows)] = got

        @pl.loop(0, n_chunks)
        def _(i):
            for j in range(chunk):
                a = pz[i * chunk + j, pl.ds(row, n)]
                b = pz[i * chunk + j, pl.ds(row + 1, n)]
                pb[0, i * chunk + j, pl.ds(lv.top, n, stride=2)] = a
                pb[0, i * chunk + j, pl.ds(lv.top + 1, n, stride=2)] = 0.5 * (a + b)

    def correct(dst, lv, table, pairs):
        def load(at, rows):
            a = pb[0, at, rows]
            return [a, 0.5 * (a + from_above(a, outers[a.shape[0]]))] if lv.parts > 1 else [a]
        outers = {n: ends(n) for _, n in lv.blocks}

        @pl.loop(0, lv.group * lv.count // (2 * pairs))
        def _(i):
            for top, n in lv.blocks:
                rows = pl.ds(top, n)
                a = load(i * pairs, rows)
                for j in range(pairs):
                    b = load(i * pairs + j + 1, rows)
                    p = lv.begin + 2 * (pairs * i + j)
                    between = every(lambda x, y: 0.5 * (x + y), a, b)
                    for q, add in ((p, a), (p + 1, between)):
                        keep = table_rows(table, valid(lv, q), lv, top, n)
                        put(dst, q, rows, every(lambda x, y: (x + y) * keep, get(dst, q, rows, lv), add))
                    a = b

    row_halo, halo = row_copies(), fine_copies()
    for copy in loads[:4]:
        copy.wait()
    half = TILE // 2
    upper = rows_of((TILE, LANES)) >= half

    batch = chip_y // 2
    many = rows_of((batch * TILE, LANES)) % TILE >= half

    @pl.loop(0, chip_y // batch)
    def _(i):
        planes = pl.ds(i * batch, batch)
        for side, row in enumerate((TILE, TILE + l0.nz - half)):
            f, u = (x.reshape(batch * TILE, LANES) for x in (stage_f[planes, pl.ds(row - half, TILE)], stage_u[planes, pl.ds(row, TILE)]))
            send_z[side, planes] = sort_x(jnp.where(many, f, u)).reshape(batch, TILE, LANES)
    begin(halo[4:])
    for copy in loads[4:]:
        copy.wait()
    step = 4

    for side, plane in enumerate((0, chip_y - l0.wide)):
        for j in range(l0.wide):
            edge_u[side, j] = sort_x(stage_u[plane + j, inner])
            edge_f[side, j] = sort_x(stage_f[plane + j, inner])
    begin(row_halo)

    def sort_planes(first, n):
        @pl.loop(0, n // step)
        def _(i):
            for j in range(step):
                y = first + i * step + j
                sorted_u[y] = sort_x(stage_u[y, inner])
                sorted_f[y] = sort_x(stage_f[y, inner])

    @pl.loop(0, PARTS)
    def _(part):
        sort_planes((1 - cx) * (chip_y - reach) + part * chunk, chunk)
        for copy in partner_copies(part):
            copy.start()
    begin(halo[:4])
    sort_planes(cx * reach, chip_y - reach)
    for offset in around_me:
        pl.semaphore_signal(ready, inc=1, device_id=peer(offset), device_id_type=MESH)

    some = reach // 3

    @pl.loop(0, PARTS)
    def _(part):
        for copy in partner_copies(part):
            copy.wait_recv()

        @pl.loop(0, chunk // step)
        def _(i):
            for j in range(step):
                k = part * chunk + i * step + j
                for src, buf, dst in ((sorted_u, part_u, u0), (sorted_f, part_f, f0)):
                    put(dst, l0.hx - cx * l0.wide + k, l0.own, split_x(src[cx * (chip_y - reach) + k], buf[k], cx))
    stages = ((u0, v0, cfg.stiffness), (v0, w0, None))
    for k, (src, dst, scale) in enumerate(stages):
        sweep(src, dst, f0, l0, mask0, scale, cut(l0, l0.z0 + k + 1, l0.nz - 2 * (k + 1)))
    arrive(row_halo)
    outer_plane = l0.hx - l0.wide + cx * reach

    for buf, dst in ((recv_yu, u0), (recv_yf, f0)):
        for j in range(l0.wide):
            put(dst, outer_plane + j, l0.own, split_x(buf[0, j], buf[1, j], 0))
    arrive(halo)
    finish(row_halo)
    finish(halo)
    for part in range(PARTS):
        for copy in partner_copies(part):
            copy.wait_send()

    def put_rows(p, side, buf, k):
        row = l0.z0 + l0.nz if side else l0.z0 - half
        for h, part in enumerate(split_x(buf[0, k], buf[1, k], 0)):
            pltpu.store(u0.at[p, h, pl.ds(row, TILE)], part, mask=jnp.logical_not(upper))
            pltpu.store(f0.at[p, h, pl.ds(row - half, TILE)], part, mask=upper)

    @pl.loop(0, reach // some)
    def _(i):
        for j in range(some):
            for side in range(2):
                put_rows(l0.hx - cx * l0.wide + i * some + j, side, recv_z.at[side], i * some + j)
    for side in range(2):
        for j in range(l0.wide):
            put_rows(outer_plane + j, side, recv_d.at[side], j)
    for k, (src, dst, scale) in enumerate(stages):
        ring = l0.wide + 1
        sweep(src, dst, f0, l0, mask0, scale, [(l0.top + k, ring), (l0.z0 + l0.nz - 1 - k, ring)], count=2, group=20)
        sweep(src, dst, f0, l0, mask0, scale, first=l0.begin + cx * l0.ny, count=1)
    restrict_level(w0, f0, l0, mask0, g1, l1, 4, 8)

    exchange(1)
    first_sweep(a1, g1, l1, mask1)
    sweep(a1, b1, g1, l1, mask1)
    restrict_level(b1, g1, l1, mask1, g2, l2, 8, 8)
    exchange(2)
    first_sweep(a2, g2, l2, mask2)
    sweep(a2, b2, g2, l2, mask2)

    restrict_planes(b2, g2, l2, mask2, 4)
    ny3, nz3, width = l2.ny // 2, l2.nz // 2, l2.nx // 2
    near = rows_of(square) - 2 * (lanes_of(square) % width)
    got = dot(stack([restricted_rows(j, l2) for j in range(ny3)]), weights(near, 2.0 * eighth, eighth))
    tile = (TILE, LANES)
    lane = lanes_of(tile)
    block = lane // width
    blocks = LANES // width
    packed = got[:nz3]
    for j in range(1, ny3):
        packed = jnp.where(block == j, got[j * nz3:(j + 1) * nz3], packed)
    packed = roll(packed, width * cy)
    message[...] = packed
    slot = yb * n_z + cz
    slots[slot] = packed

    def gather_copy(k, at):
        return pltpu.make_async_remote_copy(
            src_ref=message, dst_ref=slots.at[at], send_sem=all_s.at[k], recv_sem=all_r.at[at], device_id=peer(offsets[k]), device_id_type=MESH)

    pl.semaphore_wait(ready, len(around_me))
    for k in range(total - 1):
        gather_copy(k, slot).start()
    for k, offset in enumerate(offsets):
        who = peer(offset)
        gather_copy(k, (who['sy'] * n_x + who['sx']) * n_z + who['sz']).wait_recv()

    tall = nz3 * n_z
    data = pl.ds(TILE, tall)
    for which in range(2):
        for y in range(TILE):
            for at in (0, TILE + tall):
                s3[which, y, pl.ds(at, TILE)] = jnp.zeros(tile, F32)
    live = lane < width * n_y

    @pl.loop(0, n_x)
    def _(core):
        for j in range(ny3):
            for z in range(n_z):
                acc = jnp.zeros(tile, F32)
                for t in range(n_y):
                    acc = jnp.where((block + 2 * blocks - t - j) % blocks == 0, slots[(t * n_x + core) * n_z + z], acc)
                acc = jnp.where(live, roll(acc, back(width * j)), 0.0)
                rows = pl.ds(TILE + nz3 * z, nz3)
                g3[core * ny3 + j, rows] = acc
                s3[0, core * ny3 + j, rows] = acc * NINTH

    long = (tall, LANES)
    along = lanes_of(long)
    x_first, x_last = along % width == 0, along % width == width - 1
    y_first, y_last = along < width, along >= width * (n_y - 1)

    def coarse_sweep(k, carry):
        old, new = k % 2, (k + 1) % 2
        lowest, highest = s3[old, 0, data], s3[old, TILE - 1, data]
        c = lowest
        ym = jnp.where(y_first, 0.0, roll(highest, width % LANES))
        beyond = jnp.where(y_last, 0.0, roll(lowest, back(width)))
        for y in range(TILE):
            yp = s3[old, y + 1, data] if y < TILE - 1 else beyond
            around = (ym + yp) + (s3[old, y, pl.ds(TILE - 1, tall)] + s3[old, y, pl.ds(TILE + 1, tall)])
            left = jnp.where(x_first, 0.0, roll(c, 1))
            right = jnp.where(x_last, 0.0, roll(c, LANES - 1))
            s3[new, y, data] = (around + (left + right) + 3.0 * c + g3[y, data]) * NINTH
            ym, c = c, yp
        return carry
    lax.fori_loop(0, COARSE_SWEEPS - 1, coarse_sweep, 0)

    first = (l2.begin - l2.hx) // 2
    for i in range(e3.shape[0]):
        y = yb * ny3 + (i + first)
        c = s3[(COARSE_SWEEPS - 1) % 2, (y + TILE) % TILE, pl.ds(pl.multiple_of(cz * nz3, TILE), 3 * TILE)]
        ok = (lanes_of(c.shape) < width) & (y >= 0) & (y < row_blocks * ny3)
        e3[i, 0] = jnp.where(ok, roll(c, back((y + TILE) // TILE * width + LANES - width)), 0.0)

    prolong_planes(e3, 0, TILE, 0, 3 * TILE, width, 12, 1, l2)
    correct(b2, l2, mask2, 5)
    sweep(b2, a2, g2, l2, mask2)
    sweep(a2, b2, g2, l2, mask2)
    prolong_planes(b2, l2.hx + (l1.begin - l1.hx) // 2, l2.z0, l2.top, l2.rows, l2.nx, 16, 1, l1)
    correct(b1, l1, mask1, 7)
    sweep(b1, a1, g1, l1, mask1)
    sweep(a1, b1, g1, l1, mask1)
    prolong_planes(b1, l1.hx + (l0.begin - l0.hx) // 2, l1.z0, l1.top, l1.rows, l1.nx, 8, 3, l0)
    correct(w0, l0, mask0, 4)
    sweep(w0, v0, f0, l0, mask0)

    def results(i):
        here, there = pl.ds(i * step, step), pl.ds(cx * l0.ny + i * step, step)
        return pltpu.make_async_remote_copy(
            src_ref=stage_f.at[here, inner], dst_ref=out.at[there], send_sem=out_sem.at[0, i], recv_sem=out_sem.at[1, i],
            device_id={'sx': 1 - cx}, device_id_type=MESH)

    outer_lanes = ends(l0.nz)

    @pl.loop(0, l0.ny // step)
    def _(i):
        for j in range(step):
            k = i * step + j
            p = l0.hx + k
            c = get(v0, p, l0.own, l0)
            around = neighbours(v0, p, get(v0, p - 1, l0.own, l0), c, get(v0, p + 1, l0.own, l0), l0, l0.z0, l0.nz, outer_lanes)
            got = every(lambda x, y, g: (x + 3.0 * y + g) * (NINTH / cfg.stiffness), around, c, get(f0, p, l0.own, l0))
            out[cx * l0.ny + k], stage_f[k, inner] = merge_x(*got, cx)
        results(i).start()

    @pl.loop(0, l0.ny // step)
    def _(i):
        results(i).wait()
    drain(1)
    drain(2)

    for k in range(total - 1):
        gather_copy(k, slot).wait_send()


def write_out(held, out, rows, sem):
    batch = 2 * TILE

    def copy_out(i):
        planes = pl.ds(i * batch, batch)
        return pltpu.make_async_copy(rows.at[planes], out.at[planes], sem.at[i])

    @pl.loop(0, held.shape[0] // batch)
    def _(i):
        for j in range(batch):
            x = held[i * batch + j]
            lane = lanes_of(x.shape)
            rows[i * batch + j] = pick(x, lane // 2 + LANES // 2 * ((lane + lax.axis_index('sx')) % 2))
        copy_out(i).start()

    @pl.loop(0, held.shape[0] // batch)
    def _(i):
        copy_out(i).wait()


def local_cycle(rhs, start, counts, size):
    rhs, start = (jnp.transpose(x, (1, 2, 0)) for x in (rhs, start))
    n_x, n_y, n_z = counts
    chip_y, nz, nx = rhs.shape
    shapes = [(chip_y // n_x >> k, nz >> k, nx * n_x >> k) for k in range(3)]
    l0 = make_level(shapes[0], 6, 8, 4, nz + 8, 2, 8, (shapes[0][0] + 8) // 8, 4, nz + 8)
    l1 = make_level(shapes[1], 8, 16, 8, shapes[1][1] + 16, 2, 14, (shapes[1][0] + 12) // 14, 5, 48)
    l2 = make_level(shapes[2], 8, 16, 8, shapes[2][1] + 16, 2, 20, (shapes[2][0] + 12) // 20, 6, 32)
    cfg = types.SimpleNamespace(levels=(l0, l1, l2), counts=counts, stiffness=float((size + 1) ** 2))
    total = n_x * n_y * n_z

    def vmem(*shape):
        return pltpu.VMEM(shape, F32)

    scratch = [vmem(lv.planes, lv.parts, lv.depth, LANES) for lv, n in ((l0, 4), (l1, 3), (l2, 3)) for _ in range(n)]
    reach = l0.ny + l0.wide
    scratch += [vmem(12, 1, 3 * TILE, LANES), vmem(l1.ny + 8, l1.rows, LANES), vmem(2, l1.ny + 8, l0.depth, LANES)]
    scratch += [vmem(chip_y, l0.depth, LANES)] * 2 + [vmem(reach, nz, LANES)] * 2 + [vmem(chip_y, nz, LANES)] * 2
    scratch += [vmem(2, l0.wide, nz, LANES)] * 2
    scratch += [vmem(2, TILE, l2.nz // 2 * n_z + 2 * TILE, LANES), vmem(TILE, l2.nz // 2 * n_z + 2 * TILE, LANES), vmem(total, TILE, LANES), vmem(TILE, LANES)]
    scratch += [vmem(3, lv.rows, LANES) for lv in (l0, l1, l2)]
    scratch += [vmem(2, chip_y, TILE, LANES), vmem(2, n_x, reach, TILE, LANES), vmem(2, 2, l0.wide, TILE, LANES)]
    scratch += [vmem(2, l0.wide, nz, LANES)] * 2
    sems = [(10,), (2, l0.ny // 4), (16,), (16,), (2, len(SIDES)), (2, len(SIDES)), (total,), (total,), (PARTS, 2), (PARTS, 2)]
    scratch += [pltpu.SemaphoreType.DMA(shape) for shape in sems] + [pltpu.SemaphoreType.REGULAR]
    got = pl.pallas_call(
        functools.partial(kernel, cfg),
        out_shape=pltpu.VMEM(rhs.shape, F32),
        in_specs=[pl.BlockSpec(memory_space=pl.ANY)] * 2,
        out_specs=pl.BlockSpec(memory_space=pltpu.VMEM),
        scratch_shapes=scratch,
        compiler_params=pltpu.CompilerParams(collective_id=0, has_side_effects=True, vmem_limit_bytes=60 * 2 ** 20),
    )(rhs, start)
    got = pl.pallas_call(
        write_out,
        out_shape=jax.ShapeDtypeStruct(rhs.shape, F32),
        in_specs=[pl.BlockSpec(memory_space=pltpu.VMEM)],
        out_specs=pl.BlockSpec(memory_space=pl.ANY),
        scratch_shapes=[vmem(*rhs.shape), pltpu.SemaphoreType.DMA((chip_y // TILE,))],
    )(pltpu.with_memory_space_constraint(got, pltpu.VMEM))
    return jnp.transpose(got, (2, 0, 1))


def solution(mesh):
    counts = (mesh.shape['sx'], mesh.shape['sy'], mesh.shape['sz'])
    spec = P(('dp', 'sx'), 'sy', 'sz')

    def run(rhs_grid, u_start):
        size = rhs_grid.shape[0] // mesh.shape['dp']
        cycle = functools.partial(local_cycle, counts=counts, size=size)
        return jax.shard_map(cycle, mesh=mesh, in_specs=(spec, spec), out_specs=spec, check_vma=False)(rhs_grid, u_start)
    return run
```

```python
import functools
import types
import jax
import jax.numpy as jnp
from jax import lax
from jax.experimental import pallas as pl
from jax.experimental.pallas import tpu as pltpu
from jax.sharding import PartitionSpec as P

F32 = jnp.float32
MESH = pl.DeviceIdType.MESH
LANES = 128
TILE = 8
NINTH = 1.0 / 9.0
COARSE_SWEEPS = 16
PARTS = 3
OPPOSITE = (1, 0, 3, 2, 7, 6, 5, 4)
STEP_Y = (-1, 1, 0, 0, -1, -1, 1, 1)
STEP_Z = (0, 0, -1, 1, -1, 1, -1, 1)
SIDES = range(len(STEP_Y))


def make_level(shape, hx, z0, top, rows, begin, group, count, wide, block):
    ny, nz, nx = shape
    lv = types.SimpleNamespace(ny=ny, nz=nz, nx=nx, hx=hx, z0=z0, top=top, rows=rows, begin=begin, group=group, count=count, wide=wide)
    lv.planes = ny + 2 * hx
    lv.depth = nz + 2 * z0
    lv.parts = max(nx // LANES, 1)
    lv.own = pl.ds(z0, nz)
    lv.all = pl.ds(top, rows)
    lv.block = block
    lv.blocks = cut(lv, top, rows)
    return lv


def cut(lv, top, rows):
    return [(top + i, min(lv.block, rows - i)) for i in range(0, rows, lv.block)]


def lanes_of(shape):
    return lax.broadcasted_iota(jnp.int32, shape, len(shape) - 1)


def rows_of(shape):
    return lax.broadcasted_iota(jnp.int32, shape, len(shape) - 2)


def roll(x, shift):
    return pltpu.roll(x, shift, 1)


def ends(n):
    lane = lanes_of((n, LANES))
    return lane == 0, lane == LANES - 1, jnp.zeros((n, LANES), F32)


def from_below(x, outer):
    return lax.select(outer[0], outer[2], roll(x, 1))


def from_above(x, outer):
    return lax.select(outer[1], outer[2], roll(x, LANES - 1))


def halves(x):
    return x[:, :LANES], x[:, LANES:]


def get(ref, p, rows, lv):
    return [ref[p, h, rows] for h in range(lv.parts)]


def put(ref, p, rows, values):
    for h, value in enumerate(values):
        ref[p, h, rows] = value


def every(f, *lists):
    return [f(*values) for values in zip(*lists)]


def join(*parts):
    return jnp.concatenate(parts, axis=1)


def stack(parts):
    return jnp.concatenate(parts, axis=0)


def back(shift):
    return (4 * LANES - shift) % LANES


def flag(condition):
    return jnp.where(condition, 1, 0)


def pick(x, index):
    return jnp.take_along_axis(x, index, axis=1, mode='promise_in_bounds')


def dot(x, w):
    return jnp.dot(x, w, precision=lax.Precision.HIGHEST, preferred_element_type=F32)


def kernel(cfg, rhs, start, out, *scratch):
    (u0, v0, f0, w0, a1, b1, g1, a2, b2, g2, e3, pz, pb, stage_u, stage_f, part_u, part_f, sorted_u, sorted_f, edge_u, edge_f, s3, g3, slots, message, mask0, mask1, mask2,
     send_z, recv_z, recv_d, recv_yu, recv_yf,
     load_sem, out_sem, fine_s, fine_r, send_sem, recv_sem, all_s, all_r, part_s, part_r, ready) = scratch
    l0, l1, l2 = levels = cfg.levels
    masks = (mask0, mask1, mask2)
    n_x, n_y, n_z = cfg.counts
    cx, cy, cz = lax.axis_index('sx'), lax.axis_index('sy'), lax.axis_index('sz')
    total = n_x * n_y * n_z
    row_blocks = n_x * n_y
    yb = cy * n_x + cx

    inner = pl.ds(TILE, l0.nz)
    chip_y = n_x * l0.ny

    def load(planes, rows):
        shifted = pl.ds(rows.start + TILE, rows.size)
        k = len(loads)
        loads.append(pltpu.make_async_copy(start.at[planes, rows], stage_u.at[planes, shifted], load_sem.at[k]))
        loads.append(pltpu.make_async_copy(rhs.at[planes, rows], stage_f.at[planes, shifted], load_sem.at[k + 1]))
    loads = []
    between = pl.ds(TILE, l0.nz - 2 * TILE)
    for row in (0, l0.nz - TILE):
        load(pl.ds(0, chip_y), pl.ds(row, TILE))
    for plane in (0, chip_y - l0.wide):
        load(pl.ds(plane, l0.wide), between)
    load(pl.ds(l0.wide, chip_y - 2 * l0.wide), between)
    for copy in loads:
        copy.start()

    offsets = [(dz, dy, dx) for dz in range(n_z) for dy in range(n_y) for dx in range(n_x)][1:]
    offsets.sort(key=lambda o: -2 * (min(o[0], n_z - o[0]) + min(o[1], n_y - o[1])) - o[2])

    def peer(offset):
        return {name: lax.rem(at + d, n) for name, at, n, d in zip(('sz', 'sy', 'sx'), (cz, cy, cx), (n_z, n_y, n_x), offset)}

    def inside(step, at, count):
        if step == 0:
            return True
        return at > 0 if step < 0 else at < count - 1

    around_me = [o for o in offsets if o[0] in (0, 1, n_z - 1) and o[1] in (0, 1, n_y - 1)]
    barrier = pltpu.get_barrier_semaphore()
    for offset in around_me:
        pl.semaphore_signal(barrier, inc=1, device_id=peer(offset), device_id_type=MESH)
    outer = 2 * cx - 1
    has_outer = (cy + outer >= 0) & (cy + outer < n_y)

    def exists(d):
        return jnp.logical_and(inside(STEP_Y[d], yb, row_blocks), inside(STEP_Z[d], cz, n_z))

    def zero(ref):
        @pl.loop(0, ref.shape[0])
        def _(i):
            ref[i] = jnp.zeros(ref.shape[1:], F32)

    def span(step, first, n, wide, own):
        if step == 0:
            return pl.ds(first, n)
        if step < 0:
            return pl.ds(first if own else first - wide, wide)
        return pl.ds(first + n - wide if own else first + n, wide)

    def region(index, d, own):
        lv, arr = levels[index], (None, g1, g2)[index]
        return arr.at[span(STEP_Y[d], lv.hx, lv.ny, lv.wide, own), 0, span(STEP_Z[d], lv.z0, lv.nz, TILE, own)]

    def halo_copy(index, d, arriving):
        k = index - 1
        at = yb + STEP_Y[d]
        return pltpu.make_async_remote_copy(
            src_ref=region(index, d, not arriving), dst_ref=region(index, d if arriving else OPPOSITE[d], False),
            send_sem=send_sem.at[k, d], recv_sem=recv_sem.at[k, d if arriving else OPPOSITE[d]],
            device_id={'sx': at % n_x, 'sy': at // n_x, 'sz': cz + STEP_Z[d]}, device_id_type=MESH)

    def each(act):
        for d in (2, 3, 4, 5, 6, 7, 0, 1):
            @pl.when(exists(d))
            def _(d=d):
                act(d)

    def exchange(index):
        each(lambda d: halo_copy(index, d, False).start())
        each(lambda d: halo_copy(index, d, True).wait_recv())

    def drain(index):
        each(lambda d: halo_copy(index, d, False).wait_send())

    reach = l0.ny + l0.wide

    def fine_copies():
        got = []

        def add(sends, arrives, src, dst, arrival, k, theirs, **to):
            made = [pltpu.make_async_remote_copy(
                src_ref=a, dst_ref=b, send_sem=fine_s.at[k], recv_sem=fine_r.at[r], device_id=to, device_id_type=MESH)
                for a, b, r in ((src, dst, theirs[0]), (arrival, arrival, theirs[1]))]
            got.append((sends, arrives, *made))
        n = 0
        for z_side, z_step in enumerate((-1, 1)):
            for y_side, y_step in enumerate((-1, 1)):
                edge = pl.ds(0 if y_step < 0 else chip_y - l0.wide, l0.wide)
                to_z = jnp.logical_and(inside(y_step, cy, n_y), inside(z_step, cz, n_z))
                in_z = jnp.logical_and(has_outer, inside(z_step, cz, n_z))
                add(to_z, in_z, send_z.at[z_side, edge], recv_d.at[1 - z_side, cx], recv_d.at[z_side, y_side], n,
                    (8 + 2 * (1 - z_side) + cx, 8 + 2 * z_side + y_side), sx=1 - y_side, sy=cy + y_step, sz=cz + z_step)
                n += 1
        for z_side, z_step in enumerate((-1, 1)):
            for core in range(n_x):
                there = inside(z_step, cz, n_z)
                add(there, there, send_z.at[z_side, pl.ds(core * (chip_y - reach), reach)], recv_z.at[1 - z_side, cx],
                    recv_z.at[z_side, core], n, (12 + 2 * (1 - z_side) + cx, 12 + 2 * z_side + core), sx=core, sz=cz + z_step)
                n += 1
        return got

    def row_copies():
        got = []
        for y_side, y_step in enumerate((-1, 1)):
            for k, (edges, buf) in enumerate(((edge_u, recv_yu), (edge_f, recv_yf))):
                made = [pltpu.make_async_remote_copy(
                    src_ref=a, dst_ref=b, send_sem=fine_s.at[8 + 2 * y_side + k], recv_sem=fine_r.at[2 * r + k],
                    device_id={'sx': 1 - y_side, 'sy': cy + y_step}, device_id_type=MESH)
                    for a, b, r in ((edges.at[y_side], buf.at[cx], cx), (buf.at[y_side], buf.at[y_side], y_side))]
                got.append((inside(y_step, cy, n_y), has_outer, *made))
        return got

    chunk = reach // PARTS

    def partner_copies(part):
        other = pl.ds((1 - cx) * (chip_y - reach) + part * chunk, chunk)
        return [pltpu.make_async_remote_copy(
            src_ref=src.at[other], dst_ref=buf.at[pl.ds(part * chunk, chunk)], send_sem=part_s.at[part, k],
            recv_sem=part_r.at[part, k], device_id={'sx': 1 - cx}, device_id_type=MESH)
            for k, (src, buf) in enumerate(((sorted_u, part_u), (sorted_f, part_f)))]

    def begin(copies):
        for sends, _, copy, _ in copies:
            @pl.when(sends)
            def _(copy=copy):
                copy.start()

    def arrive(copies):
        for _, arrives, _, copy in copies:
            @pl.when(arrives)
            def _(copy=copy):
                copy.wait_recv()

    def finish(copies):
        for sends, _, copy, _ in copies:
            @pl.when(sends)
            def _(copy=copy):
                copy.wait_send()

    @pl.when(jnp.logical_not(has_outer))
    def _():
        for buf in (recv_yu, recv_yf, recv_d):
            for k in range(2):
                zero(buf.at[k])
    for z_side, z_step in enumerate((-1, 1)):
        @pl.when(jnp.logical_not(inside(z_step, cz, n_z)))
        def _(z_side=z_side):
            for core in range(n_x):
                zero(recv_z.at[z_side, core])
            zero(recv_d.at[z_side])
    for index in (1, 2):
        for d in SIDES:
            @pl.when(jnp.logical_not(exists(d)))
            def _(index=index, d=d):
                zero(region(index, d, False))

    for lv, arrays in ((l0, (u0, v0, w0)), (l1, (a1, b1)), (l2, (a2, b2))):
        for arr in arrays:
            for plane, outside in ((lv.hx - 1, yb == 0), (lv.hx + lv.ny, yb == row_blocks - 1)):
                @pl.when(outside)
                def _(arr=arr, lv=lv, plane=plane):
                    put(arr, plane, lv.all, [jnp.zeros((lv.rows, LANES), F32)] * lv.parts)

    for lv, table in zip(levels, masks):
        shape = (lv.rows, LANES)
        z = rows_of(shape) + (lv.top - lv.z0) + cz * lv.nz
        ok = (z >= 0) & (z < n_z * lv.nz) & (lanes_of(shape) < lv.nx)
        table[0] = jnp.zeros(shape, F32)
        table[1] = jnp.where(ok, 1.0, 0.0).astype(F32)
        table[2] = jnp.where(ok, NINTH, 0.0).astype(F32)

    def valid(lv, p):
        y = p + (yb * lv.ny - lv.hx)
        return flag((y >= 0) & (y < row_blocks * lv.ny))

    middle = LANES // 2

    def sort_x(x):
        lane = lanes_of(x.shape)
        return pick(x, 2 * (lane % middle) + (lane // middle + cx) % 2)

    def split_x(first, second, core):
        here = lanes_of(first.shape) // middle == core
        return [jnp.where(here, first, second), roll(jnp.where(here, second, first), middle)]

    def merge_x(even, odd, core):
        here = lanes_of(even.shape) // middle == core
        odd = roll(odd, middle)
        return jnp.where(here, even, odd), jnp.where(here, odd, even)

    pl.semaphore_wait(barrier, len(around_me))

    def across(c, lv, outer):
        if lv.parts > 1:
            even, odd = c
            return [odd + from_below(odd, outer), even + from_above(even, outer)]
        if lv.nx == LANES:
            return [from_below(c[0], outer) + from_above(c[0], outer)]
        return [roll(c[0], 1) + roll(c[0], LANES - 1)]

    def neighbours(src, p, xm, c, xp, lv, top, n, outer):
        zm, zp = get(src, p, pl.ds(top - 1, n), lv), get(src, p, pl.ds(top + 1, n), lv)
        return every(lambda a, b, d, e, f: ((a + b) + (d + e)) + f, xm, xp, zm, zp, across(c, lv, outer))

    def table_rows(table, k, lv, top, n):
        return table[k, pl.ds(top - lv.top, n)]

    def sweep(src, dst, rhs_ref, lv, table, scale=None, blocks=None, first=None, count=None, group=None):
        group, blocks = group or lv.group, blocks or lv.blocks
        outers = {n: ends(n) for _, n in blocks}

        @pl.loop(0, count or lv.count)
        def _(g):
            base = (lv.begin if first is None else first) + g * group
            for top, n in blocks:
                rows = pl.ds(top, n)
                xm, c = get(src, base - 1, rows, lv), get(src, base, rows, lv)
                for j in range(group):
                    p = base + j
                    xp = get(src, p + 1, rows, lv)
                    t = every(lambda a, b: a + 3.0 * b, neighbours(src, p, xm, c, xp, lv, top, n, outers[n]), c)
                    if scale is not None:
                        t = [x * scale for x in t]
                    keep = table_rows(table, 2 * valid(lv, p), lv, top, n)
                    put(dst, p, rows, every(lambda a, b: (a + b) * keep, t, get(rhs_ref, p, rows, lv)))
                    xm, c = c, xp

    def first_sweep(dst, rhs_ref, lv, table):
        @pl.loop(0, lv.count)
        def _(g):
            for j in range(lv.group):
                p = lv.begin + g * lv.group + j
                dst[p, 0, lv.all] = rhs_ref[p, 0, lv.all] * table[2 * valid(lv, p)]

    def restrict_planes(src, rhs_ref, lv, table, group):
        outers = {n: ends(n) for _, n in lv.blocks}

        def res(p, xm, c, xp, top, n):
            return every(lambda a, b, d: a + b - 6.0 * d, neighbours(src, p, xm, c, xp, lv, top, n, outers[n]), get(rhs_ref, p, pl.ds(top, n), lv), c)

        @pl.loop(0, lv.ny // 2 // group)
        def _(i):
            for top, n in lv.blocks:
                rows = pl.ds(top, n)
                p = lv.hx + 2 * group * i
                xm, c = get(src, p - 1, rows, lv), get(src, p, rows, lv)
                prev = res(p - 1, get(src, p - 2, rows, lv), xm, c, top, n)
                prev = [jnp.where((yb > 0) | (i > 0), x, 0.0) for x in prev]
                keep = table_rows(table, 1, lv, top, n)
                for j in range(group):
                    x1, x2 = get(src, p + 1, rows, lv), get(src, p + 2, rows, lv)
                    even = res(p, xm, c, x1, top, n)
                    odd = res(p + 1, c, x1, x2, top, n)
                    for h in range(lv.parts):
                        pb[h, i * group + j, rows] = ((prev[h] + odd[h]) + (even[h] + even[h])) * keep
                    prev, xm, c, p = odd, x1, x2, p + 2

    def restricted_rows(i, lv, h=0):
        half = lv.nz // 2
        return ((pb[h, i, pl.ds(lv.z0 - 1, half, stride=2)] + pb[h, i, pl.ds(lv.z0 + 1, half, stride=2)])
                + 2.0 * pb[h, i, pl.ds(lv.z0, half, stride=2)])

    def weights(near, one, other):
        return jnp.where(near == 0, one, jnp.where((near == 1) | (near == -1), other, 0.0)).astype(F32)

    square = (LANES, LANES)
    eighth = 1.0 / (TILE * TILE)

    def restrict_level(src, rhs_ref, lv, table, coarse_rhs, coarse, group, step):
        restrict_planes(src, rhs_ref, lv, table, group)
        lane = lanes_of(square)
        outer = ends(coarse.nz)
        w = jnp.where(lane < coarse.nx, weights(rows_of(square) - 2 * lane, 2.0 * eighth, eighth), 0.0)

        @pl.loop(0, coarse.ny // step)
        def _(i):
            got = [restricted_rows(i * step + j, lv) for j in range(step)]
            if lv.parts > 1:
                odds = [restricted_rows(i * step + j, lv, 1) for j in range(step)]
                got = [((odd + from_below(odd, outer)) + 2.0 * even) * eighth for even, odd in zip(got, odds)]
            else:
                got = dot(stack(got), w)
                got = [got[j * coarse.nz:(j + 1) * coarse.nz] for j in range(step)]
            for j in range(step):
                coarse_rhs[coarse.hx + i * step + j, 0, coarse.own] = got[j]

    def prolong_planes(e, first, e_z0, e_top, e_rows, e_nx, chunk, n_chunks, lv):
        lane, below = lanes_of(square), rows_of(square)
        w = jnp.where(below < e_nx, weights(lane - 2 * below, 4.0, 2.0), 0.0)
        row = e_z0 - e_top - (lv.z0 - lv.top) // 2
        n = lv.rows // 2

        @pl.loop(0, n_chunks)
        def _(i):
            planes = pl.ds(first + i * chunk, chunk)
            got = e[planes, 0, pl.ds(e_top, e_rows)]
            if lv.parts == 1:
                got = dot(got.reshape(chunk * e_rows, LANES), w).reshape(chunk, e_rows, LANES)
            else:
                got = got * 4.0
            pz[pl.ds(i * chunk, chunk), pl.ds(0, e_rows)] = got

        @pl.loop(0, n_chunks)
        def _(i):
            for j in range(chunk):
                a = pz[i * chunk + j, pl.ds(row, n)]
                b = pz[i * chunk + j, pl.ds(row + 1, n)]
                pb[0, i * chunk + j, pl.ds(lv.top, n, stride=2)] = a
                pb[0, i * chunk + j, pl.ds(lv.top + 1, n, stride=2)] = 0.5 * (a + b)

    def correct(dst, lv, table, pairs):
        def load(at, rows):
            a = pb[0, at, rows]
            return [a, 0.5 * (a + from_above(a, outers[a.shape[0]]))] if lv.parts > 1 else [a]
        outers = {n: ends(n) for _, n in lv.blocks}

        @pl.loop(0, lv.group * lv.count // (2 * pairs))
        def _(i):
            for top, n in lv.blocks:
                rows = pl.ds(top, n)
                a = load(i * pairs, rows)
                for j in range(pairs):
                    b = load(i * pairs + j + 1, rows)
                    p = lv.begin + 2 * (pairs * i + j)
                    between = every(lambda x, y: 0.5 * (x + y), a, b)
                    for q, add in ((p, a), (p + 1, between)):
                        keep = table_rows(table, valid(lv, q), lv, top, n)
                        put(dst, q, rows, every(lambda x, y: (x + y) * keep, get(dst, q, rows, lv), add))
                    a = b

    row_halo, halo = row_copies(), fine_copies()
    for copy in loads[:4]:
        copy.wait()
    half = TILE // 2
    upper = rows_of((TILE, LANES)) >= half

    batch = chip_y // 2
    many = rows_of((batch * TILE, LANES)) % TILE >= half

    @pl.loop(0, chip_y // batch)
    def _(i):
        planes = pl.ds(i * batch, batch)
        for side, row in enumerate((TILE, TILE + l0.nz - half)):
            f, u = (x.reshape(batch * TILE, LANES) for x in (stage_f[planes, pl.ds(row - half, TILE)], stage_u[planes, pl.ds(row, TILE)]))
            send_z[side, planes] = sort_x(jnp.where(many, f, u)).reshape(batch, TILE, LANES)
    begin(halo[4:])
    for copy in loads[4:]:
        copy.wait()
    step = 4

    def sort_planes_of(stage, first, n):
        return sort_x(stage[pl.ds(first, n), inner].reshape(n * l0.nz, LANES)).reshape(n, l0.nz, LANES)

    for side, plane in enumerate((0, chip_y - l0.wide)):
        for stage, edges in ((stage_u, edge_u), (stage_f, edge_f)):
            edges[side] = sort_planes_of(stage, plane, l0.wide)
    begin(row_halo)

    def sort_planes(first, n):
        @pl.loop(0, n // step)
        def _(i):
            y = first + i * step
            sorted_u[pl.ds(y, step)] = sort_planes_of(stage_u, y, step)
            sorted_f[pl.ds(y, step)] = sort_planes_of(stage_f, y, step)

    @pl.loop(0, PARTS)
    def _(part):
        sort_planes((1 - cx) * (chip_y - reach) + part * chunk, chunk)
        for copy in partner_copies(part):
            copy.start()
    begin(halo[:4])
    sort_planes(cx * reach, chip_y - reach)
    for offset in around_me:
        pl.semaphore_signal(ready, inc=1, device_id=peer(offset), device_id_type=MESH)

    some = reach // 3

    @pl.loop(0, PARTS)
    def _(part):
        for copy in partner_copies(part):
            copy.wait_recv()

        @pl.loop(0, chunk // step)
        def _(i):
            for j in range(step):
                k = part * chunk + i * step + j
                for src, buf, dst in ((sorted_u, part_u, u0), (sorted_f, part_f, f0)):
                    put(dst, l0.hx - cx * l0.wide + k, l0.own, split_x(src[cx * (chip_y - reach) + k], buf[k], cx))
    stages = ((u0, v0, cfg.stiffness), (v0, w0, None))
    for k, (src, dst, scale) in enumerate(stages):
        sweep(src, dst, f0, l0, mask0, scale, cut(l0, l0.z0 + k + 1, l0.nz - 2 * (k + 1)))
    arrive(row_halo)
    outer_plane = l0.hx - l0.wide + cx * reach

    for buf, dst in ((recv_yu, u0), (recv_yf, f0)):
        for j in range(l0.wide):
            put(dst, outer_plane + j, l0.own, split_x(buf[0, j], buf[1, j], 0))
    arrive(halo)
    finish(row_halo)
    finish(halo)
    for part in range(PARTS):
        for copy in partner_copies(part):
            copy.wait_send()

    def put_rows(p, side, buf, k):
        row = l0.z0 + l0.nz if side else l0.z0 - half
        for h, part in enumerate(split_x(buf[0, k], buf[1, k], 0)):
            pltpu.store(u0.at[p, h, pl.ds(row, TILE)], part, mask=jnp.logical_not(upper))
            pltpu.store(f0.at[p, h, pl.ds(row - half, TILE)], part, mask=upper)

    @pl.loop(0, reach // some)
    def _(i):
        for j in range(some):
            for side in range(2):
                put_rows(l0.hx - cx * l0.wide + i * some + j, side, recv_z.at[side], i * some + j)
    for side in range(2):
        for j in range(l0.wide):
            put_rows(outer_plane + j, side, recv_d.at[side], j)
    for k, (src, dst, scale) in enumerate(stages):
        ring = l0.wide + 1
        sweep(src, dst, f0, l0, mask0, scale, [(l0.top + k, ring), (l0.z0 + l0.nz - 1 - k, ring)], count=2, group=20)
        sweep(src, dst, f0, l0, mask0, scale, first=l0.begin + cx * l0.ny, count=1)
    restrict_level(w0, f0, l0, mask0, g1, l1, 8, 8)

    exchange(1)
    first_sweep(a1, g1, l1, mask1)
    sweep(a1, b1, g1, l1, mask1)
    restrict_level(b1, g1, l1, mask1, g2, l2, 8, 8)
    exchange(2)
    first_sweep(a2, g2, l2, mask2)
    sweep(a2, b2, g2, l2, mask2)

    restrict_planes(b2, g2, l2, mask2, 4)
    ny3, nz3, width = l2.ny // 2, l2.nz // 2, l2.nx // 2
    near = rows_of(square) - 2 * (lanes_of(square) % width)
    got = dot(stack([restricted_rows(j, l2) for j in range(ny3)]), weights(near, 2.0 * eighth, eighth))
    tile = (TILE, LANES)
    lane = lanes_of(tile)
    block = lane // width
    blocks = LANES // width
    packed = got[:nz3]
    for j in range(1, ny3):
        packed = jnp.where(block == j, got[j * nz3:(j + 1) * nz3], packed)
    packed = roll(packed, width * cy)
    message[...] = packed
    slot = yb * n_z + cz
    slots[slot] = packed

    def gather_copy(k, at):
        return pltpu.make_async_remote_copy(
            src_ref=message, dst_ref=slots.at[at], send_sem=all_s.at[k], recv_sem=all_r.at[at], device_id=peer(offsets[k]), device_id_type=MESH)

    pl.semaphore_wait(ready, len(around_me))
    for k in range(total - 1):
        gather_copy(k, slot).start()
    for k, offset in enumerate(offsets):
        who = peer(offset)
        gather_copy(k, (who['sy'] * n_x + who['sx']) * n_z + who['sz']).wait_recv()

    tall = nz3 * n_z
    data = pl.ds(TILE, tall)
    for which in range(2):
        for y in range(TILE):
            for at in (0, TILE + tall):
                s3[which, y, pl.ds(at, TILE)] = jnp.zeros(tile, F32)
    live = lane < width * n_y

    @pl.loop(0, n_x)
    def _(core):
        for j in range(ny3):
            for z in range(n_z):
                acc = jnp.zeros(tile, F32)
                for t in range(n_y):
                    acc = jnp.where((block + 2 * blocks - t - j) % blocks == 0, slots[(t * n_x + core) * n_z + z], acc)
                acc = jnp.where(live, roll(acc, back(width * j)), 0.0)
                rows = pl.ds(TILE + nz3 * z, nz3)
                g3[core * ny3 + j, rows] = acc
                s3[0, core * ny3 + j, rows] = acc * NINTH

    long = (tall, LANES)
    along = lanes_of(long)
    x_first, x_last = along % width == 0, along % width == width - 1
    y_first, y_last = along < width, along >= width * (n_y - 1)

    def coarse_sweep(k, carry):
        old, new = k % 2, (k + 1) % 2
        lowest, highest = s3[old, 0, data], s3[old, TILE - 1, data]
        c = lowest
        ym = jnp.where(y_first, 0.0, roll(highest, width % LANES))
        beyond = jnp.where(y_last, 0.0, roll(lowest, back(width)))
        for y in range(TILE):
            yp = s3[old, y + 1, data] if y < TILE - 1 else beyond
            around = (ym + yp) + (s3[old, y, pl.ds(TILE - 1, tall)] + s3[old, y, pl.ds(TILE + 1, tall)])
            left = jnp.where(x_first, 0.0, roll(c, 1))
            right = jnp.where(x_last, 0.0, roll(c, LANES - 1))
            s3[new, y, data] = (around + (left + right) + 3.0 * c + g3[y, data]) * NINTH
            ym, c = c, yp
        return carry
    lax.fori_loop(0, COARSE_SWEEPS - 1, coarse_sweep, 0)

    first = (l2.begin - l2.hx) // 2
    for i in range(e3.shape[0]):
        y = yb * ny3 + (i + first)
        c = s3[(COARSE_SWEEPS - 1) % 2, (y + TILE) % TILE, pl.ds(pl.multiple_of(cz * nz3, TILE), 3 * TILE)]
        ok = (lanes_of(c.shape) < width) & (y >= 0) & (y < row_blocks * ny3)
        e3[i, 0] = jnp.where(ok, roll(c, back((y + TILE) // TILE * width + LANES - width)), 0.0)

    prolong_planes(e3, 0, TILE, 0, 3 * TILE, width, 12, 1, l2)
    correct(b2, l2, mask2, 5)
    sweep(b2, a2, g2, l2, mask2)
    sweep(a2, b2, g2, l2, mask2)
    prolong_planes(b2, l2.hx + (l1.begin - l1.hx) // 2, l2.z0, l2.top, l2.rows, l2.nx, 16, 1, l1)
    correct(b1, l1, mask1, 7)
    sweep(b1, a1, g1, l1, mask1)
    sweep(a1, b1, g1, l1, mask1)
    prolong_planes(b1, l1.hx + (l0.begin - l0.hx) // 2, l1.z0, l1.top, l1.rows, l1.nx, 8, 3, l0)
    correct(w0, l0, mask0, 4)
    sweep(w0, v0, f0, l0, mask0)

    def results(i):
        here, there = pl.ds(i * step, step), pl.ds(cx * l0.ny + i * step, step)
        return pltpu.make_async_remote_copy(
            src_ref=stage_f.at[here, inner], dst_ref=out.at[there], send_sem=out_sem.at[0, i], recv_sem=out_sem.at[1, i],
            device_id={'sx': 1 - cx}, device_id_type=MESH)

    outer_lanes = ends(l0.nz)

    @pl.loop(0, l0.ny // step)
    def _(i):
        for j in range(step):
            k = i * step + j
            p = l0.hx + k
            c = get(v0, p, l0.own, l0)
            around = neighbours(v0, p, get(v0, p - 1, l0.own, l0), c, get(v0, p + 1, l0.own, l0), l0, l0.z0, l0.nz, outer_lanes)
            got = every(lambda x, y, g: (x + 3.0 * y + g) * (NINTH / cfg.stiffness), around, c, get(f0, p, l0.own, l0))
            out[cx * l0.ny + k], stage_f[k, inner] = merge_x(*got, cx)
        results(i).start()

    @pl.loop(0, l0.ny // step)
    def _(i):
        results(i).wait()
    drain(1)
    drain(2)

    for k in range(total - 1):
        gather_copy(k, slot).wait_send()


def write_out(held, out, rows, sem):
    batch = 2 * TILE

    def copy_out(i):
        planes = pl.ds(i * batch, batch)
        return pltpu.make_async_copy(rows.at[planes], out.at[planes], sem.at[i])

    @pl.loop(0, held.shape[0] // batch)
    def _(i):
        for j in range(batch):
            x = held[i * batch + j]
            lane = lanes_of(x.shape)
            rows[i * batch + j] = pick(x, lane // 2 + LANES // 2 * ((lane + lax.axis_index('sx')) % 2))
        copy_out(i).start()

    @pl.loop(0, held.shape[0] // batch)
    def _(i):
        copy_out(i).wait()


def local_cycle(rhs, start, counts, size):
    rhs, start = (jnp.transpose(x, (1, 2, 0)) for x in (rhs, start))
    n_x, n_y, n_z = counts
    chip_y, nz, nx = rhs.shape
    shapes = [(chip_y // n_x >> k, nz >> k, nx * n_x >> k) for k in range(3)]
    l0 = make_level(shapes[0], 6, 8, 4, nz + 8, 2, 8, (shapes[0][0] + 8) // 8, 4, nz + 8)
    l1 = make_level(shapes[1], 8, 16, 8, shapes[1][1] + 16, 2, 28, (shapes[1][0] + 12) // 28, 5, 48)
    l2 = make_level(shapes[2], 8, 16, 8, shapes[2][1] + 16, 2, 20, (shapes[2][0] + 12) // 20, 6, 32)
    cfg = types.SimpleNamespace(levels=(l0, l1, l2), counts=counts, stiffness=float((size + 1) ** 2))
    total = n_x * n_y * n_z

    def vmem(*shape):
        return pltpu.VMEM(shape, F32)

    scratch = [vmem(lv.planes, lv.parts, lv.depth, LANES) for lv, n in ((l0, 4), (l1, 3), (l2, 3)) for _ in range(n)]
    reach = l0.ny + l0.wide
    scratch += [vmem(12, 1, 3 * TILE, LANES), vmem(l1.ny + 8, l1.rows, LANES), vmem(2, l1.ny + 8, l0.depth, LANES)]
    scratch += [vmem(chip_y, l0.depth, LANES)] * 2 + [vmem(reach, nz, LANES)] * 2 + [vmem(chip_y, nz, LANES)] * 2
    scratch += [vmem(2, l0.wide, nz, LANES)] * 2
    scratch += [vmem(2, TILE, l2.nz // 2 * n_z + 2 * TILE, LANES), vmem(TILE, l2.nz // 2 * n_z + 2 * TILE, LANES), vmem(total, TILE, LANES), vmem(TILE, LANES)]
    scratch += [vmem(3, lv.rows, LANES) for lv in (l0, l1, l2)]
    scratch += [vmem(2, chip_y, TILE, LANES), vmem(2, n_x, reach, TILE, LANES), vmem(2, 2, l0.wide, TILE, LANES)]
    scratch += [vmem(2, l0.wide, nz, LANES)] * 2
    sems = [(10,), (2, l0.ny // 4), (16,), (16,), (2, len(SIDES)), (2, len(SIDES)), (total,), (total,), (PARTS, 2), (PARTS, 2)]
    scratch += [pltpu.SemaphoreType.DMA(shape) for shape in sems] + [pltpu.SemaphoreType.REGULAR]
    got = pl.pallas_call(
        functools.partial(kernel, cfg),
        out_shape=pltpu.VMEM(rhs.shape, F32),
        in_specs=[pl.BlockSpec(memory_space=pl.ANY)] * 2,
        out_specs=pl.BlockSpec(memory_space=pltpu.VMEM),
        scratch_shapes=scratch,
        compiler_params=pltpu.CompilerParams(collective_id=0, has_side_effects=True, vmem_limit_bytes=60 * 2 ** 20),
    )(rhs, start)
    got = pl.pallas_call(
        write_out,
        out_shape=jax.ShapeDtypeStruct(rhs.shape, F32),
        in_specs=[pl.BlockSpec(memory_space=pltpu.VMEM)],
        out_specs=pl.BlockSpec(memory_space=pl.ANY),
        scratch_shapes=[vmem(*rhs.shape), pltpu.SemaphoreType.DMA((chip_y // TILE,))],
    )(pltpu.with_memory_space_constraint(got, pltpu.VMEM))
    return jnp.transpose(got, (2, 0, 1))


def solution(mesh):
    counts = (mesh.shape['sx'], mesh.shape['sy'], mesh.shape['sz'])
    spec = P(('dp', 'sx'), 'sy', 'sz')

    def run(rhs_grid, u_start):
        size = rhs_grid.shape[0] // mesh.shape['dp']
        cycle = functools.partial(local_cycle, counts=counts, size=size)
        return jax.shard_map(cycle, mesh=mesh, in_specs=(spec, spec), out_specs=spec, check_vma=False)(rhs_grid, u_start)
    return run
```
